256 devices in a mesh: gx: 16 (over y, z_hi, core), gy: 16 (over x, z_lo).
Axes of the slice: x: 4, y: 4, z: 8 (z_hi: 2, z_lo: 4; z = z_hi * 4 + z_lo), core: 2. Of those that a mesh axis runs over, the one named last changes fastest.
Arguments:
- populations: float32 [19, 64, 128, 128], P(None, 'gx', 'gy'), may hold values from 0.004 to 0.8, as said below
- solid: int32 [64, 128, 128], P('gx', 'gy'), may hold values 0 or 1
- base_cell: int32 [3, 16, 16, 2, 768], P(None, 'gx', 'gy'), may hold values from 0 to 127, as said below
- offset: float32 [3, 16, 16, 2, 768], P(None, 'gx', 'gy'), may hold values from 0 to 1
- rest_displacement: float32 [3, 16, 16, 2, 768], P(None, 'gx', 'gy'), may hold values from 0 to 1
- stiffness: float32 [16, 16, 2], P('gx', 'gy'), may hold values from 0.006380062 to 0.063800626
- occupied: int32 [16, 16, 2], P('gx', 'gy'), may hold values from 0 to 1, as said below
- triangles: int32 [1280, 3], replicated, may hold values from 0 to 641, as said below
Outputs:
- populations_out: float32 [19, 64, 128, 128], P(None, 'gx', 'gy')
- offset_out: float32 [3, 16, 16, 2, 768], P(None, 'gx', 'gy')
The draws below stay inside these ranges and needn't reach their ends.
Inputs may be any that keep to these rules, and one draw needn't show every extreme that they name: `populations`: every entry is positive. `base_cell`: component 0 of a vertex stored at index i of gx lies in [i * 4, (i + 1) * 4), component 1 of one stored at index j of gy lies in [j * 8, (j + 1) * 8), component 2 lies below 128. The occupied slots of a device come first; each device has at least one, and some device has all 2. `triangles`: each row holds three different vertex numbers below 642.
All inputs are finite; a program needn't handle non-finite values. No bound on the sum of `solid` on one device may be relied on, other than what follows from the above.
Results may differ from the reference program's by a relative error of at most 0.0001.
Values sent between devices are 32-bit elements; how exact they have to be, the bound alone decides.
No kernel may reach another device: no remote copies, remote signals or barrier semaphores. Data moves between devices by JAX's collectives and lax.ppermute only.
A program may use at most 64 MiB of HBM per device.

```python
import math
import jax
import jax.numpy as jnp

CX = 4
CY = 8
CZ = 128
MEMBRANE_SLOTS = 2
VERTS = 642
PADDED_VERTICES = 768
TRIS = 1280
SUBSTEPS = 3
NX = 64
NY = 128
NZ = 128
N_GX = 16
N_GY = 16


DRAW_VELOCITIES = [[0, 0, 0], [1, 0, 0], [-1, 0, 0], [0, 1, 0], [0, -1, 0], [0, 0, 1], [0, 0, -1], [1, 1, 0], [-1, -1, 0], [1, -1, 0], [-1, 1, 0], [1, 0, 1], [-1, 0, -1], [1, 0, -1], [-1, 0, 1], [0, 1, 1], [0, -1, -1], [0, 1, -1], [0, -1, 1]]


DRAW_WEIGHTS = [1.0 / 3.0] + [1.0 / 18.0] * 6 + [1.0 / 36.0] * 12


def draw_populations(key, part):
    key_flow, key_noise = jax.random.split(jax.random.fold_in(key, 11))
    flow = jax.random.uniform(key_flow, (3, NX, NY, NZ), jnp.float32, -0.1, 0.1)
    noise = jax.random.uniform(key_noise, (19, NX, NY, NZ), jnp.float32, 0.7, 1.3)
    halo_layers = []
    for lattice_direction in range(19):
        vector = DRAW_VELOCITIES[lattice_direction]
        along = vector[0] * flow[0] + vector[1] * flow[1] + vector[2] * flow[2]
        halo_layers.append(DRAW_WEIGHTS[lattice_direction] * (1.0 + 3.0 * along) * noise[lattice_direction])
    return jnp.stack(halo_layers)


def draw_base_cell(key, part):
    key_x, key_y, key_z = jax.random.split(jax.random.fold_in(key, 23), 3)
    domain_extent = (N_GX, N_GY, MEMBRANE_SLOTS, PADDED_VERTICES)
    start_x = (jnp.arange(N_GX, dtype=jnp.int32) * CX).reshape(N_GX, 1, 1, 1)
    start_y = (jnp.arange(N_GY, dtype=jnp.int32) * CY).reshape(1, N_GY, 1, 1)
    cell_x = jax.random.randint(key_x, domain_extent, 0, CX, dtype=jnp.int32) + start_x
    cell_y = jax.random.randint(key_y, domain_extent, 0, CY, dtype=jnp.int32) + start_y
    cell_z = jax.random.randint(key_z, domain_extent, 0, CZ, dtype=jnp.int32)
    return jnp.stack([cell_x, cell_y, cell_z])


def draw_occupied(key, part):
    key_level, key_full = jax.random.split(jax.random.fold_in(key, 37))
    level = jax.random.randint(key_level, (N_GX, N_GY), 1, MEMBRANE_SLOTS + 1, dtype=jnp.int32)
    chosen = jax.random.randint(key_full, (), 0, N_GX * N_GY, dtype=jnp.int32)
    device_number = jnp.arange(N_GX * N_GY, dtype=jnp.int32).reshape(N_GX, N_GY)
    level = jnp.where(device_number == chosen, MEMBRANE_SLOTS, level)
    slot_number = jnp.arange(MEMBRANE_SLOTS, dtype=jnp.int32)[None, None, :]
    return (slot_number < level[:, :, None]).astype(jnp.int32)


def draw_triangles(key, part):
    key_first, key_near, distant_key = jax.random.split(jax.random.fold_in(key, 53), 3)
    half = VERTS // 2
    first = jax.random.randint(key_first, (TRIS,), 0, VERTS, dtype=jnp.int32)
    near = jax.random.randint(key_near, (TRIS,), 1, half, dtype=jnp.int32)
    far = jax.random.randint(distant_key, (TRIS,), half, VERTS, dtype=jnp.int32)
    return jnp.stack([first, (first + near) % VERTS, (first + far) % VERTS], axis=1)


def touch_ends(entries, rng, smallest, high):
    place = [jax.random.randint(jax.random.fold_in(rng, axis), (), 0, length) for axis, length in enumerate(entries.shape)]
    main_axis = entries.shape.index(max(entries.shape))
    beside = place[:main_axis] + [(place[main_axis] + 1) % entries.shape[main_axis]] + place[main_axis + 1:]
    return entries.at[tuple(place)].set(smallest).at[tuple(beside)].set(high)


def block_levels(own_key, shape, cuts, low, top_value):
    def one(dim, blocks):
        steps = jax.random.uniform(jax.random.fold_in(jax.random.fold_in(own_key, 6), dim), (blocks,), jnp.float32, low / len(cuts), top_value / len(cuts))
        return jnp.repeat(jnp.exp(steps), shape[dim] // blocks).reshape((-1,) + (1,) * (len(shape) - dim - 1))

    factor_of = one(*cuts[0])
    for cut in cuts[1:]:
        factor_of = factor_of * one(*cut)
    return factor_of


def setup_inputs(seed: int = 0) -> dict:
    key_of = jax.random.split(jax.random.key(seed), 9)
    return {
        "populations": draw_populations(jax.random.fold_in(key_of[8], 71), 0),
        "solid": touch_ends((jax.random.randint(key_of[1], (NX, NY, NZ), 0, 8) < 1).astype(jnp.int32), jax.random.fold_in(key_of[1], 1), 0, 1),
        "base_cell": draw_base_cell(jax.random.fold_in(key_of[8], 71), 0),
        "offset": jnp.clip(1.0 * jax.random.uniform(key_of[3], (3, N_GX, N_GY, MEMBRANE_SLOTS, PADDED_VERTICES), jnp.float32) ** block_levels(key_of[3], (3, N_GX, N_GY, MEMBRANE_SLOTS, PADDED_VERTICES), ((1, 16), (2, 16)), -0.2, 0.2), 0.0, 1.0),
        "rest_displacement": jnp.clip(1.0 * jax.random.uniform(key_of[4], (3, N_GX, N_GY, MEMBRANE_SLOTS, PADDED_VERTICES), jnp.float32) ** block_levels(key_of[4], (3, N_GX, N_GY, MEMBRANE_SLOTS, PADDED_VERTICES), ((1, 16), (2, 16)), -0.2, 0.2), 0.0, 1.0),
        "stiffness": jnp.clip(jnp.exp(math.log(0.063800626) - 2.3025852 * jax.random.uniform(key_of[5], (N_GX, N_GY, MEMBRANE_SLOTS), jnp.float32) ** block_levels(key_of[5], (N_GX, N_GY, MEMBRANE_SLOTS), ((0, 16), (1, 16)), -0.2, 0.2)), 0.006380062, 0.063800626),
        "occupied": draw_occupied(jax.random.fold_in(key_of[8], 71), 0),
        "triangles": draw_triangles(jax.random.fold_in(key_of[8], 71), 0),
    }


VELOCITIES = [[0, 0, 0], [1, 0, 0], [-1, 0, 0], [0, 1, 0], [0, -1, 0], [0, 0, 1], [0, 0, -1], [1, 1, 0], [-1, -1, 0], [1, -1, 0], [-1, 1, 0], [1, 0, 1], [-1, 0, -1], [1, 0, -1], [-1, 0, 1], [0, 1, 1], [0, -1, -1], [0, 1, -1], [0, -1, 1]]
OPPOSITE = [0, 2, 1, 4, 3, 6, 5, 8, 7, 10, 9, 12, 11, 14, 13, 16, 15, 18, 17]
LATTICE_WEIGHTS = [1.0 / 3.0] + [1.0 / 18.0] * 6 + [1.0 / 36.0] * 12
RELAX = 0.8


def kernel_weights(offset):
    return jnp.stack([(1.0 + jnp.cos(math.pi * (stencil_shift - offset) / 2.0)) / 4.0 for stencil_shift in (-1, 0, 1, 2)])


def membrane_force(offset, rest_displacement, stiffness, occupied, triangles):
    strain = offset - rest_displacement
    corners = [triangles[:, 0], triangles[:, 1], triangles[:, 2]]
    summed = strain[..., corners[0]] + strain[..., corners[1]] + strain[..., corners[2]]
    pulled_populations = jnp.zeros_like(strain)
    counts = jnp.zeros((strain.shape[-1],), jnp.float32)
    for corner in corners:
        pulled_populations = pulled_populations.at[..., corner].add(summed)
        counts = counts.at[corner].add(1.0)
    scaling = (stiffness * occupied.astype(jnp.float32))[None, :, :, :, None]
    return scaling * (pulled_populations - 3.0 * counts * strain)


def macro_state(populations, force_cell):
    density = jnp.sum(populations, axis=0)
    velocity_parts = []
    for dimension in range(3):
        moving = force_cell[dimension] * 0.5
        for lattice_direction in range(19):
            component = VELOCITIES[lattice_direction][dimension]
            if component != 0:
                moving = moving + component * populations[lattice_direction]
        velocity_parts.append(moving / density)
    return density, jnp.stack(velocity_parts)


def collide(populations, force_cell, solid):
    density, velocity = macro_state(populations, force_cell)
    squared = velocity[0] * velocity[0] + velocity[1] * velocity[1] + velocity[2] * velocity[2]
    working = velocity[0] * force_cell[0] + velocity[1] * force_cell[1] + velocity[2] * force_cell[2]
    walled = solid != 0
    relaxed = []
    for lattice_direction in range(19):
        vector = VELOCITIES[lattice_direction]
        along = vector[0] * velocity[0] + vector[1] * velocity[1] + vector[2] * velocity[2]
        pushed = vector[0] * force_cell[0] + vector[1] * force_cell[1] + vector[2] * force_cell[2]
        equilibrium = LATTICE_WEIGHTS[lattice_direction] * density * (1.0 + 3.0 * along + 4.5 * along * along - 1.5 * squared)
        source = (1.0 - 0.5 / RELAX) * LATTICE_WEIGHTS[lattice_direction] * (3.0 * (pushed - working) + 9.0 * along * pushed)
        current = populations[lattice_direction]
        updated = current - (current - equilibrium) / RELAX + source
        relaxed.append(jnp.where(walled, populations[OPPOSITE[lattice_direction]], updated))
    return relaxed


def reference(populations, solid, base_cell, offset, rest_displacement, stiffness, occupied, triangles):
    lattice = (NX, NY, NZ)
    cells = NX * NY * NZ
    coordinates = [[(base_cell[dimension] + stencil_shift) % lattice[dimension] for stencil_shift in (-1, 0, 1, 2)] for dimension in range(3)]
    live = occupied.astype(jnp.float32)[None, :, :, :, None]
    for substep in range(SUBSTEPS):
        force_vertex = membrane_force(offset, rest_displacement, stiffness, occupied, triangles)
        kernels = kernel_weights(offset)
        grid = jnp.zeros((3, cells), jnp.float32)
        for first in range(4):
            for second in range(4):
                for third in range(4):
                    index = (coordinates[0][first] * NY + coordinates[1][second]) * NZ + coordinates[2][third]
                    weight = kernels[first][0] * kernels[second][1] * kernels[third][2]
                    grid = grid.at[:, index.reshape(-1)].add((force_vertex * weight[None]).reshape(3, -1))
        force_cell = grid.reshape(3, NX, NY, NZ)
        relaxed = collide(populations, force_cell, solid)
        populations = jnp.stack([jnp.roll(relaxed[lattice_direction], tuple(VELOCITIES[lattice_direction]), axis=(0, 1, 2)) for lattice_direction in range(19)])
        flow = macro_state(populations, force_cell)[1].reshape(3, cells)
        moved = jnp.zeros_like(offset)
        for first in range(4):
            for second in range(4):
                for third in range(4):
                    index = (coordinates[0][first] * NY + coordinates[1][second]) * NZ + coordinates[2][third]
                    weight = kernels[first][0] * kernels[second][1] * kernels[third][2]
                    moved = moved + weight[None] * flow[:, index.reshape(-1)].reshape(offset.shape)
        offset = offset + live * moved
    return populations, offset
```

```python
import functools
import math

import jax
import jax.numpy as jnp
from jax import lax
from jax.experimental import pallas as pl
from jax.experimental.pallas import tpu as pltpu
from jax.sharding import PartitionSpec as P

SUBSTEPS = 3
AX = ("gx", "gy")

VELOCITIES = [
    [0, 0, 0],
    [1, 0, 0],
    [-1, 0, 0],
    [0, 1, 0],
    [0, -1, 0],
    [0, 0, 1],
    [0, 0, -1],
    [1, 1, 0],
    [-1, -1, 0],
    [1, -1, 0],
    [-1, 1, 0],
    [1, 0, 1],
    [-1, 0, -1],
    [1, 0, -1],
    [-1, 0, 1],
    [0, 1, 1],
    [0, -1, -1],
    [0, 1, -1],
    [0, -1, 1],
]
OPPOSITE = [0, 2, 1, 4, 3, 6, 5, 8, 7, 10, 9, 12, 11, 14, 13, 16, 15, 18, 17]
LATTICE_WEIGHTS = [1.0 / 3.0] + [1.0 / 18.0] * 6 + [1.0 / 36.0] * 12
RELAX = 0.8
CX, CY, CZ = 4, 8, 128
SLOTS, PAD = 2, 768
UP_X = [q for q in range(19) if VELOCITIES[q][0] == 1]
DOWN_X = [q for q in range(19) if VELOCITIES[q][0] == -1]
UP_Y = [q for q in range(19) if VELOCITIES[q][1] == 1]
DOWN_Y = [q for q in range(19) if VELOCITIES[q][1] == -1]
X_ORDER = [0, 1, 2, 3, 4, 5, -1]
Y_RIM = [8, 9, -1]
MAIN_ROWS = 3 * 7 * 8
RIM_ROWS = 3 * 3 * 8
TABLE_ROWS = MAIN_ROWS + RIM_ROWS
F32 = jnp.float32
HIGH = lax.Precision.HIGH
TILE = (8, CZ)


def tile_rows():
    return lax.broadcasted_iota(jnp.int32, TILE, 0)


def row_of(tile, r):
    return jnp.broadcast_to(tile[r : r + 1, :], (8, tile.shape[1]))


def choose(first, a, b):
    return jnp.where(first, a, b)


def stencil_kernels(offset):
    angle = offset * (math.pi / 2.0)
    c, s = jnp.cos(angle), jnp.sin(angle)
    return [(1.0 - s) * 0.25, (1.0 + c) * 0.25, (1.0 + s) * 0.25, (1.0 - c) * 0.25]


def pick(distance, kernels, r):
    out = jnp.zeros(distance.shape, F32)
    for n in range(4):
        out = jnp.where(distance == n, kernels[n][r : r + 1, :], out)
    return out


def vertex_tables(base, kernels, slot):
    rows = lax.broadcasted_iota(jnp.int32, (8, PAD), 0)
    x_value = jnp.where(rows < 6, rows, jnp.where(rows == 6, -1, 100))
    y_rim = jnp.where(rows < 2, rows + 8, jnp.where(rows == 2, -1, 100))
    base_x, base_y, base_z = [base[2 * a + slot : 2 * a + slot + 1, :] for a in range(3)]
    table_x = pick(x_value - base_x + 1, kernels, slot)
    table_y = pick(rows - base_y + 1, kernels, 2 + slot)
    table_rim = pick(y_rim - base_y + 1, kernels, 2 + slot)
    depth = lax.broadcasted_iota(jnp.int32, (CZ, PAD), 0)
    table_z = pick(jnp.bitwise_and(depth - base_z + 1, CZ - 1), kernels, 4 + slot)
    return table_x, table_y, table_rim, table_z


def vertex_force(offset, rest, scale, links_high, links_low):
    strain = offset - rest
    high = strain.astype(jnp.bfloat16)
    low = (strain - high.astype(F32)).astype(jnp.bfloat16)
    both = jnp.concatenate([high, low], axis=0)
    first = jnp.dot(both, links_high, preferred_element_type=F32)
    second = jnp.dot(both, links_low, preferred_element_type=F32)
    total = first + second
    return scale * (total[:8] + total[8:])


def spread(offset, rest, scale, base, links_high, links_low, terms, main_ref, rim_ref):
    force = vertex_force(offset, rest, scale, links_high, links_low)
    kernels = stencil_kernels(offset)
    grid = None
    for slot in range(SLOTS):
        table_x, table_y, table_rim, table_z = vertex_tables(base, kernels, slot)
        for a in range(3):
            pushed = force[2 * a + slot : 2 * a + slot + 1, :]
            along_x = table_x * pushed
            for n in range(7):
                terms[(a * 7 + n) * 8 : (a * 7 + n + 1) * 8, :] = row_of(along_x, n) * table_y
            along_y = table_rim * pushed
            for n in range(3):
                start = MAIN_ROWS + (a * 3 + n) * 8
                terms[start : start + 8, :] = row_of(along_y, n) * table_x
        part = lax.dot_general(
            terms[...], table_z, (((1,), (1,)), ((), ())), precision=HIGH, preferred_element_type=F32
        )
        grid = part if grid is None else grid + part
    main_ref[...] = grid[:MAIN_ROWS].reshape(3, 7, 8, CZ)
    rim_ref[...] = grid[MAIN_ROWS:].reshape(3, 3, 8, CZ)


def spread_messages(parity, main_ref, rim_ref, first_ref, second_ref):
    even = parity == 0
    zero = jnp.zeros((2, CZ), F32)
    for a in range(3):
        up_rows, down_rows = [], []
        for n in range(3):
            rim = rim_ref[a, n]
            up_rows.append(rim[4:6])
            down_rows.append(rim[6:8])
        ups = [main_ref[a, 4], main_ref[a, 5], jnp.concatenate(up_rows + [zero], axis=0)]
        downs = [main_ref[a, 6], main_ref[a, 6], jnp.concatenate(down_rows + [zero], axis=0)]
        for t in range(3):
            first_ref[a, t] = choose(even, ups[t], downs[t])
            second_ref[a, t] = choose(even, downs[t], ups[t])


def links_kernel(triangles_ref, high_ref, low_ref, incidence):
    vertex = lax.broadcasted_iota(jnp.int32, incidence.shape, 0)
    hit = jnp.zeros(incidence.shape, F32)
    for corner in range(3):
        hit = jnp.where(triangles_ref[corner : corner + 1, :] == vertex, 1.0, hit)
    incidence[...] = hit.astype(jnp.bfloat16)
    shared = lax.dot_general(
        incidence[...], incidence[...], (((1,), (1,)), ((), ())), preferred_element_type=F32
    )
    same = lax.broadcasted_iota(jnp.int32, shared.shape, 0) == lax.broadcasted_iota(
        jnp.int32, shared.shape, 1
    )
    shared = jnp.where(same, -2.0 * shared, shared)
    high = shared.astype(jnp.bfloat16)
    high_ref[...] = high
    low_ref[...] = (shared - high.astype(F32)).astype(jnp.bfloat16)


def spread_kernel(
    place_ref, offset_ref, rest_ref, scale_ref, base_ref, high_ref, low_ref,
    main_ref, rim_ref, first_ref, second_ref, terms,
):
    spread(
        offset_ref[...], rest_ref[...], scale_ref[...], base_ref[...],
        high_ref[...], low_ref[...], terms, main_ref, rim_ref,
    )
    spread_messages(place_ref[0], main_ref, rim_ref, first_ref, second_ref)


def force_corner_kernel(place_ref, rim_ref, first_in, second_in, first_ref, second_ref):
    even_x = place_ref[0] == 0
    even_y = place_ref[1] == 0
    rows = tile_rows()
    for a in range(3):
        above = choose(even_x, first_in[a, 2], second_in[a, 2])
        below = choose(even_x, second_in[a, 2], first_in[a, 2])
        whole = []
        for n in range(3):
            from_below = below[2 * n : 2 * n + 2]
            from_above = above[2 * n : 2 * n + 1]
            part = rim_ref[a, n][:4]
            whole.append(
                jnp.concatenate([part[0:2] + from_below, part[2:3], part[3:4] + from_above], axis=0)
            )
        up = jnp.concatenate([whole[0], whole[1]], axis=0)
        down = jnp.concatenate([whole[2], whole[2]], axis=0)
        first_ref[a] = choose(even_y, up, down)
        second_ref[a] = choose(even_y, down, up)


def moment_sums(members, rows):
    groups = {}
    for step in (0, 1, -1):
        of_step = [(q, t) for q, t in members if VELOCITIES[q][1] == step]
        sums = []
        for what in (None, 0, 2):
            total = None
            for q, t in of_step:
                weight = 1 if what is None else VELOCITIES[q][what]
                if weight == 0:
                    continue
                term = t if weight == 1 else -t
                total = term if total is None else total + term
            sums.append(jnp.zeros(TILE, F32) if total is None else total)
        groups[step] = sums
    up = [jnp.where(rows == 0, 0.0, t) for t in groups[1]]
    down = [jnp.where(rows == 7, 0.0, t) for t in groups[-1]]
    density, along_x, along_z = [groups[0][k] + up[k] + down[k] for k in range(3)]
    inside = [density, along_x, up[0] - down[0], along_z]
    edge = [
        jnp.where(rows == 0, groups[1][k], jnp.where(rows == 7, groups[-1][k], 0.0)) for k in range(3)
    ]
    return inside, edge


def pack_edges(edge):
    return edge[0] + pltpu.roll(edge[1], 2, 0) + pltpu.roll(edge[2], 4, 0)


def unpack_edges(packed, rows):
    keep = (rows == 0) | (rows == 7)
    tiles = [packed, pltpu.roll(packed, 6, 0), pltpu.roll(packed, 4, 0)]
    return [jnp.where(keep, t, 0.0) for t in tiles]


def collide_kernel(
    place_ref, populations_ref, solid_ref, main_ref, first_x, second_x, first_y, second_y,
    stepped_ref, force_ref, first_ref, second_ref,
):
    even_x = place_ref[0] == 0
    even_y = place_ref[1] == 0
    rows = tile_rows()
    for x in range(4):
        force = []
        for a in range(3):
            f = main_ref[a, x]
            if x < 2:
                f = f + choose(even_x, second_x[a, x], first_x[a, x])
            if x == 3:
                f = f + choose(even_x, first_x[a, 0], second_x[a, 0])
            below = choose(even_y, second_y[a], first_y[a])
            above = choose(even_y, first_y[a], second_y[a])
            f = f + jnp.where(
                rows == 0,
                row_of(below, x),
                jnp.where(rows == 1, row_of(below, 4 + x), jnp.where(rows == 7, row_of(above, x), 0.0)),
            )
            force_ref[a, x] = f
            force.append(f)
        current = [populations_ref[q, x] for q in range(19)]
        density = functools.reduce(lambda u, v: u + v, current)
        velocity = []
        for a in range(3):
            moving = force[a] * 0.5
            for q in range(19):
                if VELOCITIES[q][a] == 1:
                    moving = moving + current[q]
                elif VELOCITIES[q][a] == -1:
                    moving = moving - current[q]
            velocity.append(moving)
        inverse = 1.0 / density
        velocity = [m * inverse for m in velocity]
        squared = velocity[0] * velocity[0] + velocity[1] * velocity[1] + velocity[2] * velocity[2]
        working = velocity[0] * force[0] + velocity[1] * force[1] + velocity[2] * force[2]
        walled = solid_ref[x] != 0
        common = 1.0 - 1.5 * squared
        factor = 1.0 - 0.5 / RELAX
        for q in range(19):
            vector = VELOCITIES[q]
            w = LATTICE_WEIGHTS[q]
            if q == 0:
                equilibrium = w * density * common
                source = (-3.0 * factor * w) * working
            else:
                along, pushed = None, None
                for a in range(3):
                    if vector[a] == 0:
                        continue
                    u = velocity[a] if vector[a] == 1 else -velocity[a]
                    f = force[a] if vector[a] == 1 else -force[a]
                    along = u if along is None else along + u
                    pushed = f if pushed is None else pushed + f
                equilibrium = w * density * (common + along * (3.0 + 4.5 * along))
                source = (factor * w) * (3.0 * (pushed - working) + 9.0 * along * pushed)
            updated = current[q] - (current[q] - equilibrium) / RELAX + source
            relaxed = jnp.where(walled, current[OPPOSITE[q]], updated)
            if vector[2] != 0:
                relaxed = pltpu.roll(relaxed, vector[2] % CZ, 1)
            if vector[1] != 0:
                relaxed = pltpu.roll(relaxed, vector[1] % 8, 0)
            stepped_ref[q, (x + vector[0]) % 4] = relaxed
    messages = []
    for crossing, lines in ((UP_X, (3,)), (DOWN_X, (0, 1))):
        slot = 0 if crossing is UP_X else 3
        tiles = [stepped_ref[q, slot] for q in crossing]
        for x in lines:
            members = [
                (q, stepped_ref[q, x])
                for q in range(19)
                if not (x == 0 and VELOCITIES[q][0] == 1) and not (x == 3 and VELOCITIES[q][0] == -1)
            ]
            inside, edge = moment_sums(members, rows)
            for k in range(3):
                inside[1 + k] = inside[1 + k] + 0.5 * force_ref[k, x]
            tiles += inside + [pack_edges(edge)]
        messages.append(tiles)
    up, down = messages
    for t in range(15):
        u = up[t] if t < len(up) else down[t]
        first_ref[t] = choose(even_x, u, down[t])
        second_ref[t] = choose(even_x, down[t], u)


def flow_corner_kernel(
    place_ref, stepped_in, force_ref, first_x, second_x,
    stepped_ref, inside_ref, leaving_ref, first_ref, second_ref, edges, up_tiles, down_tiles,
):
    even_x = place_ref[0] == 0
    even_y = place_ref[1] == 0
    rows = tile_rows()
    below = [choose(even_x, second_x[t], first_x[t]) for t in range(10)]
    above = [choose(even_x, first_x[t], second_x[t]) for t in range(15)]
    out_up = [(q, stepped_in[q, 0]) for q in UP_X]
    out_down = [(q, stepped_in[q, 3]) for q in DOWN_X]
    for q in range(19):
        for x in range(4):
            s = stepped_in[q, x]
            if q in UP_X and x == 0:
                s = below[UP_X.index(q)]
            if q in DOWN_X and x == 3:
                s = above[DOWN_X.index(q)]
            stepped_ref[(q * 4 + x) * 8 : (q * 4 + x + 1) * 8, :] = s
    for n, x in enumerate(X_ORDER):
        if 0 <= x < 4:
            members = [(q, stepped_ref[(q * 4 + x) * 8 : (q * 4 + x + 1) * 8, :]) for q in range(19)]
            inside, edge = moment_sums(members, rows)
            for k in range(3):
                inside[1 + k] = inside[1 + k] + 0.5 * force_ref[k, x]
        else:
            received = below[5:10] if x == -1 else above[5 + 5 * (x - 4) : 10 + 5 * (x - 4)]
            inside, edge = received[:4], unpack_edges(received[4], rows)
            if x != 5:
                own_inside, own_edge = moment_sums(out_down if x == -1 else out_up, rows)
                inside = [u + v for u, v in zip(inside, own_inside)]
                edge = [u + v for u, v in zip(edge, own_edge)]
        for k in range(4):
            inside_ref[(k * 8 + n) * 8 : (k * 8 + n + 1) * 8, :] = inside[k]
        for k in range(3):
            edges[(k * 8 + n) * 8 : (k * 8 + n + 1) * 8, :] = edge[k]
    for k in range(4):
        inside_ref[(k * 8 + 7) * 8 : (k * 8 + 8) * 8, :] = jnp.ones(TILE, F32)
    for k in range(3):
        edges[(k * 8 + 7) * 8 : (k * 8 + 8) * 8, :] = jnp.zeros(TILE, F32)
    for k in range(3):
        up = edges[pl.ds(k * 64, 8, stride=8), :]
        down = edges[pl.ds(k * 64 + 7, 8, stride=8), :]
        leaving_ref[k] = up
        leaving_ref[3 + k] = down
        up_tiles[k] = up
        down_tiles[k] = down
    for t in range(3, 5):
        up_tiles[t] = jnp.zeros(TILE, F32)
        down_tiles[t] = jnp.zeros(TILE, F32)
    for t in range(5):
        up_tiles[t, 0:4, :] = stepped_ref[pl.ds(UP_Y[t] * 32, 4, stride=8), :]
        down_tiles[t, 0:4, :] = stepped_ref[pl.ds(DOWN_Y[t] * 32 + 7, 4, stride=8), :]
    for k in range(4):
        up_tiles[5 + k] = inside_ref[pl.ds(k * 64 + 7, 8, stride=8), :]
        down_tiles[5 + k] = inside_ref[pl.ds(k * 64, 8, stride=8), :]
        down_tiles[9 + k] = inside_ref[pl.ds(k * 64 + 1, 8, stride=8), :]
    for t in range(13):
        u = up_tiles[t] if t < 9 else down_tiles[t]
        d = down_tiles[t]
        first_ref[t] = choose(even_y, u, d)
        second_ref[t] = choose(even_y, d, u)


def finish_fluid(place_ref, stepped_ref, inside_ref, leaving_ref, first_y, second_y, out_ref, flow):
    even_y = place_ref[1] == 0
    rows = tile_rows()
    below = [choose(even_y, second_y[t], first_y[t]) for t in range(9)]
    above = [choose(even_y, first_y[t], second_y[t]) for t in range(13)]
    for q in range(19):
        for x in range(4):
            s = stepped_ref[(q * 4 + x) * 8 : (q * 4 + x + 1) * 8, :]
            if q in UP_Y:
                s = jnp.where(rows == 0, row_of(below[UP_Y.index(q)], x), s)
            if q in DOWN_Y:
                s = jnp.where(rows == 7, row_of(above[DOWN_Y.index(q)], x), s)
            out_ref[q, x] = s
    if flow is None:
        return

    def arriving(tiles, members):
        out = []
        for k, what in enumerate((None, 0, 2)):
            total = None
            for n, q in enumerate(members):
                weight = 1 if what is None else VELOCITIES[q][what]
                if weight:
                    term = tiles[n] if weight == 1 else -tiles[n]
                    total = term if total is None else total + term
            out.append(jnp.where(rows < 4, total, tiles[k]))
        return [out[0], out[1], None, out[2]]

    from_below = arriving(below, UP_Y)
    from_above = arriving(above, DOWN_Y)
    from_below[2] = from_below[0]
    from_above[2] = -from_above[0]
    for n in range(7):
        total = []
        for k in range(4):
            t = inside_ref[(k * 8 + n) * 8 : (k * 8 + n + 1) * 8, :]
            t = t + jnp.where(
                rows == 0,
                row_of(from_below[k], n),
                jnp.where(rows == 7, row_of(from_above[k], n), 0.0),
            )
            total.append(t)
        inverse = 1.0 / total[0]
        for a in range(3):
            flow[(a * 7 + n) * 8 : (a * 7 + n + 1) * 8, :] = total[1 + a] * inverse
    up = [leaving_ref[0], leaving_ref[1], leaving_ref[0], leaving_ref[2]]
    down = [leaving_ref[3], leaving_ref[4], -leaving_ref[3], leaving_ref[5]]
    rims = (
        [above[5 + k] + up[k] for k in range(4)],
        [above[9 + k] for k in range(4)],
        [below[5 + k] + down[k] for k in range(4)],
    )
    for n, total in enumerate(rims):
        inverse = 1.0 / jnp.where(rows == 7, 1.0, total[0])
        for a in range(3):
            start = MAIN_ROWS + (a * 3 + n) * 8
            flow[start : start + 8, :] = jnp.where(rows == 7, 0.0, total[1 + a] * inverse)


def sample(offset, live, base, flow):
    kernels = stencil_kernels(offset)
    moved = [None] * 8
    zero = jnp.zeros((1, PAD), F32)
    for slot in range(SLOTS):
        table_x, table_y, table_rim, table_z = vertex_tables(base, kernels, slot)
        along = jnp.dot(flow[...], table_z, precision=HIGH, preferred_element_type=F32)
        for a in range(3):
            inner = None
            for n in range(7):
                tile = along[(a * 7 + n) * 8 : (a * 7 + n + 1) * 8, :]
                term = tile * row_of(table_x, n)
                inner = term if inner is None else inner + term
            total = inner * table_y
            outer = None
            for n in range(3):
                start = MAIN_ROWS + (a * 3 + n) * 8
                term = along[start : start + 8, :] * row_of(table_rim, n)
                outer = term if outer is None else outer + term
            total = total + outer * table_x
            moved[2 * a + slot] = jnp.sum(total, axis=0, keepdims=True)
    stacked = jnp.concatenate(moved[:6] + [zero, zero], axis=0)
    return offset + live * stacked


def next_kernel(
    place_ref, stepped_ref, inside_ref, leaving_ref, first_y, second_y,
    offset_ref, rest_ref, scale_ref, live_ref, base_ref, high_ref, low_ref,
    out_ref, offset_out, main_ref, rim_ref, first_ref, second_ref, flow, terms,
):
    finish_fluid(place_ref, stepped_ref, inside_ref, leaving_ref, first_y, second_y, out_ref, flow)
    offset = sample(offset_ref[...], live_ref[...], base_ref[...], flow)
    offset_out[...] = offset
    spread(
        offset, rest_ref[...], scale_ref[...], base_ref[...],
        high_ref[...], low_ref[...], terms, main_ref, rim_ref,
    )
    spread_messages(place_ref[0], main_ref, rim_ref, first_ref, second_ref)


def last_kernel(
    place_ref, stepped_ref, inside_ref, leaving_ref, first_y, second_y,
    offset_ref, live_ref, base_ref,
    out_ref, offset_out, flow,
):
    finish_fluid(place_ref, stepped_ref, inside_ref, leaving_ref, first_y, second_y, out_ref, flow)
    offset_out[...] = sample(offset_ref[...], live_ref[...], base_ref[...], flow)


INTERPRET = False


def call(kernel, outs, scratch, *operands, name):
    in_specs = [pl.BlockSpec(memory_space=pltpu.SMEM)] if kernel is not links_kernel else []
    in_specs += [pl.BlockSpec(memory_space=pltpu.VMEM)] * (len(operands) - len(in_specs))
    return pl.pallas_call(
        kernel,
        out_shape=[jax.ShapeDtypeStruct(shape, dtype) for shape, dtype in outs],
        in_specs=in_specs,
        out_specs=[pl.BlockSpec(memory_space=pltpu.VMEM)] * len(outs),
        scratch_shapes=[pltpu.VMEM(shape, dtype) for shape, dtype in scratch],
        compiler_params=pltpu.CompilerParams(vmem_limit_bytes=24 * 1024 * 1024),
        interpret=INTERPRET,
        name=name,
    )(*operands)


def partner(index, kind, size):
    return (index + 1) % size if (index + kind) % 2 == 0 else (index - 1) % size


def exchange(first, second, axis):
    size = lax.axis_size(axis)
    out = []
    for kind, message in ((0, first), (1, second)):
        pairs = [(i, partner(i, kind, size)) for i in range(size)]
        out.append(lax.ppermute(message, axis, pairs))
    return out


SPREAD_OUT = [
    ((3, 7, 8, CZ), F32),
    ((3, 3, 8, CZ), F32),
    ((3, 3, 8, CZ), F32),
    ((3, 3, 8, CZ), F32),
]
STEPPED = ((19, 4, 8, CZ), F32)


def local(populations, solid, base_cell, offset, rest_displacement, stiffness, occupied, triangles):
    place_x = lax.axis_index("gx")
    place_y = lax.axis_index("gy")
    place = jnp.stack([place_x % 2, place_y % 2]).astype(jnp.int32)

    def pad(rows):
        return jnp.pad(rows.reshape(6, PAD), ((0, 2), (0, 0)))

    start = jnp.stack([place_x * CX, place_y * CY, place_x * 0]).astype(jnp.int32)
    base = pad(base_cell.reshape(3, SLOTS, PAD) - start[:, None, None])
    where = pad(offset)
    rest = pad(rest_displacement)
    held = occupied.reshape(1, SLOTS, 1).astype(F32)
    spring = stiffness.reshape(1, SLOTS, 1) * held
    scale = pad(jnp.broadcast_to(spring, (3, SLOTS, PAD)))
    live = pad(jnp.broadcast_to(held, (3, SLOTS, PAD)))
    corners = triangles.T
    links = [((PAD, PAD), jnp.bfloat16)] * 2
    high, low = call(
        links_kernel, links, [((PAD, triangles.shape[0]), jnp.bfloat16)], corners, name="links"
    )
    terms = ((TABLE_ROWS, PAD), F32)
    flow = ((TABLE_ROWS, CZ), F32)
    main, rim, first, second = call(
        spread_kernel, SPREAD_OUT, [terms], place, where, rest, scale, base, high, low, name="spread"
    )
    for substep in range(SUBSTEPS):
        first_x, second_x = exchange(first, second, "gx")
        corner = call(
            force_corner_kernel, [((3, 8, CZ), F32)] * 2, [], place, rim, first_x, second_x,
            name="force_corner",
        )
        first_y, second_y = exchange(*corner, "gy")
        stepped, force, first, second = call(
            collide_kernel,
            [STEPPED, ((3, 4, 8, CZ), F32), ((15, 8, CZ), F32), ((15, 8, CZ), F32)],
            [],
            place, populations, solid, main, first_x, second_x, first_y, second_y,
            name="collide",
        )
        first_x, second_x = exchange(first, second, "gx")
        stepped, inside, leaving, first, second = call(
            flow_corner_kernel,
            [
                ((19 * 4 * 8, CZ), F32), ((4 * 8 * 8, CZ), F32), ((6, 8, CZ), F32),
                ((13, 8, CZ), F32), ((13, 8, CZ), F32),
            ],
            [((3 * 8 * 8, CZ), F32), ((5, 8, CZ), F32), ((13, 8, CZ), F32)][:1]
            + [((9, 8, CZ), F32), ((13, 8, CZ), F32)],
            place, stepped, force, first_x, second_x,
            name="flow_corner",
        )
        first_y, second_y = exchange(first, second, "gy")
        fluid = (place, stepped, inside, leaving, first_y, second_y)
        if substep < SUBSTEPS - 1:
            populations, where, main, rim, first, second = call(
                next_kernel, [STEPPED, ((8, PAD), F32)] + SPREAD_OUT, [flow, terms],
                *fluid, where, rest, scale, live, base, high, low, name="next",
            )
        else:
            populations, where = call(
                last_kernel, [STEPPED, ((8, PAD), F32)], [flow], *fluid, where, live, base, name="last"
            )
    return populations, where[:6].reshape(offset.shape)


def solution(mesh):
    in_specs = (
        P(None, "gx", "gy", None),
        P("gx", "gy", None),
        P(None, "gx", "gy", None, None),
        P(None, "gx", "gy", None, None),
        P(None, "gx", "gy", None, None),
        P("gx", "gy", None),
        P("gx", "gy", None),
        P(),
    )
    out_specs = (P(None, "gx", "gy", None), P(None, "gx", "gy", None, None))
    return jax.shard_map(local, mesh=mesh, in_specs=in_specs, out_specs=out_specs, check_vma=False)
```

```python
import functools
import math

import jax
import jax.numpy as jnp
from jax import lax
from jax.experimental import pallas as pl
from jax.experimental.pallas import tpu as pltpu
from jax.sharding import PartitionSpec as P

SUBSTEPS = 3
AX = ("gx", "gy")

VELOCITIES = [
    [0, 0, 0],
    [1, 0, 0],
    [-1, 0, 0],
    [0, 1, 0],
    [0, -1, 0],
    [0, 0, 1],
    [0, 0, -1],
    [1, 1, 0],
    [-1, -1, 0],
    [1, -1, 0],
    [-1, 1, 0],
    [1, 0, 1],
    [-1, 0, -1],
    [1, 0, -1],
    [-1, 0, 1],
    [0, 1, 1],
    [0, -1, -1],
    [0, 1, -1],
    [0, -1, 1],
]
OPPOSITE = [0, 2, 1, 4, 3, 6, 5, 8, 7, 10, 9, 12, 11, 14, 13, 16, 15, 18, 17]
LATTICE_WEIGHTS = [1.0 / 3.0] + [1.0 / 18.0] * 6 + [1.0 / 36.0] * 12
RELAX = 0.8
CX, CY, CZ = 4, 8, 128
SLOTS, PAD = 2, 768
UP_X = [q for q in range(19) if VELOCITIES[q][0] == 1]
DOWN_X = [q for q in range(19) if VELOCITIES[q][0] == -1]
UP_Y = [q for q in range(19) if VELOCITIES[q][1] == 1]
DOWN_Y = [q for q in range(19) if VELOCITIES[q][1] == -1]
X_ORDER = [0, 1, 2, 3, 4, 5, -1]
Y_RIM = [8, 9, -1]
MAIN_ROWS = 3 * 7 * 8
RIM_ROWS = 3 * 3 * 8
TABLE_ROWS = MAIN_ROWS + RIM_ROWS
F32 = jnp.float32
HIGH = lax.Precision.HIGH
TILE = (8, CZ)


def tile_rows():
    return lax.broadcasted_iota(jnp.int32, TILE, 0)


def wide(row):
    return jnp.concatenate([row] * (PAD // CZ), axis=1)


def six_rows(ref):
    return jnp.concatenate([ref[0], ref[1], ref[2], jnp.zeros((2, PAD), ref.dtype)], axis=0)


def own_base(info_ref, base_ref):
    base = six_rows(base_ref)
    rows = lax.broadcasted_iota(jnp.int32, TILE, 0)
    start = jnp.where(rows < 2, info_ref[2], jnp.where(rows < 4, info_ref[3], 0.0))
    return base - wide(start.astype(jnp.int32))


def row_of(tile, r):
    return jnp.broadcast_to(tile[r : r + 1, :], (8, tile.shape[1]))


def choose(first, a, b):
    return jnp.where(first, a, b)


def stencil_kernels(offset):
    angle = offset * (math.pi / 2.0)
    c, s = jnp.cos(angle), jnp.sin(angle)
    return [(1.0 - s) * 0.25, (1.0 + c) * 0.25, (1.0 + s) * 0.25, (1.0 - c) * 0.25]


def pick(distance, kernels, r):
    out = jnp.zeros(distance.shape, F32)
    for n in range(4):
        out = jnp.where(distance == n, kernels[n][r : r + 1, :], out)
    return out


def vertex_tables(base, kernels, slot):
    rows = lax.broadcasted_iota(jnp.int32, (8, PAD), 0)
    x_value = jnp.where(rows < 6, rows, jnp.where(rows == 6, -1, 100))
    y_rim = jnp.where(rows < 2, rows + 8, jnp.where(rows == 2, -1, 100))
    base_x, base_y, base_z = [base[2 * a + slot : 2 * a + slot + 1, :] for a in range(3)]
    table_x = pick(x_value - base_x + 1, kernels, slot)
    table_y = pick(rows - base_y + 1, kernels, 2 + slot)
    table_rim = pick(y_rim - base_y + 1, kernels, 2 + slot)
    depth = lax.broadcasted_iota(jnp.int32, (CZ, PAD), 0)
    table_z = pick(jnp.bitwise_and(depth - base_z + 1, CZ - 1), kernels, 4 + slot)
    return table_x, table_y, table_rim, table_z


def halves(rows):
    high = rows.astype(jnp.bfloat16)
    return jnp.concatenate([high, (rows - high.astype(F32)).astype(jnp.bfloat16)], axis=0)


def vertex_force(offset, rest, scale, incidence):
    strain = offset - rest
    summed = jnp.dot(halves(strain), incidence[...], preferred_element_type=F32)
    summed = summed[:8] + summed[8:]
    rows = lax.broadcasted_iota(jnp.int32, summed.shape, 0)
    summed = jnp.where(rows == 6, 1.0, summed)
    pulled = lax.dot_general(
        halves(summed), incidence[...], (((1,), (1,)), ((), ())), preferred_element_type=F32
    )
    pulled = pulled[:8] + pulled[8:]
    return scale * (pulled - 3.0 * pulled[6:7] * strain)


def spread(offset, rest, scale, base, incidence, terms, main_ref, rim_ref):
    force = vertex_force(offset, rest, scale, incidence)
    kernels = stencil_kernels(offset)
    grid = None
    for slot in range(SLOTS):
        table_x, table_y, table_rim, table_z = vertex_tables(base, kernels, slot)
        for a in range(3):
            pushed = force[2 * a + slot : 2 * a + slot + 1, :]
            along_x = table_x * pushed
            for n in range(7):
                terms[(a * 7 + n) * 8 : (a * 7 + n + 1) * 8, :] = row_of(along_x, n) * table_y
            along_y = table_rim * pushed
            for n in range(3):
                start = MAIN_ROWS + (a * 3 + n) * 8
                terms[start : start + 8, :] = row_of(along_y, n) * table_x
        part = lax.dot_general(
            terms[...], table_z, (((1,), (1,)), ((), ())), precision=HIGH, preferred_element_type=F32
        )
        grid = part if grid is None else grid + part
    main_ref[...] = grid[:MAIN_ROWS].reshape(3, 7, 8, CZ)
    rim_ref[...] = grid[MAIN_ROWS:].reshape(3, 3, 8, CZ)


def spread_messages(info_ref, main_ref, rim_ref, first_ref, second_ref):
    even = info_ref[0] == 0.0
    zero = jnp.zeros((2, CZ), F32)
    for a in range(3):
        up_rows, down_rows = [], []
        for n in range(3):
            rim = rim_ref[a, n]
            up_rows.append(rim[4:6])
            down_rows.append(rim[6:8])
        ups = [main_ref[a, 4], main_ref[a, 5], jnp.concatenate(up_rows + [zero], axis=0)]
        downs = [main_ref[a, 6], main_ref[a, 6], jnp.concatenate(down_rows + [zero], axis=0)]
        for t in range(3):
            first_ref[a, t] = choose(even, ups[t], downs[t])
            second_ref[a, t] = choose(even, downs[t], ups[t])


def incidence_kernel(triangles_ref, incidence_ref):
    vertex = lax.broadcasted_iota(jnp.int32, incidence_ref.shape, 0)
    corners = [triangles_ref[corner : corner + 1, :] == vertex for corner in range(3)]
    hit = corners[0] | corners[1] | corners[2]
    incidence_ref[...] = jnp.where(hit, 1.0, 0.0).astype(jnp.bfloat16)


def spread_kernel(
    info_ref, offset_in, rest_in, base_in, populations_in, solid_in, incidence_ref,
    main_ref, rim_ref, first_ref, second_ref,
    offset_ref, rest_ref, base_ref, populations_ref, solid_ref, terms,
):
    offset_ref[...] = six_rows(offset_in)
    rest_ref[...] = six_rows(rest_in)
    base_ref[...] = own_base(info_ref, base_in)
    populations_ref[...] = populations_in[...]
    solid_ref[...] = solid_in[...]
    spread(
        offset_ref[...], rest_ref[...], wide(info_ref[4]), base_ref[...],
        incidence_ref, terms, main_ref, rim_ref,
    )
    spread_messages(info_ref, main_ref, rim_ref, first_ref, second_ref)


def force_corner_kernel(info_ref, rim_ref, first_in, second_in, first_ref, second_ref):
    even_x = info_ref[0] == 0.0
    even_y = info_ref[1] == 0.0
    rows = tile_rows()
    for a in range(3):
        above = choose(even_x, first_in[a, 2], second_in[a, 2])
        below = choose(even_x, second_in[a, 2], first_in[a, 2])
        whole = []
        for n in range(3):
            from_below = below[2 * n : 2 * n + 2]
            from_above = above[2 * n : 2 * n + 1]
            part = rim_ref[a, n][:4]
            whole.append(
                jnp.concatenate([part[0:2] + from_below, part[2:3], part[3:4] + from_above], axis=0)
            )
        up = jnp.concatenate([whole[0], whole[1]], axis=0)
        down = jnp.concatenate([whole[2], whole[2]], axis=0)
        first_ref[a] = choose(even_y, up, down)
        second_ref[a] = choose(even_y, down, up)


def moment_sums(members, rows):
    groups = {}
    for step in (0, 1, -1):
        of_step = [(q, t) for q, t in members if VELOCITIES[q][1] == step]
        sums = []
        for what in (None, 0, 2):
            total = None
            for q, t in of_step:
                weight = 1 if what is None else VELOCITIES[q][what]
                if weight == 0:
                    continue
                term = t if weight == 1 else -t
                total = term if total is None else total + term
            sums.append(jnp.zeros(TILE, F32) if total is None else total)
        groups[step] = sums
    up = [jnp.where(rows == 0, 0.0, t) for t in groups[1]]
    down = [jnp.where(rows == 7, 0.0, t) for t in groups[-1]]
    density, along_x, along_z = [groups[0][k] + up[k] + down[k] for k in range(3)]
    inside = [density, along_x, up[0] - down[0], along_z]
    edge = [
        jnp.where(rows == 0, groups[1][k], jnp.where(rows == 7, groups[-1][k], 0.0)) for k in range(3)
    ]
    return inside, edge


def pack_edges(edge):
    return edge[0] + pltpu.roll(edge[1], 2, 0) + pltpu.roll(edge[2], 4, 0)


def unpack_edges(packed, rows):
    keep = (rows == 0) | (rows == 7)
    tiles = [packed, pltpu.roll(packed, 6, 0), pltpu.roll(packed, 4, 0)]
    return [jnp.where(keep, t, 0.0) for t in tiles]


def collide_kernel(
    info_ref, populations_ref, solid_ref, main_ref, first_x, second_x, first_y, second_y,
    stepped_ref, force_ref, first_ref, second_ref,
):
    even_x = info_ref[0] == 0.0
    even_y = info_ref[1] == 0.0
    rows = tile_rows()
    for x in range(4):
        force = []
        for a in range(3):
            f = main_ref[a, x]
            if x < 2:
                f = f + choose(even_x, second_x[a, x], first_x[a, x])
            if x == 3:
                f = f + choose(even_x, first_x[a, 0], second_x[a, 0])
            below = choose(even_y, second_y[a], first_y[a])
            above = choose(even_y, first_y[a], second_y[a])
            f = f + jnp.where(
                rows == 0,
                row_of(below, x),
                jnp.where(rows == 1, row_of(below, 4 + x), jnp.where(rows == 7, row_of(above, x), 0.0)),
            )
            force_ref[a, x] = f
            force.append(f)
        current = [populations_ref[q, x] for q in range(19)]
        density = functools.reduce(lambda u, v: u + v, current)
        velocity = []
        for a in range(3):
            moving = force[a] * 0.5
            for q in range(19):
                if VELOCITIES[q][a] == 1:
                    moving = moving + current[q]
                elif VELOCITIES[q][a] == -1:
                    moving = moving - current[q]
            velocity.append(moving)
        inverse = 1.0 / density
        velocity = [m * inverse for m in velocity]
        squared = velocity[0] * velocity[0] + velocity[1] * velocity[1] + velocity[2] * velocity[2]
        working = velocity[0] * force[0] + velocity[1] * force[1] + velocity[2] * force[2]
        walled = solid_ref[x] != 0
        common = 1.0 - 1.5 * squared
        factor = 1.0 - 0.5 / RELAX
        for q in range(19):
            vector = VELOCITIES[q]
            w = LATTICE_WEIGHTS[q]
            if q == 0:
                equilibrium = w * density * common
                source = (-3.0 * factor * w) * working
            else:
                along, pushed = None, None
                for a in range(3):
                    if vector[a] == 0:
                        continue
                    u = velocity[a] if vector[a] == 1 else -velocity[a]
                    f = force[a] if vector[a] == 1 else -force[a]
                    along = u if along is None else along + u
                    pushed = f if pushed is None else pushed + f
                equilibrium = w * density * (common + along * (3.0 + 4.5 * along))
                source = (factor * w) * (3.0 * (pushed - working) + 9.0 * along * pushed)
            updated = current[q] - (current[q] - equilibrium) / RELAX + source
            relaxed = jnp.where(walled, current[OPPOSITE[q]], updated)
            if vector[2] != 0:
                relaxed = pltpu.roll(relaxed, vector[2] % CZ, 1)
            if vector[1] != 0:
                relaxed = pltpu.roll(relaxed, vector[1] % 8, 0)
            stepped_ref[q, (x + vector[0]) % 4] = relaxed
    messages = []
    for crossing, lines in ((UP_X, (3,)), (DOWN_X, (0, 1))):
        slot = 0 if crossing is UP_X else 3
        tiles = [stepped_ref[q, slot] for q in crossing]
        for x in lines:
            members = [
                (q, stepped_ref[q, x])
                for q in range(19)
                if not (x == 0 and VELOCITIES[q][0] == 1) and not (x == 3 and VELOCITIES[q][0] == -1)
            ]
            inside, edge = moment_sums(members, rows)
            for k in range(3):
                inside[1 + k] = inside[1 + k] + 0.5 * force_ref[k, x]
            tiles += inside + [pack_edges(edge)]
        messages.append(tiles)
    up, down = messages
    for t in range(15):
        u = up[t] if t < len(up) else down[t]
        first_ref[t] = choose(even_x, u, down[t])
        second_ref[t] = choose(even_x, down[t], u)


def flow_corner_kernel(
    info_ref, stepped_in, force_ref, first_x, second_x,
    stepped_ref, inside_ref, leaving_ref, first_ref, second_ref, edges, up_tiles, down_tiles,
):
    even_x = info_ref[0] == 0.0
    even_y = info_ref[1] == 0.0
    rows = tile_rows()
    below = [choose(even_x, second_x[t], first_x[t]) for t in range(10)]
    above = [choose(even_x, first_x[t], second_x[t]) for t in range(15)]
    out_up = [(q, stepped_in[q, 0]) for q in UP_X]
    out_down = [(q, stepped_in[q, 3]) for q in DOWN_X]
    for q in range(19):
        for x in range(4):
            s = stepped_in[q, x]
            if q in UP_X and x == 0:
                s = below[UP_X.index(q)]
            if q in DOWN_X and x == 3:
                s = above[DOWN_X.index(q)]
            stepped_ref[(q * 4 + x) * 8 : (q * 4 + x + 1) * 8, :] = s
    for n, x in enumerate(X_ORDER):
        if 0 <= x < 4:
            members = [(q, stepped_ref[(q * 4 + x) * 8 : (q * 4 + x + 1) * 8, :]) for q in range(19)]
            inside, edge = moment_sums(members, rows)
            for k in range(3):
                inside[1 + k] = inside[1 + k] + 0.5 * force_ref[k, x]
        else:
            received = below[5:10] if x == -1 else above[5 + 5 * (x - 4) : 10 + 5 * (x - 4)]
            inside, edge = received[:4], unpack_edges(received[4], rows)
            if x != 5:
                own_inside, own_edge = moment_sums(out_down if x == -1 else out_up, rows)
                inside = [u + v for u, v in zip(inside, own_inside)]
                edge = [u + v for u, v in zip(edge, own_edge)]
        for k in range(4):
            inside_ref[(k * 8 + n) * 8 : (k * 8 + n + 1) * 8, :] = inside[k]
        for k in range(3):
            edges[(k * 8 + n) * 8 : (k * 8 + n + 1) * 8, :] = edge[k]
    for k in range(4):
        inside_ref[(k * 8 + 7) * 8 : (k * 8 + 8) * 8, :] = jnp.ones(TILE, F32)
    for k in range(3):
        edges[(k * 8 + 7) * 8 : (k * 8 + 8) * 8, :] = jnp.zeros(TILE, F32)
    for k in range(3):
        up = edges[pl.ds(k * 64, 8, stride=8), :]
        down = edges[pl.ds(k * 64 + 7, 8, stride=8), :]
        leaving_ref[k] = up
        leaving_ref[3 + k] = down
        up_tiles[k] = up
        down_tiles[k] = down
    for n in range(5):
        t, r = (n, 0) if n < 4 else (3, 4)
        up_tiles[t, r : r + 4, :] = stepped_ref[pl.ds(UP_Y[n] * 32, 4, stride=8), :]
        down_tiles[t, r : r + 4, :] = stepped_ref[pl.ds(DOWN_Y[n] * 32 + 7, 4, stride=8), :]
    for k in range(4):
        up_tiles[4 + k] = inside_ref[pl.ds(k * 64 + 7, 8, stride=8), :]
        down_tiles[4 + k] = inside_ref[pl.ds(k * 64, 8, stride=8), :]
    inverse = 1.0 / inside_ref[pl.ds(1, 8, stride=8), :]
    for k in range(3):
        down_tiles[8 + k] = inside_ref[pl.ds((k + 1) * 64 + 1, 8, stride=8), :] * inverse
    for t in range(11):
        u = up_tiles[t] if t < 8 else down_tiles[t]
        d = down_tiles[t]
        first_ref[t] = choose(even_y, u, d)
        second_ref[t] = choose(even_y, d, u)


def crossing(tiles, n, x):
    return row_of(tiles[n], x) if n < 4 else row_of(tiles[3], 4 + x)


def finish_fluid(info_ref, stepped_ref, inside_ref, leaving_ref, first_y, second_y, out_ref, flow):
    even_y = info_ref[1] == 0.0
    rows = tile_rows()
    below = [choose(even_y, second_y[t], first_y[t]) for t in range(8)]
    above = [choose(even_y, first_y[t], second_y[t]) for t in range(11)]
    for q in range(19):
        for x in range(4):
            s = stepped_ref[(q * 4 + x) * 8 : (q * 4 + x + 1) * 8, :]
            if q in UP_Y:
                s = jnp.where(rows == 0, crossing(below, UP_Y.index(q), x), s)
            if q in DOWN_Y:
                s = jnp.where(rows == 7, crossing(above, DOWN_Y.index(q), x), s)
            out_ref[q, x] = s

    def arriving(tiles, members):
        crossed = list(tiles[:4]) + [pltpu.roll(tiles[3], 4, 0)]
        out = []
        for k, what in enumerate((None, 0, 2)):
            total = None
            for n, q in enumerate(members):
                weight = 1 if what is None else VELOCITIES[q][what]
                if weight:
                    term = crossed[n] if weight == 1 else -crossed[n]
                    total = term if total is None else total + term
            out.append(jnp.where(rows < 4, total, tiles[k]))
        return [out[0], out[1], None, out[2]]

    from_below = arriving(below, UP_Y)
    from_above = arriving(above, DOWN_Y)
    from_below[2] = from_below[0]
    from_above[2] = -from_above[0]
    for n in range(7):
        total = []
        for k in range(4):
            t = inside_ref[(k * 8 + n) * 8 : (k * 8 + n + 1) * 8, :]
            t = t + jnp.where(
                rows == 0,
                row_of(from_below[k], n),
                jnp.where(rows == 7, row_of(from_above[k], n), 0.0),
            )
            total.append(t)
        inverse = 1.0 / total[0]
        for a in range(3):
            flow[(a * 7 + n) * 8 : (a * 7 + n + 1) * 8, :] = total[1 + a] * inverse
    up = [leaving_ref[0], leaving_ref[1], leaving_ref[0], leaving_ref[2]]
    down = [leaving_ref[3], leaving_ref[4], -leaving_ref[3], leaving_ref[5]]
    rims = (
        (0, [above[4 + k] + up[k] for k in range(4)]),
        (2, [below[4 + k] + down[k] for k in range(4)]),
    )
    for n, total in rims:
        inverse = 1.0 / jnp.where(rows == 7, 1.0, total[0])
        for a in range(3):
            start = MAIN_ROWS + (a * 3 + n) * 8
            flow[start : start + 8, :] = jnp.where(rows == 7, 0.0, total[1 + a] * inverse)
    for a in range(3):
        start = MAIN_ROWS + (a * 3 + 1) * 8
        flow[start : start + 8, :] = above[8 + a]


def sample(offset, live, base, flow):
    kernels = stencil_kernels(offset)
    moved = [None] * 8
    zero = jnp.zeros((1, PAD), F32)
    for slot in range(SLOTS):
        table_x, table_y, table_rim, table_z = vertex_tables(base, kernels, slot)
        along = jnp.dot(flow[...], table_z, precision=HIGH, preferred_element_type=F32)
        for a in range(3):
            inner = None
            for n in range(7):
                tile = along[(a * 7 + n) * 8 : (a * 7 + n + 1) * 8, :]
                term = tile * row_of(table_x, n)
                inner = term if inner is None else inner + term
            total = inner * table_y
            outer = None
            for n in range(3):
                start = MAIN_ROWS + (a * 3 + n) * 8
                term = along[start : start + 8, :] * row_of(table_rim, n)
                outer = term if outer is None else outer + term
            total = total + outer * table_x
            moved[2 * a + slot] = jnp.sum(total, axis=0, keepdims=True)
    stacked = jnp.concatenate(moved[:6] + [zero, zero], axis=0)
    return offset + live * stacked


def next_kernel(
    info_ref, stepped_ref, inside_ref, leaving_ref, first_y, second_y,
    offset_ref, rest_ref, base_ref, incidence_ref,
    out_ref, offset_out, main_ref, rim_ref, first_ref, second_ref, flow, terms,
):
    finish_fluid(info_ref, stepped_ref, inside_ref, leaving_ref, first_y, second_y, out_ref, flow)
    base = base_ref[...]
    offset = sample(offset_ref[...], wide(info_ref[5]), base, flow)
    offset_out[...] = offset
    spread(offset, rest_ref[...], wide(info_ref[4]), base, incidence_ref, terms, main_ref, rim_ref)
    spread_messages(info_ref, main_ref, rim_ref, first_ref, second_ref)


def last_kernel(
    info_ref, stepped_ref, inside_ref, leaving_ref, first_y, second_y, offset_ref, base_ref,
    out_ref, offset_out, flow,
):
    finish_fluid(info_ref, stepped_ref, inside_ref, leaving_ref, first_y, second_y, out_ref, flow)
    offset = sample(offset_ref[...], wide(info_ref[5]), base_ref[...], flow)
    for a in range(3):
        offset_out[a] = offset[2 * a : 2 * a + 2]


INTERPRET = False


def call(kernel, outs, scratch, *operands, name):
    return pl.pallas_call(
        kernel,
        out_shape=[jax.ShapeDtypeStruct(shape, dtype) for shape, dtype in outs],
        in_specs=[pl.BlockSpec(memory_space=pltpu.VMEM)] * len(operands),
        out_specs=[pl.BlockSpec(memory_space=pltpu.VMEM)] * len(outs),
        scratch_shapes=[pltpu.VMEM(shape, dtype) for shape, dtype in scratch],
        compiler_params=pltpu.CompilerParams(vmem_limit_bytes=24 * 1024 * 1024),
        interpret=INTERPRET,
        name=name,
    )(*operands)


def partner(index, kind, size):
    return (index + 1) % size if (index + kind) % 2 == 0 else (index - 1) % size


def exchange(first, second, axis):
    size = lax.axis_size(axis)
    out = [None, None]
    for kind, message in ((1, second), (0, first)):
        pairs = [(i, partner(i, kind, size)) for i in range(size)]
        out[kind] = lax.ppermute(message, axis, pairs)
    return out


SPREAD_OUT = [
    ((3, 7, 8, CZ), F32),
    ((3, 3, 8, CZ), F32),
    ((3, 3, 8, CZ), F32),
    ((3, 3, 8, CZ), F32),
]
STEPPED = ((19, 4, 8, CZ), F32)


def local(populations, solid, base_cell, offset, rest_displacement, stiffness, occupied, triangles):
    place_x = lax.axis_index("gx")
    place_y = lax.axis_index("gy")
    held = occupied.reshape(SLOTS).astype(F32)
    spring = stiffness.reshape(SLOTS) * held
    lead = lax.broadcasted_iota(jnp.int32, (6, 8, CZ), 0)
    even_row = lax.broadcasted_iota(jnp.int32, (6, 8, CZ), 1) % 2 == 0
    info = jnp.where(even_row, held[0], held[1])
    info = jnp.where(lead == 4, jnp.where(even_row, spring[0], spring[1]), info)
    numbers = (place_x % 2, place_y % 2, place_x * CX, place_y * CY)
    for n, number in enumerate(numbers):
        info = jnp.where(lead == n, number.astype(F32), info)
    stored = (3, SLOTS, PAD)
    rows = (8, PAD)
    terms = ((TABLE_ROWS, PAD), F32)
    flow = ((TABLE_ROWS, CZ), F32)
    corners = triangles.T
    (incidence,) = call(
        incidence_kernel, [((PAD, corners.shape[1]), jnp.bfloat16)], [], corners, name="incidence"
    )
    main, rim, first, second, where, rest, base, populations, solid = call(
        spread_kernel,
        SPREAD_OUT
        + [(rows, F32), (rows, F32), (rows, jnp.int32), STEPPED, (solid.shape, jnp.int32)],
        [terms],
        info, offset.reshape(stored), rest_displacement.reshape(stored), base_cell.reshape(stored),
        populations, solid, incidence, name="spread",
    )
    for substep in range(SUBSTEPS):
        first_x, second_x = exchange(first, second, "gx")
        corner = call(
            force_corner_kernel, [((3, 8, CZ), F32)] * 2, [], info, rim, first_x, second_x,
            name="force_corner",
        )
        first_y, second_y = exchange(*corner, "gy")
        stepped, force, first, second = call(
            collide_kernel,
            [STEPPED, ((3, 4, 8, CZ), F32), ((15, 8, CZ), F32), ((15, 8, CZ), F32)],
            [],
            info, populations, solid, main, first_x, second_x, first_y, second_y,
            name="collide",
        )
        first_x, second_x = exchange(first, second, "gx")
        stepped, inside, leaving, first, second = call(
            flow_corner_kernel,
            [
                ((19 * 4 * 8, CZ), F32), ((4 * 8 * 8, CZ), F32), ((6, 8, CZ), F32),
                ((11, 8, CZ), F32), ((11, 8, CZ), F32),
            ],
            [((3 * 8 * 8, CZ), F32), ((8, 8, CZ), F32), ((11, 8, CZ), F32)],
            info, stepped, force, first_x, second_x,
            name="flow_corner",
        )
        first_y, second_y = exchange(first, second, "gy")
        fluid = (info, stepped, inside, leaving, first_y, second_y)
        if substep < SUBSTEPS - 1:
            populations, where, main, rim, first, second = call(
                next_kernel, [STEPPED, (rows, F32)] + SPREAD_OUT, [flow, terms],
                *fluid, where, rest, base, incidence, name="next",
            )
        else:
            populations, where = call(
                last_kernel, [STEPPED, (stored, F32)], [flow], *fluid, where, base, name="last"
            )
    return populations, where.reshape(offset.shape)


def solution(mesh):
    in_specs = (
        P(None, "gx", "gy", None),
        P("gx", "gy", None),
        P(None, "gx", "gy", None, None),
        P(None, "gx", "gy", None, None),
        P(None, "gx", "gy", None, None),
        P("gx", "gy", None),
        P("gx", "gy", None),
        P(),
    )
    out_specs = (P(None, "gx", "gy", None), P(None, "gx", "gy", None, None))
    return jax.shard_map(local, mesh=mesh, in_specs=in_specs, out_specs=out_specs, check_vma=False)
```

```python
import functools
import math

import jax
import jax.numpy as jnp
from jax import lax
from jax.experimental import pallas as pl
from jax.experimental.pallas import tpu as pltpu
from jax.sharding import PartitionSpec as P


SUBSTEPS = 3

VELOCITIES = [
    [0, 0, 0],
    [1, 0, 0],
    [-1, 0, 0],
    [0, 1, 0],
    [0, -1, 0],
    [0, 0, 1],
    [0, 0, -1],
    [1, 1, 0],
    [-1, -1, 0],
    [1, -1, 0],
    [-1, 1, 0],
    [1, 0, 1],
    [-1, 0, -1],
    [1, 0, -1],
    [-1, 0, 1],
    [0, 1, 1],
    [0, -1, -1],
    [0, 1, -1],
    [0, -1, 1],
]
OPPOSITE = [0, 2, 1, 4, 3, 6, 5, 8, 7, 10, 9, 12, 11, 14, 13, 16, 15, 18, 17]
LATTICE_WEIGHTS = [1.0 / 3.0] + [1.0 / 18.0] * 6 + [1.0 / 36.0] * 12
RELAX = 0.8
CX, CY, CZ = 4, 8, 128
SLOTS, PAD = 2, 768
UP_X = [q for q in range(19) if VELOCITIES[q][0] == 1]
DOWN_X = [q for q in range(19) if VELOCITIES[q][0] == -1]
UP_Y = [q for q in range(19) if VELOCITIES[q][1] == 1]
DOWN_Y = [q for q in range(19) if VELOCITIES[q][1] == -1]
X_ORDER = [0, 1, 2, 3, 4, 5, -1]
MAIN_ROWS = 3 * 7 * 8
RIM_ROWS = 3 * 3 * 8
TABLE_ROWS = MAIN_ROWS + RIM_ROWS
F32 = jnp.float32
HIGH = lax.Precision.HIGH
TILE = (8, CZ)


def tile_rows():
    return lax.broadcasted_iota(jnp.int32, TILE, 0)


def wide(row):
    return jnp.concatenate([row] * (PAD // CZ), axis=1)


def six_rows(ref):
    return jnp.concatenate([ref[0], ref[1], ref[2], jnp.zeros((2, PAD), ref.dtype)], axis=0)


def own_base(info_ref, base_ref):
    base = six_rows(base_ref)
    rows = lax.broadcasted_iota(jnp.int32, TILE, 0)
    start = jnp.where(rows < 2, info_ref[2], jnp.where(rows < 4, info_ref[3], 0.0))
    return base - wide(start.astype(jnp.int32))


def row_of(tile, r):
    return jnp.broadcast_to(tile[r : r + 1, :], (8, tile.shape[1]))


def choose(first, a, b):
    return jnp.where(first, a, b)


def stencil_kernels(offset):
    angle = offset * (math.pi / 2.0)
    c, s = jnp.cos(angle), jnp.sin(angle)
    return [(1.0 - s) * 0.25, (1.0 + c) * 0.25, (1.0 + s) * 0.25, (1.0 - c) * 0.25]


def pick(distance, kernels, r):
    out = jnp.zeros(distance.shape, F32)
    for n in range(4):
        out = jnp.where(distance == n, kernels[n][r : r + 1, :], out)
    return out


def vertex_tables(base, kernels, slot):
    rows = lax.broadcasted_iota(jnp.int32, (8, PAD), 0)
    x_value = jnp.where(rows < 6, rows, jnp.where(rows == 6, -1, 100))
    y_rim = jnp.where(rows < 2, rows + 8, jnp.where(rows == 2, -1, 100))
    base_x, base_y, base_z = [base[2 * a + slot : 2 * a + slot + 1, :] for a in range(3)]
    table_x = pick(x_value - base_x + 1, kernels, slot)
    table_y = pick(rows - base_y + 1, kernels, 2 + slot)
    table_rim = pick(y_rim - base_y + 1, kernels, 2 + slot)
    depth = lax.broadcasted_iota(jnp.int32, (CZ, PAD), 0)
    table_z = pick(jnp.bitwise_and(depth - base_z + 1, CZ - 1), kernels, 4 + slot)
    return table_x, table_y, table_rim, table_z


def halves(rows):
    high = rows.astype(jnp.bfloat16)
    return jnp.concatenate([high, (rows - high.astype(F32)).astype(jnp.bfloat16)], axis=0)


def vertex_force(offset, rest, scale, incidence):
    strain = offset - rest
    summed = jnp.dot(halves(strain), incidence[...], preferred_element_type=F32)
    summed = summed[:8] + summed[8:]
    rows = lax.broadcasted_iota(jnp.int32, summed.shape, 0)
    summed = jnp.where(rows == 6, 1.0, summed)
    pulled = lax.dot_general(
        halves(summed), incidence[...], (((1,), (1,)), ((), ())), preferred_element_type=F32
    )
    pulled = pulled[:8] + pulled[8:]
    return scale * (pulled - 3.0 * pulled[6:7] * strain)


def spread(offset, rest, scale, base, incidence, terms, main_ref, rim_ref):
    force = vertex_force(offset, rest, scale, incidence)
    kernels = stencil_kernels(offset)
    grid = None
    for slot in range(SLOTS):
        table_x, table_y, table_rim, table_z = vertex_tables(base, kernels, slot)
        for a in range(3):
            pushed = force[2 * a + slot : 2 * a + slot + 1, :]
            along_x = table_x * pushed
            for n in range(7):
                terms[(a * 7 + n) * 8 : (a * 7 + n + 1) * 8, :] = row_of(along_x, n) * table_y
            along_y = table_rim * pushed
            for n in range(3):
                start = MAIN_ROWS + (a * 3 + n) * 8
                terms[start : start + 8, :] = row_of(along_y, n) * table_x
        part = lax.dot_general(
            terms[...], table_z, (((1,), (1,)), ((), ())), precision=HIGH, preferred_element_type=F32
        )
        grid = part if grid is None else grid + part
    main_ref[...] = grid[:MAIN_ROWS].reshape(3, 7, 8, CZ)
    rim_ref[...] = grid[MAIN_ROWS:].reshape(3, 3, 8, CZ)


def spread_messages(info_ref, main_ref, rim_ref, first_ref, second_ref):
    even = info_ref[0] == 0.0
    zero = jnp.zeros((2, CZ), F32)
    for a in range(3):
        up_rows, down_rows = [], []
        for n in range(3):
            rim = rim_ref[a, n]
            up_rows.append(rim[4:6])
            down_rows.append(rim[6:8])
        ups = [main_ref[a, 4], main_ref[a, 5], jnp.concatenate(up_rows + [zero], axis=0)]
        downs = [main_ref[a, 6], main_ref[a, 6], jnp.concatenate(down_rows + [zero], axis=0)]
        for t in range(3):
            first_ref[a, t] = choose(even, ups[t], downs[t])
            second_ref[a, t] = choose(even, downs[t], ups[t])


def incidence_kernel(triangles_ref, incidence_ref):
    vertex = lax.broadcasted_iota(jnp.int32, incidence_ref.shape, 0)
    corners = [triangles_ref[corner : corner + 1, :] == vertex for corner in range(3)]
    hit = corners[0] | corners[1] | corners[2]
    incidence_ref[...] = jnp.where(hit, 1.0, 0.0).astype(jnp.bfloat16)


def spread_kernel(
    info_ref, offset_in, rest_in, base_in, populations_in, solid_in, incidence_ref,
    main_ref, rim_ref, first_ref, second_ref,
    offset_ref, rest_ref, base_ref, populations_ref, solid_ref, terms,
):
    offset_ref[...] = six_rows(offset_in)
    rest_ref[...] = six_rows(rest_in)
    base_ref[...] = own_base(info_ref, base_in)
    populations_ref[...] = populations_in[...]
    solid_ref[...] = solid_in[...]
    spread(
        offset_ref[...], rest_ref[...], wide(info_ref[4]), base_ref[...],
        incidence_ref, terms, main_ref, rim_ref,
    )
    spread_messages(info_ref, main_ref, rim_ref, first_ref, second_ref)


def force_corner_kernel(info_ref, rim_ref, first_in, second_in, first_ref, second_ref):
    even_x = info_ref[0] == 0.0
    even_y = info_ref[1] == 0.0
    rows = tile_rows()
    for a in range(3):
        above = choose(even_x, first_in[a, 2], second_in[a, 2])
        below = choose(even_x, second_in[a, 2], first_in[a, 2])
        whole = []
        for n in range(3):
            from_below = below[2 * n : 2 * n + 2]
            from_above = above[2 * n : 2 * n + 1]
            part = rim_ref[a, n][:4]
            whole.append(
                jnp.concatenate([part[0:2] + from_below, part[2:3], part[3:4] + from_above], axis=0)
            )
        up = jnp.concatenate([whole[0], whole[1]], axis=0)
        down = jnp.concatenate([whole[2], whole[2]], axis=0)
        first_ref[a] = choose(even_y, up, down)
        second_ref[a] = choose(even_y, down, up)


def moment_sums(members, rows):
    groups = {}
    for step in (0, 1, -1):
        of_step = [(q, t) for q, t in members if VELOCITIES[q][1] == step]
        sums = []
        for what in (None, 0, 2):
            total = None
            for q, t in of_step:
                weight = 1 if what is None else VELOCITIES[q][what]
                if weight == 0:
                    continue
                term = t if weight == 1 else -t
                total = term if total is None else total + term
            sums.append(jnp.zeros(TILE, F32) if total is None else total)
        groups[step] = sums
    up = [jnp.where(rows == 0, 0.0, t) for t in groups[1]]
    down = [jnp.where(rows == 7, 0.0, t) for t in groups[-1]]
    density, along_x, along_z = [groups[0][k] + up[k] + down[k] for k in range(3)]
    inside = [density, along_x, up[0] - down[0], along_z]
    edge = [
        jnp.where(rows == 0, groups[1][k], jnp.where(rows == 7, groups[-1][k], 0.0)) for k in range(3)
    ]
    return inside, edge


def pack_edges(edge):
    return edge[0] + pltpu.roll(edge[1], 2, 0) + pltpu.roll(edge[2], 4, 0)


def unpack_edges(packed, rows):
    keep = (rows == 0) | (rows == 7)
    tiles = [packed, pltpu.roll(packed, 6, 0), pltpu.roll(packed, 4, 0)]
    return [jnp.where(keep, t, 0.0) for t in tiles]


def collide_kernel(
    info_ref, populations_ref, solid_ref, main_ref, first_x, second_x, first_y, second_y,
    stepped_ref, force_ref, first_ref, second_ref,
):
    even_x = info_ref[0] == 0.0
    even_y = info_ref[1] == 0.0
    rows = tile_rows()
    for x in range(4):
        force = []
        for a in range(3):
            f = main_ref[a, x]
            if x < 2:
                f = f + choose(even_x, second_x[a, x], first_x[a, x])
            if x == 3:
                f = f + choose(even_x, first_x[a, 0], second_x[a, 0])
            below = choose(even_y, second_y[a], first_y[a])
            above = choose(even_y, first_y[a], second_y[a])
            f = f + jnp.where(
                rows == 0,
                row_of(below, x),
                jnp.where(rows == 1, row_of(below, 4 + x), jnp.where(rows == 7, row_of(above, x), 0.0)),
            )
            force_ref[a, x] = f
            force.append(f)
        current = [populations_ref[q, x] for q in range(19)]
        density = functools.reduce(lambda u, v: u + v, current)
        velocity = []
        for a in range(3):
            moving = force[a] * 0.5
            for q in range(19):
                if VELOCITIES[q][a] == 1:
                    moving = moving + current[q]
                elif VELOCITIES[q][a] == -1:
                    moving = moving - current[q]
            velocity.append(moving)
        inverse = 1.0 / density
        velocity = [m * inverse for m in velocity]
        squared = velocity[0] * velocity[0] + velocity[1] * velocity[1] + velocity[2] * velocity[2]
        working = velocity[0] * force[0] + velocity[1] * force[1] + velocity[2] * force[2]
        walled = solid_ref[x] != 0
        common = 1.0 - 1.5 * squared
        factor = 1.0 - 0.5 / RELAX
        for q in range(19):
            vector = VELOCITIES[q]
            w = LATTICE_WEIGHTS[q]
            if q == 0:
                equilibrium = w * density * common
                source = (-3.0 * factor * w) * working
            else:
                along, pushed = None, None
                for a in range(3):
                    if vector[a] == 0:
                        continue
                    u = velocity[a] if vector[a] == 1 else -velocity[a]
                    f = force[a] if vector[a] == 1 else -force[a]
                    along = u if along is None else along + u
                    pushed = f if pushed is None else pushed + f
                equilibrium = w * density * (common + along * (3.0 + 4.5 * along))
                source = (factor * w) * (3.0 * (pushed - working) + 9.0 * along * pushed)
            updated = current[q] - (current[q] - equilibrium) / RELAX + source
            relaxed = jnp.where(walled, current[OPPOSITE[q]], updated)
            if vector[2] != 0:
                relaxed = pltpu.roll(relaxed, vector[2] % CZ, 1)
            if vector[1] != 0:
                relaxed = pltpu.roll(relaxed, vector[1] % 8, 0)
            stepped_ref[q, (x + vector[0]) % 4] = relaxed
    messages = []
    for crossing, lines in ((UP_X, (3,)), (DOWN_X, (0, 1))):
        slot = 0 if crossing is UP_X else 3
        tiles = [stepped_ref[q, slot] for q in crossing]
        for x in lines:
            members = [
                (q, stepped_ref[q, x])
                for q in range(19)
                if not (x == 0 and VELOCITIES[q][0] == 1) and not (x == 3 and VELOCITIES[q][0] == -1)
            ]
            inside, edge = moment_sums(members, rows)
            for k in range(3):
                inside[1 + k] = inside[1 + k] + 0.5 * force_ref[k, x]
            tiles += inside + [pack_edges(edge)]
        messages.append(tiles)
    up, down = messages
    for t in range(15):
        u = up[t] if t < len(up) else down[t]
        first_ref[t] = choose(even_x, u, down[t])
        second_ref[t] = choose(even_x, down[t], u)


def flow_corner_kernel(
    info_ref, stepped_in, force_ref, first_x, second_x,
    stepped_ref, inside_ref, leaving_ref, first_ref, second_ref, edges, up_tiles, down_tiles,
):
    even_x = info_ref[0] == 0.0
    even_y = info_ref[1] == 0.0
    rows = tile_rows()
    below = [choose(even_x, second_x[t], first_x[t]) for t in range(10)]
    above = [choose(even_x, first_x[t], second_x[t]) for t in range(15)]
    out_up = [(q, stepped_in[q, 0]) for q in UP_X]
    out_down = [(q, stepped_in[q, 3]) for q in DOWN_X]
    for q in range(19):
        for x in range(4):
            s = stepped_in[q, x]
            if q in UP_X and x == 0:
                s = below[UP_X.index(q)]
            if q in DOWN_X and x == 3:
                s = above[DOWN_X.index(q)]
            stepped_ref[(q * 4 + x) * 8 : (q * 4 + x + 1) * 8, :] = s
    for n, x in enumerate(X_ORDER):
        if 0 <= x < 4:
            members = [(q, stepped_ref[(q * 4 + x) * 8 : (q * 4 + x + 1) * 8, :]) for q in range(19)]
            inside, edge = moment_sums(members, rows)
            for k in range(3):
                inside[1 + k] = inside[1 + k] + 0.5 * force_ref[k, x]
        else:
            received = below[5:10] if x == -1 else above[5 + 5 * (x - 4) : 10 + 5 * (x - 4)]
            inside, edge = received[:4], unpack_edges(received[4], rows)
            if x != 5:
                own_inside, own_edge = moment_sums(out_down if x == -1 else out_up, rows)
                inside = [u + v for u, v in zip(inside, own_inside)]
                edge = [u + v for u, v in zip(edge, own_edge)]
        for k in range(4):
            inside_ref[(k * 8 + n) * 8 : (k * 8 + n + 1) * 8, :] = inside[k]
        for k in range(3):
            edges[(k * 8 + n) * 8 : (k * 8 + n + 1) * 8, :] = edge[k]
    for k in range(4):
        inside_ref[(k * 8 + 7) * 8 : (k * 8 + 8) * 8, :] = jnp.ones(TILE, F32)
    for k in range(3):
        edges[(k * 8 + 7) * 8 : (k * 8 + 8) * 8, :] = jnp.zeros(TILE, F32)
    for k in range(3):
        up = edges[pl.ds(k * 64, 8, stride=8), :]
        down = edges[pl.ds(k * 64 + 7, 8, stride=8), :]
        leaving_ref[k] = up
        leaving_ref[3 + k] = down
        up_tiles[k] = up
        down_tiles[k] = down
    for n in range(5):
        t, r = (n, 0) if n < 4 else (3, 4)
        up_tiles[t, r : r + 4, :] = stepped_ref[pl.ds(UP_Y[n] * 32, 4, stride=8), :]
        down_tiles[t, r : r + 4, :] = stepped_ref[pl.ds(DOWN_Y[n] * 32 + 7, 4, stride=8), :]
    for k in range(4):
        up_tiles[4 + k] = inside_ref[pl.ds(k * 64 + 7, 8, stride=8), :]
        down_tiles[4 + k] = inside_ref[pl.ds(k * 64, 8, stride=8), :]
    inverse = 1.0 / inside_ref[pl.ds(1, 8, stride=8), :]
    for k in range(3):
        down_tiles[8 + k] = inside_ref[pl.ds((k + 1) * 64 + 1, 8, stride=8), :] * inverse
    for t in range(11):
        u = up_tiles[t] if t < 8 else down_tiles[t]
        d = down_tiles[t]
        first_ref[t] = choose(even_y, u, d)
        second_ref[t] = choose(even_y, d, u)


def crossing(tiles, n, x):
    return row_of(tiles[n], x) if n < 4 else row_of(tiles[3], 4 + x)


def finish_fluid(info_ref, stepped_ref, inside_ref, leaving_ref, first_y, second_y, out_ref, flow):
    even_y = info_ref[1] == 0.0
    rows = tile_rows()
    below = [choose(even_y, second_y[t], first_y[t]) for t in range(8)]
    above = [choose(even_y, first_y[t], second_y[t]) for t in range(11)]
    for q in range(19):
        for x in range(4):
            s = stepped_ref[(q * 4 + x) * 8 : (q * 4 + x + 1) * 8, :]
            if q in UP_Y:
                s = jnp.where(rows == 0, crossing(below, UP_Y.index(q), x), s)
            if q in DOWN_Y:
                s = jnp.where(rows == 7, crossing(above, DOWN_Y.index(q), x), s)
            out_ref[q, x] = s

    def arriving(tiles, members):
        crossed = list(tiles[:4]) + [pltpu.roll(tiles[3], 4, 0)]
        out = []
        for k, what in enumerate((None, 0, 2)):
            total = None
            for n, q in enumerate(members):
                weight = 1 if what is None else VELOCITIES[q][what]
                if weight:
                    term = crossed[n] if weight == 1 else -crossed[n]
                    total = term if total is None else total + term
            out.append(jnp.where(rows < 4, total, tiles[k]))
        return [out[0], out[1], None, out[2]]

    from_below = arriving(below, UP_Y)
    from_above = arriving(above, DOWN_Y)
    from_below[2] = from_below[0]
    from_above[2] = -from_above[0]
    for n in range(7):
        total = []
        for k in range(4):
            t = inside_ref[(k * 8 + n) * 8 : (k * 8 + n + 1) * 8, :]
            t = t + jnp.where(
                rows == 0,
                row_of(from_below[k], n),
                jnp.where(rows == 7, row_of(from_above[k], n), 0.0),
            )
            total.append(t)
        inverse = 1.0 / total[0]
        for a in range(3):
            flow[(a * 7 + n) * 8 : (a * 7 + n + 1) * 8, :] = total[1 + a] * inverse
    up = [leaving_ref[0], leaving_ref[1], leaving_ref[0], leaving_ref[2]]
    down = [leaving_ref[3], leaving_ref[4], -leaving_ref[3], leaving_ref[5]]
    rims = (
        (0, [above[4 + k] + up[k] for k in range(4)]),
        (2, [below[4 + k] + down[k] for k in range(4)]),
    )
    for n, total in rims:
        inverse = 1.0 / jnp.where(rows == 7, 1.0, total[0])
        for a in range(3):
            start = MAIN_ROWS + (a * 3 + n) * 8
            flow[start : start + 8, :] = jnp.where(rows == 7, 0.0, total[1 + a] * inverse)
    for a in range(3):
        start = MAIN_ROWS + (a * 3 + 1) * 8
        flow[start : start + 8, :] = above[8 + a]


def sample(offset, live, base, flow):
    kernels = stencil_kernels(offset)
    moved = [None] * 8
    zero = jnp.zeros((1, PAD), F32)
    for slot in range(SLOTS):
        table_x, table_y, table_rim, table_z = vertex_tables(base, kernels, slot)
        along = jnp.dot(flow[...], table_z, precision=HIGH, preferred_element_type=F32)
        for a in range(3):
            inner = None
            for n in range(7):
                tile = along[(a * 7 + n) * 8 : (a * 7 + n + 1) * 8, :]
                term = tile * row_of(table_x, n)
                inner = term if inner is None else inner + term
            total = inner * table_y
            outer = None
            for n in range(3):
                start = MAIN_ROWS + (a * 3 + n) * 8
                term = along[start : start + 8, :] * row_of(table_rim, n)
                outer = term if outer is None else outer + term
            total = total + outer * table_x
            moved[2 * a + slot] = jnp.sum(total, axis=0, keepdims=True)
    stacked = jnp.concatenate(moved[:6] + [zero, zero], axis=0)
    return offset + live * stacked


def next_kernel(
    info_ref, stepped_ref, inside_ref, leaving_ref, first_y, second_y,
    offset_ref, rest_ref, base_ref, incidence_ref,
    out_ref, offset_out, main_ref, rim_ref, first_ref, second_ref, flow, terms,
):
    finish_fluid(info_ref, stepped_ref, inside_ref, leaving_ref, first_y, second_y, out_ref, flow)
    base = base_ref[...]
    offset = sample(offset_ref[...], wide(info_ref[5]), base, flow)
    offset_out[...] = offset
    spread(offset, rest_ref[...], wide(info_ref[4]), base, incidence_ref, terms, main_ref, rim_ref)
    spread_messages(info_ref, main_ref, rim_ref, first_ref, second_ref)


def last_kernel(
    info_ref, stepped_ref, inside_ref, leaving_ref, first_y, second_y, offset_ref, base_ref,
    out_ref, offset_out, flow,
):
    finish_fluid(info_ref, stepped_ref, inside_ref, leaving_ref, first_y, second_y, out_ref, flow)
    offset = sample(offset_ref[...], wide(info_ref[5]), base_ref[...], flow)
    for a in range(3):
        offset_out[a] = offset[2 * a : 2 * a + 2]


INTERPRET = False


def call(kernel, outs, scratch, *operands):
    return pl.pallas_call(
        kernel,
        out_shape=[jax.ShapeDtypeStruct(shape, dtype) for shape, dtype in outs],
        in_specs=[pl.BlockSpec(memory_space=pltpu.VMEM)] * len(operands),
        out_specs=[pl.BlockSpec(memory_space=pltpu.VMEM)] * len(outs),
        scratch_shapes=[pltpu.VMEM(shape, dtype) for shape, dtype in scratch],
        compiler_params=pltpu.CompilerParams(vmem_limit_bytes=24 * 1024 * 1024),
        interpret=INTERPRET,
    )(*operands)


def partner(index, kind, size):
    return (index + 1) % size if (index + kind) % 2 == 0 else (index - 1) % size


def exchange(first, second, axis):
    size = lax.axis_size(axis)
    out = [None, None]
    for kind, message in ((1, second), (0, first)):
        pairs = [(i, partner(i, kind, size)) for i in range(size)]
        out[kind] = lax.ppermute(message, axis, pairs)
    return out


SPREAD_OUT = [
    ((3, 7, 8, CZ), F32),
    ((3, 3, 8, CZ), F32),
    ((3, 3, 8, CZ), F32),
    ((3, 3, 8, CZ), F32),
]
STEPPED = ((19, 4, 8, CZ), F32)


def steps(populations, solid, base_cell, offset, rest_displacement, stiffness, occupied, triangles):
    place_x = lax.axis_index("gx")
    place_y = lax.axis_index("gy")
    held = occupied.reshape(SLOTS).astype(F32)
    spring = stiffness.reshape(SLOTS) * held
    lead = lax.broadcasted_iota(jnp.int32, (6, 8, CZ), 0)
    even_row = lax.broadcasted_iota(jnp.int32, (6, 8, CZ), 1) % 2 == 0
    info = jnp.where(even_row, held[0], held[1])
    info = jnp.where(lead == 4, jnp.where(even_row, spring[0], spring[1]), info)
    numbers = (place_x % 2, place_y % 2, place_x * CX, place_y * CY)
    for n, number in enumerate(numbers):
        info = jnp.where(lead == n, number.astype(F32), info)
    stored = (3, SLOTS, PAD)
    rows = (8, PAD)
    terms = ((TABLE_ROWS, PAD), F32)
    flow = ((TABLE_ROWS, CZ), F32)
    corners = triangles.T
    (incidence,) = call(incidence_kernel, [((PAD, corners.shape[1]), jnp.bfloat16)], [], corners)
    main, rim, first, second, where, rest, base, populations, solid = call(
        spread_kernel,
        SPREAD_OUT
        + [(rows, F32), (rows, F32), (rows, jnp.int32), STEPPED, (solid.shape, jnp.int32)],
        [terms],
        info, offset.reshape(stored), rest_displacement.reshape(stored), base_cell.reshape(stored),
        populations, solid, incidence,
    )
    for substep in range(SUBSTEPS):
        first_x, second_x = exchange(first, second, "gx")
        corner = call(
            force_corner_kernel, [((3, 8, CZ), F32)] * 2, [], info, rim, first_x, second_x,
        )
        first_y, second_y = exchange(*corner, "gy")
        stepped, force, first, second = call(
            collide_kernel,
            [STEPPED, ((3, 4, 8, CZ), F32), ((15, 8, CZ), F32), ((15, 8, CZ), F32)],
            [],
            info, populations, solid, main, first_x, second_x, first_y, second_y,
        )
        first_x, second_x = exchange(first, second, "gx")
        stepped, inside, leaving, first, second = call(
            flow_corner_kernel,
            [
                ((19 * 4 * 8, CZ), F32), ((4 * 8 * 8, CZ), F32), ((6, 8, CZ), F32),
                ((11, 8, CZ), F32), ((11, 8, CZ), F32),
            ],
            [((3 * 8 * 8, CZ), F32), ((8, 8, CZ), F32), ((11, 8, CZ), F32)],
            info, stepped, force, first_x, second_x,
        )
        first_y, second_y = exchange(first, second, "gy")
        fluid = (info, stepped, inside, leaving, first_y, second_y)
        if substep < SUBSTEPS - 1:
            populations, where, main, rim, first, second = call(
                next_kernel, [STEPPED, (rows, F32)] + SPREAD_OUT, [flow, terms],
                *fluid, where, rest, base, incidence,
            )
        else:
            populations, where = call(
                last_kernel, [STEPPED, (stored, F32)], [flow], *fluid, where, base
            )
    return populations, where.reshape(offset.shape)


def solution(mesh):
    in_specs = (
        P(None, "gx", "gy", None),
        P("gx", "gy", None),
        P(None, "gx", "gy", None, None),
        P(None, "gx", "gy", None, None),
        P(None, "gx", "gy", None, None),
        P("gx", "gy", None),
        P("gx", "gy", None),
        P(),
    )
    out_specs = (P(None, "gx", "gy", None), P(None, "gx", "gy", None, None))
    return jax.shard_map(steps, mesh=mesh, in_specs=in_specs, out_specs=out_specs, check_vma=False)
```

```python
import functools
import math

import jax
import jax.numpy as jnp
from jax import lax
from jax.experimental import pallas as pl
from jax.experimental.pallas import tpu as pltpu
from jax.sharding import PartitionSpec as P


SUBSTEPS = 3

VELOCITIES = [
    [0, 0, 0],
    [1, 0, 0],
    [-1, 0, 0],
    [0, 1, 0],
    [0, -1, 0],
    [0, 0, 1],
    [0, 0, -1],
    [1, 1, 0],
    [-1, -1, 0],
    [1, -1, 0],
    [-1, 1, 0],
    [1, 0, 1],
    [-1, 0, -1],
    [1, 0, -1],
    [-1, 0, 1],
    [0, 1, 1],
    [0, -1, -1],
    [0, 1, -1],
    [0, -1, 1],
]
OPPOSITE = [0, 2, 1, 4, 3, 6, 5, 8, 7, 10, 9, 12, 11, 14, 13, 16, 15, 18, 17]
LATTICE_WEIGHTS = [1.0 / 3.0] + [1.0 / 18.0] * 6 + [1.0 / 36.0] * 12
RELAX = 0.8
CX, CY, CZ = 4, 8, 128
SLOTS, PAD = 2, 768
UP_X = [q for q in range(19) if VELOCITIES[q][0] == 1]
DOWN_X = [q for q in range(19) if VELOCITIES[q][0] == -1]
UP_Y = [q for q in range(19) if VELOCITIES[q][1] == 1]
DOWN_Y = [q for q in range(19) if VELOCITIES[q][1] == -1]
X_ORDER = [0, 1, 2, 3, 4, 5, -1]
MAIN_ROWS = 3 * 7 * 8
RIM_ROWS = 3 * 3 * 8
TABLE_ROWS = MAIN_ROWS + RIM_ROWS
F32 = jnp.float32
TILE = (8, CZ)


def tile_rows():
    return lax.broadcasted_iota(jnp.int32, TILE, 0)


def wide(row):
    return jnp.concatenate([row] * (PAD // CZ), axis=1)


def six_rows(ref):
    return jnp.concatenate([ref[0], ref[1], ref[2], jnp.zeros((2, PAD), ref.dtype)], axis=0)


def own_base(info_ref, base_ref):
    base = six_rows(base_ref)
    rows = lax.broadcasted_iota(jnp.int32, TILE, 0)
    start = jnp.where(rows < 2, info_ref[2], jnp.where(rows < 4, info_ref[3], 0.0))
    return base - wide(start.astype(jnp.int32))


def row_of(tile, r):
    return jnp.broadcast_to(tile[r : r + 1, :], (8, tile.shape[1]))


def choose(first, a, b):
    return jnp.where(first, a, b)


def stencil_kernels(offset):
    angle = offset * (math.pi / 2.0)
    c, s = jnp.cos(angle), jnp.sin(angle)
    return [(1.0 - s) * 0.25, (1.0 + c) * 0.25, (1.0 + s) * 0.25, (1.0 - c) * 0.25]


def pick(distance, kernels, r):
    out = jnp.zeros(distance.shape, F32)
    for n in range(4):
        out = jnp.where(distance == n, kernels[n][r : r + 1, :], out)
    return out


def vertex_tables(base, kernels, slot):
    rows = lax.broadcasted_iota(jnp.int32, (8, PAD), 0)
    x_value = jnp.where(rows < 6, rows, jnp.where(rows == 6, -1, 100))
    y_rim = jnp.where(rows < 2, rows + 8, jnp.where(rows == 2, -1, 100))
    base_x, base_y, base_z = [base[2 * a + slot : 2 * a + slot + 1, :] for a in range(3)]
    table_x = pick(x_value - base_x + 1, kernels, slot)
    table_y = pick(rows - base_y + 1, kernels, 2 + slot)
    table_rim = pick(y_rim - base_y + 1, kernels, 2 + slot)
    depth = lax.broadcasted_iota(jnp.int32, (CZ, PAD), 0)
    table_z = pick(jnp.bitwise_and(depth - base_z + 1, CZ - 1), kernels, 4 + slot)
    return table_x, table_y, table_rim, table_z


def halves(rows):
    high = rows.astype(jnp.bfloat16)
    return jnp.concatenate([high, (rows - high.astype(F32)).astype(jnp.bfloat16)], axis=0)


def vertex_force(offset, rest, scale, incidence):
    strain = offset - rest
    summed = jnp.dot(halves(strain), incidence[...], preferred_element_type=F32)
    summed = summed[:8] + summed[8:]
    rows = lax.broadcasted_iota(jnp.int32, summed.shape, 0)
    summed = jnp.where(rows == 6, 1.0, summed)
    pulled = lax.dot_general(
        halves(summed), incidence[...], (((1,), (1,)), ((), ())), preferred_element_type=F32
    )
    pulled = pulled[:8] + pulled[8:]
    return scale * (pulled - 3.0 * pulled[6:7] * strain)


def spread(offset, rest, scale, base, incidence, terms, main_ref, rim_ref, plane_ref, depth_ref):
    force = vertex_force(offset, rest, scale, incidence)
    kernels = stencil_kernels(offset)
    grid = None
    for slot in range(SLOTS):
        table_x, table_y, table_rim, table_z = vertex_tables(base, kernels, slot)
        high = table_z.astype(jnp.bfloat16)
        low = (table_z - high.astype(F32)).astype(jnp.bfloat16)
        if depth_ref is not None:
            for n, table in enumerate((table_x, table_y, table_rim)):
                plane_ref[slot, n] = table
            depth_ref[slot, 0] = high
            depth_ref[slot, 1] = low
        for a in range(3):
            pushed = force[2 * a + slot : 2 * a + slot + 1, :]
            along_x = table_x * pushed
            for n in range(7):
                terms[(a * 7 + n) * 8 : (a * 7 + n + 1) * 8, :] = row_of(along_x, n) * table_y
            along_y = table_rim * pushed
            for n in range(3):
                start = MAIN_ROWS + (a * 3 + n) * 8
                terms[start : start + 8, :] = row_of(along_y, n) * table_x
        both = halves(terms[...])
        contract = (((1,), (1,)), ((), ()))
        part = lax.dot_general(both, high, contract, preferred_element_type=F32)
        rest_part = lax.dot_general(both[:TABLE_ROWS], low, contract, preferred_element_type=F32)
        part = part[:TABLE_ROWS] + part[TABLE_ROWS:] + rest_part
        grid = part if grid is None else grid + part
    main_ref[...] = grid[:MAIN_ROWS].reshape(3, 7, 8, CZ)
    rim_ref[...] = grid[MAIN_ROWS:].reshape(3, 3, 8, CZ)


def spread_messages(info_ref, main_ref, rim_ref, first_ref, second_ref):
    even = info_ref[0] == 0.0
    zero = jnp.zeros((2, CZ), F32)
    for a in range(3):
        up_rows, down_rows = [], []
        for n in range(3):
            rim = rim_ref[a, n]
            up_rows.append(rim[4:6])
            down_rows.append(rim[6:8])
        ups = [main_ref[a, 4], main_ref[a, 5], jnp.concatenate(up_rows + [zero], axis=0)]
        downs = [main_ref[a, 6], main_ref[a, 6], jnp.concatenate(down_rows + [zero], axis=0)]
        for t in range(3):
            first_ref[a, t] = choose(even, ups[t], downs[t])
            second_ref[a, t] = choose(even, downs[t], ups[t])


def incidence_kernel(triangles_ref, incidence_ref):
    vertex = lax.broadcasted_iota(jnp.int32, incidence_ref.shape, 0)
    corners = [triangles_ref[corner : corner + 1, :] == vertex for corner in range(3)]
    hit = corners[0] | corners[1] | corners[2]
    incidence_ref[...] = jnp.where(hit, 1.0, 0.0).astype(jnp.bfloat16)


def spread_kernel(
    stiffness_ref, occupied_ref, offset_in, rest_in, base_in, populations_in, solid_in, incidence_ref,
    main_ref, rim_ref, first_ref, second_ref, plane_ref, depth_ref,
    offset_ref, rest_ref, base_ref, populations_ref, solid_ref, info_ref, terms,
):
    place_x = lax.axis_index("gx")
    place_y = lax.axis_index("gy")
    even_row = lax.rem(tile_rows(), 2) == 0

    def by_slot(row):
        return jnp.where(even_row, row[:, 0:1], row[:, 1:2])

    held = by_slot(occupied_ref[...].astype(F32))
    info_ref[4] = by_slot(stiffness_ref[...]) * held
    info_ref[5] = held
    numbers = (lax.rem(place_x, 2), lax.rem(place_y, 2), place_x * CX, place_y * CY)
    for n, number in enumerate(numbers):
        info_ref[n] = jnp.full(TILE, number, jnp.int32).astype(F32)
    offset_ref[...] = six_rows(offset_in)
    rest_ref[...] = six_rows(rest_in)
    base_ref[...] = own_base(info_ref, base_in)
    populations_ref[...] = populations_in[...]
    solid_ref[...] = solid_in[...]
    spread(
        offset_ref[...], rest_ref[...], wide(info_ref[4]), base_ref[...],
        incidence_ref, terms, main_ref, rim_ref, plane_ref, depth_ref,
    )
    spread_messages(info_ref, main_ref, rim_ref, first_ref, second_ref)


def force_corner_kernel(info_ref, rim_ref, first_in, second_in, first_ref, second_ref):
    even_x = info_ref[0] == 0.0
    even_y = info_ref[1] == 0.0
    rows = tile_rows()
    for a in range(3):
        above = choose(even_x, first_in[a, 2], second_in[a, 2])
        below = choose(even_x, second_in[a, 2], first_in[a, 2])
        whole = []
        for n in range(3):
            from_below = below[2 * n : 2 * n + 2]
            from_above = above[2 * n : 2 * n + 1]
            part = rim_ref[a, n][:4]
            whole.append(
                jnp.concatenate([part[0:2] + from_below, part[2:3], part[3:4] + from_above], axis=0)
            )
        up = jnp.concatenate([whole[0], whole[1]], axis=0)
        down = jnp.concatenate([whole[2], whole[2]], axis=0)
        first_ref[a] = choose(even_y, up, down)
        second_ref[a] = choose(even_y, down, up)


def moment_sums(members, rows):
    groups = {}
    for step in (0, 1, -1):
        of_step = [(q, t) for q, t in members if VELOCITIES[q][1] == step]
        sums = []
        for what in (None, 0, 2):
            total = None
            for q, t in of_step:
                weight = 1 if what is None else VELOCITIES[q][what]
                if weight == 0:
                    continue
                term = t if weight == 1 else -t
                total = term if total is None else total + term
            sums.append(jnp.zeros(TILE, F32) if total is None else total)
        groups[step] = sums
    up = [jnp.where(rows == 0, 0.0, t) for t in groups[1]]
    down = [jnp.where(rows == 7, 0.0, t) for t in groups[-1]]
    density, along_x, along_z = [groups[0][k] + up[k] + down[k] for k in range(3)]
    inside = [density, along_x, up[0] - down[0], along_z]
    edge = [
        jnp.where(rows == 0, groups[1][k], jnp.where(rows == 7, groups[-1][k], 0.0)) for k in range(3)
    ]
    return inside, edge


def pack_edges(edge):
    return edge[0] + pltpu.roll(edge[1], 2, 0) + pltpu.roll(edge[2], 4, 0)


def unpack_edges(packed, rows):
    keep = (rows == 0) | (rows == 7)
    tiles = [packed, pltpu.roll(packed, 6, 0), pltpu.roll(packed, 4, 0)]
    return [jnp.where(keep, t, 0.0) for t in tiles]


def collide_kernel(
    info_ref, populations_ref, solid_ref, main_ref, first_x, second_x, first_y, second_y,
    stepped_ref, force_ref, first_ref, second_ref,
):
    even_x = info_ref[0] == 0.0
    even_y = info_ref[1] == 0.0
    rows = tile_rows()
    for x in range(4):
        force = []
        for a in range(3):
            f = main_ref[a, x]
            if x < 2:
                f = f + choose(even_x, second_x[a, x], first_x[a, x])
            if x == 3:
                f = f + choose(even_x, first_x[a, 0], second_x[a, 0])
            below = choose(even_y, second_y[a], first_y[a])
            above = choose(even_y, first_y[a], second_y[a])
            f = f + jnp.where(
                rows == 0,
                row_of(below, x),
                jnp.where(rows == 1, row_of(below, 4 + x), jnp.where(rows == 7, row_of(above, x), 0.0)),
            )
            force_ref[a, x] = f
            force.append(f)
        current = [populations_ref[q, x] for q in range(19)]
        density = functools.reduce(lambda u, v: u + v, current)
        velocity = []
        for a in range(3):
            moving = force[a] * 0.5
            for q in range(19):
                if VELOCITIES[q][a] == 1:
                    moving = moving + current[q]
                elif VELOCITIES[q][a] == -1:
                    moving = moving - current[q]
            velocity.append(moving)
        inverse = 1.0 / density
        velocity = [m * inverse for m in velocity]
        squared = velocity[0] * velocity[0] + velocity[1] * velocity[1] + velocity[2] * velocity[2]
        working = velocity[0] * force[0] + velocity[1] * force[1] + velocity[2] * force[2]
        walled = solid_ref[x] != 0
        common = 1.0 - 1.5 * squared
        factor = 1.0 - 0.5 / RELAX
        for q in range(19):
            vector = VELOCITIES[q]
            w = LATTICE_WEIGHTS[q]
            if q == 0:
                equilibrium = w * density * common
                source = (-3.0 * factor * w) * working
            else:
                along, pushed = None, None
                for a in range(3):
                    if vector[a] == 0:
                        continue
                    u = velocity[a] if vector[a] == 1 else -velocity[a]
                    f = force[a] if vector[a] == 1 else -force[a]
                    along = u if along is None else along + u
                    pushed = f if pushed is None else pushed + f
                equilibrium = w * density * (common + along * (3.0 + 4.5 * along))
                source = (factor * w) * (3.0 * (pushed - working) + 9.0 * along * pushed)
            updated = current[q] - (current[q] - equilibrium) / RELAX + source
            relaxed = jnp.where(walled, current[OPPOSITE[q]], updated)
            if vector[2] != 0:
                relaxed = pltpu.roll(relaxed, vector[2] % CZ, 1)
            if vector[1] != 0:
                relaxed = pltpu.roll(relaxed, vector[1] % 8, 0)
            stepped_ref[q, (x + vector[0]) % 4] = relaxed
    messages = []
    for crossing, lines in ((UP_X, (3,)), (DOWN_X, (0, 1))):
        slot = 0 if crossing is UP_X else 3
        tiles = [stepped_ref[q, slot] for q in crossing]
        for x in lines:
            members = [
                (q, stepped_ref[q, x])
                for q in range(19)
                if not (x == 0 and VELOCITIES[q][0] == 1) and not (x == 3 and VELOCITIES[q][0] == -1)
            ]
            inside, edge = moment_sums(members, rows)
            for k in range(3):
                inside[1 + k] = inside[1 + k] + 0.5 * force_ref[k, x]
            tiles += inside + [pack_edges(edge)]
        messages.append(tiles)
    up, down = messages
    for t in range(15):
        u = up[t] if t < len(up) else down[t]
        first_ref[t] = choose(even_x, u, down[t])
        second_ref[t] = choose(even_x, down[t], u)


def flow_corner_kernel(
    info_ref, stepped_in, force_ref, first_x, second_x,
    stepped_ref, inside_ref, leaving_ref, first_ref, second_ref, edges, up_tiles, down_tiles,
):
    even_x = info_ref[0] == 0.0
    even_y = info_ref[1] == 0.0
    rows = tile_rows()
    below = [choose(even_x, second_x[t], first_x[t]) for t in range(10)]
    above = [choose(even_x, first_x[t], second_x[t]) for t in range(15)]
    out_up = [(q, stepped_in[q, 0]) for q in UP_X]
    out_down = [(q, stepped_in[q, 3]) for q in DOWN_X]
    for q in range(19):
        for x in range(4):
            s = stepped_in[q, x]
            if q in UP_X and x == 0:
                s = below[UP_X.index(q)]
            if q in DOWN_X and x == 3:
                s = above[DOWN_X.index(q)]
            stepped_ref[(q * 4 + x) * 8 : (q * 4 + x + 1) * 8, :] = s
    for n, x in enumerate(X_ORDER):
        if 0 <= x < 4:
            members = [(q, stepped_ref[(q * 4 + x) * 8 : (q * 4 + x + 1) * 8, :]) for q in range(19)]
            inside, edge = moment_sums(members, rows)
            for k in range(3):
                inside[1 + k] = inside[1 + k] + 0.5 * force_ref[k, x]
        else:
            received = below[5:10] if x == -1 else above[5 + 5 * (x - 4) : 10 + 5 * (x - 4)]
            inside, edge = received[:4], unpack_edges(received[4], rows)
            if x != 5:
                own_inside, own_edge = moment_sums(out_down if x == -1 else out_up, rows)
                inside = [u + v for u, v in zip(inside, own_inside)]
                edge = [u + v for u, v in zip(edge, own_edge)]
        for k in range(4):
            inside_ref[(k * 8 + n) * 8 : (k * 8 + n + 1) * 8, :] = inside[k]
        for k in range(3):
            edges[(k * 8 + n) * 8 : (k * 8 + n + 1) * 8, :] = edge[k]
    for k in range(4):
        inside_ref[(k * 8 + 7) * 8 : (k * 8 + 8) * 8, :] = jnp.ones(TILE, F32)
    for k in range(3):
        edges[(k * 8 + 7) * 8 : (k * 8 + 8) * 8, :] = jnp.zeros(TILE, F32)
    for k in range(3):
        up = edges[pl.ds(k * 64, 8, stride=8), :]
        down = edges[pl.ds(k * 64 + 7, 8, stride=8), :]
        leaving_ref[k] = up
        leaving_ref[3 + k] = down
        up_tiles[k] = up
        down_tiles[k] = down
    for n in range(5):
        t, r = (n, 0) if n < 4 else (3, 4)
        up_tiles[t, r : r + 4, :] = stepped_ref[pl.ds(UP_Y[n] * 32, 4, stride=8), :]
        down_tiles[t, r : r + 4, :] = stepped_ref[pl.ds(DOWN_Y[n] * 32 + 7, 4, stride=8), :]
    for k in range(4):
        up_tiles[4 + k] = inside_ref[pl.ds(k * 64 + 7, 8, stride=8), :]
        down_tiles[4 + k] = inside_ref[pl.ds(k * 64, 8, stride=8), :]
    inverse = 1.0 / inside_ref[pl.ds(1, 8, stride=8), :]
    for k in range(3):
        down_tiles[8 + k] = inside_ref[pl.ds((k + 1) * 64 + 1, 8, stride=8), :] * inverse
    for t in range(11):
        u = up_tiles[t] if t < 8 else down_tiles[t]
        d = down_tiles[t]
        first_ref[t] = choose(even_y, u, d)
        second_ref[t] = choose(even_y, d, u)


def crossing(tiles, n, x):
    return row_of(tiles[n], x) if n < 4 else row_of(tiles[3], 4 + x)


def finish_fluid(info_ref, stepped_ref, inside_ref, leaving_ref, first_y, second_y, out_ref, flow):
    even_y = info_ref[1] == 0.0
    rows = tile_rows()
    below = [choose(even_y, second_y[t], first_y[t]) for t in range(8)]
    above = [choose(even_y, first_y[t], second_y[t]) for t in range(11)]
    for q in range(19):
        for x in range(4):
            s = stepped_ref[(q * 4 + x) * 8 : (q * 4 + x + 1) * 8, :]
            if q in UP_Y:
                s = jnp.where(rows == 0, crossing(below, UP_Y.index(q), x), s)
            if q in DOWN_Y:
                s = jnp.where(rows == 7, crossing(above, DOWN_Y.index(q), x), s)
            out_ref[q, x] = s

    def arriving(tiles, members):
        crossed = list(tiles[:4]) + [pltpu.roll(tiles[3], 4, 0)]
        out = []
        for k, what in enumerate((None, 0, 2)):
            total = None
            for n, q in enumerate(members):
                weight = 1 if what is None else VELOCITIES[q][what]
                if weight:
                    term = crossed[n] if weight == 1 else -crossed[n]
                    total = term if total is None else total + term
            out.append(jnp.where(rows < 4, total, tiles[k]))
        return [out[0], out[1], None, out[2]]

    from_below = arriving(below, UP_Y)
    from_above = arriving(above, DOWN_Y)
    from_below[2] = from_below[0]
    from_above[2] = -from_above[0]
    for n in range(7):
        total = []
        for k in range(4):
            t = inside_ref[(k * 8 + n) * 8 : (k * 8 + n + 1) * 8, :]
            t = t + jnp.where(
                rows == 0,
                row_of(from_below[k], n),
                jnp.where(rows == 7, row_of(from_above[k], n), 0.0),
            )
            total.append(t)
        inverse = 1.0 / total[0]
        for a in range(3):
            flow[(a * 7 + n) * 8 : (a * 7 + n + 1) * 8, :] = total[1 + a] * inverse
    up = [leaving_ref[0], leaving_ref[1], leaving_ref[0], leaving_ref[2]]
    down = [leaving_ref[3], leaving_ref[4], -leaving_ref[3], leaving_ref[5]]
    rims = (
        (0, [above[4 + k] + up[k] for k in range(4)]),
        (2, [below[4 + k] + down[k] for k in range(4)]),
    )
    for n, total in rims:
        inverse = 1.0 / jnp.where(rows == 7, 1.0, total[0])
        for a in range(3):
            start = MAIN_ROWS + (a * 3 + n) * 8
            flow[start : start + 8, :] = jnp.where(rows == 7, 0.0, total[1 + a] * inverse)
    for a in range(3):
        start = MAIN_ROWS + (a * 3 + 1) * 8
        flow[start : start + 8, :] = above[8 + a]


def sample(offset, live, plane_ref, depth_ref, flow):
    moved = [None] * 8
    zero = jnp.zeros((1, PAD), F32)
    both = halves(flow[...])
    for slot in range(SLOTS):
        table_x, table_y, table_rim = [plane_ref[slot, n] for n in range(3)]
        along = jnp.dot(both, depth_ref[slot, 0], preferred_element_type=F32)
        rest = jnp.dot(both[:TABLE_ROWS], depth_ref[slot, 1], preferred_element_type=F32)
        along = along[:TABLE_ROWS] + along[TABLE_ROWS:] + rest
        for a in range(3):
            inner = None
            for n in range(7):
                tile = along[(a * 7 + n) * 8 : (a * 7 + n + 1) * 8, :]
                term = tile * row_of(table_x, n)
                inner = term if inner is None else inner + term
            total = inner * table_y
            outer = None
            for n in range(3):
                start = MAIN_ROWS + (a * 3 + n) * 8
                term = along[start : start + 8, :] * row_of(table_rim, n)
                outer = term if outer is None else outer + term
            total = total + outer * table_x
            moved[2 * a + slot] = jnp.sum(total, axis=0, keepdims=True)
    stacked = jnp.concatenate(moved[:6] + [zero, zero], axis=0)
    return offset + live * stacked


def next_kernel(
    info_ref, stepped_ref, inside_ref, leaving_ref, first_y, second_y, plane_in, depth_in,
    offset_ref, rest_ref, base_ref, incidence_ref,
    out_ref, offset_out, main_ref, rim_ref, first_ref, second_ref, plane_ref, depth_ref, flow, terms,
):
    finish_fluid(info_ref, stepped_ref, inside_ref, leaving_ref, first_y, second_y, out_ref, flow)
    offset = sample(offset_ref[...], wide(info_ref[5]), plane_in, depth_in, flow)
    offset_out[...] = offset
    spread(
        offset, rest_ref[...], wide(info_ref[4]), base_ref[...],
        incidence_ref, terms, main_ref, rim_ref, plane_ref, depth_ref,
    )
    spread_messages(info_ref, main_ref, rim_ref, first_ref, second_ref)


def last_kernel(
    info_ref, stepped_ref, inside_ref, leaving_ref, first_y, second_y, plane_in, depth_in, offset_ref,
    out_ref, offset_out, flow,
):
    finish_fluid(info_ref, stepped_ref, inside_ref, leaving_ref, first_y, second_y, out_ref, flow)
    offset = sample(offset_ref[...], wide(info_ref[5]), plane_in, depth_in, flow)
    for a in range(3):
        offset_out[a] = offset[2 * a : 2 * a + 2]


INTERPRET = False


def call(kernel, outs, scratch, *operands):
    return pl.pallas_call(
        kernel,
        out_shape=[jax.ShapeDtypeStruct(shape, dtype) for shape, dtype in outs],
        in_specs=[pl.BlockSpec(memory_space=pltpu.VMEM)] * len(operands),
        out_specs=[pl.BlockSpec(memory_space=pltpu.VMEM)] * len(outs),
        scratch_shapes=[pltpu.VMEM(shape, dtype) for shape, dtype in scratch],
        compiler_params=pltpu.CompilerParams(vmem_limit_bytes=24 * 1024 * 1024),
        interpret=INTERPRET,
    )(*operands)


def partner(index, kind, size):
    return (index + 1) % size if (index + kind) % 2 == 0 else (index - 1) % size


def exchange(first, second, axis):
    size = lax.axis_size(axis)
    out = [None, None]
    for kind, message in ((1, second), (0, first)):
        pairs = [(i, partner(i, kind, size)) for i in range(size)]
        out[kind] = lax.ppermute(message, axis, pairs)
    return out


SPREAD_OUT = [
    ((3, 7, 8, CZ), F32),
    ((3, 3, 8, CZ), F32),
    ((3, 3, 8, CZ), F32),
    ((3, 3, 8, CZ), F32),
    ((SLOTS, 3, 8, PAD), F32),
    ((SLOTS, 2, CZ, PAD), jnp.bfloat16),
]
STEPPED = ((19, 4, 8, CZ), F32)


def steps(populations, solid, base_cell, offset, rest_displacement, stiffness, occupied, triangles):
    stored = (3, SLOTS, PAD)
    rows = (8, PAD)
    terms = ((TABLE_ROWS, PAD), F32)
    flow = ((TABLE_ROWS, CZ), F32)
    corners = triangles.T
    (incidence,) = call(incidence_kernel, [((PAD, corners.shape[1]), jnp.bfloat16)], [], corners)
    main, rim, first, second, plane, depth, where, rest, base, populations, solid, info = call(
        spread_kernel,
        SPREAD_OUT
        + [(rows, F32), (rows, F32), (rows, jnp.int32), STEPPED, (solid.shape, jnp.int32), ((6, 8, CZ), F32)],
        [terms],
        stiffness.reshape(1, SLOTS), occupied.reshape(1, SLOTS), offset.reshape(stored), rest_displacement.reshape(stored), base_cell.reshape(stored),
        populations, solid, incidence,
    )
    for substep in range(SUBSTEPS):
        first_x, second_x = exchange(first, second, "gx")
        corner = call(force_corner_kernel, [((3, 8, CZ), F32)] * 2, [], info, rim, first_x, second_x)
        first_y, second_y = exchange(*corner, "gy")
        stepped, force, first, second = call(
            collide_kernel,
            [STEPPED, ((3, 4, 8, CZ), F32), ((15, 8, CZ), F32), ((15, 8, CZ), F32)],
            [],
            info, populations, solid, main, first_x, second_x, first_y, second_y,
        )
        first_x, second_x = exchange(first, second, "gx")
        stepped, inside, leaving, first, second = call(
            flow_corner_kernel,
            [
                ((19 * 4 * 8, CZ), F32), ((4 * 8 * 8, CZ), F32), ((6, 8, CZ), F32),
                ((11, 8, CZ), F32), ((11, 8, CZ), F32),
            ],
            [((3 * 8 * 8, CZ), F32), ((8, 8, CZ), F32), ((11, 8, CZ), F32)],
            info, stepped, force, first_x, second_x,
        )
        first_y, second_y = exchange(first, second, "gy")
        fluid = (info, stepped, inside, leaving, first_y, second_y, plane, depth)
        if substep < SUBSTEPS - 1:
            populations, where, main, rim, first, second, plane, depth = call(
                next_kernel, [STEPPED, (rows, F32)] + SPREAD_OUT, [flow, terms],
                *fluid, where, rest, base, incidence,
            )
        else:
            populations, where = call(last_kernel, [STEPPED, (stored, F32)], [flow], *fluid, where)
    return populations, where.reshape(offset.shape)


def solution(mesh):
    in_specs = (
        P(None, "gx", "gy", None),
        P("gx", "gy", None),
        P(None, "gx", "gy", None, None),
        P(None, "gx", "gy", None, None),
        P(None, "gx", "gy", None, None),
        P("gx", "gy", None),
        P("gx", "gy", None),
        P(),
    )
    out_specs = (P(None, "gx", "gy", None), P(None, "gx", "gy", None, None))
    return jax.shard_map(steps, mesh=mesh, in_specs=in_specs, out_specs=out_specs, check_vma=False)
```

```python
import functools
import math

import jax
import jax.numpy as jnp
from jax import lax
from jax.experimental import pallas as pl
from jax.experimental.pallas import tpu as pltpu
from jax.sharding import PartitionSpec as P


SUBSTEPS = 3

VELOCITIES = [
    [0, 0, 0],
    [1, 0, 0],
    [-1, 0, 0],
    [0, 1, 0],
    [0, -1, 0],
    [0, 0, 1],
    [0, 0, -1],
    [1, 1, 0],
    [-1, -1, 0],
    [1, -1, 0],
    [-1, 1, 0],
    [1, 0, 1],
    [-1, 0, -1],
    [1, 0, -1],
    [-1, 0, 1],
    [0, 1, 1],
    [0, -1, -1],
    [0, 1, -1],
    [0, -1, 1],
]
OPPOSITE = [0, 2, 1, 4, 3, 6, 5, 8, 7, 10, 9, 12, 11, 14, 13, 16, 15, 18, 17]
LATTICE_WEIGHTS = [1.0 / 3.0] + [1.0 / 18.0] * 6 + [1.0 / 36.0] * 12
RELAX = 0.8
CX, CY, CZ = 4, 8, 128
SLOTS, PAD = 2, 768
UP_X = [q for q in range(19) if VELOCITIES[q][0] == 1]
DOWN_X = [q for q in range(19) if VELOCITIES[q][0] == -1]
UP_Y = [q for q in range(19) if VELOCITIES[q][1] == 1]
DOWN_Y = [q for q in range(19) if VELOCITIES[q][1] == -1]
FLAT_X = [q for q in range(19) if VELOCITIES[q][0] == 0]
X_ORDER = [0, 1, 2, 3, 4, 5, -1]
MAIN_ROWS = 3 * 7 * 8
RIM_ROWS = 3 * 3 * 8
TABLE_ROWS = MAIN_ROWS + RIM_ROWS
F32 = jnp.float32
TILE = (8, CZ)


def tile_rows():
    return lax.broadcasted_iota(jnp.int32, TILE, 0)


def wide(row):
    return jnp.concatenate([row] * (PAD // CZ), axis=1)


def six_rows(ref):
    return jnp.concatenate([ref[0], ref[1], ref[2], jnp.zeros((2, PAD), ref.dtype)], axis=0)


def own_base(info_ref, base_ref):
    base = six_rows(base_ref)
    rows = lax.broadcasted_iota(jnp.int32, TILE, 0)
    start = jnp.where(rows < 2, info_ref[2], jnp.where(rows < 4, info_ref[3], 0.0))
    return base - wide(start.astype(jnp.int32))


def row_of(tile, r):
    return jnp.broadcast_to(tile[r : r + 1, :], (8, tile.shape[1]))


def choose(first, a, b):
    return jnp.where(first, a, b)


def stencil_kernels(offset):
    angle = offset * (math.pi / 2.0)
    c, s = jnp.cos(angle), jnp.sin(angle)
    return [(1.0 - s) * 0.25, (1.0 + c) * 0.25, (1.0 + s) * 0.25, (1.0 - c) * 0.25]


def pick(distance, kernels, r):
    out = jnp.zeros(distance.shape, F32)
    for n in range(4):
        out = jnp.where(distance == n, kernels[n][r : r + 1, :], out)
    return out


def vertex_tables(base, kernels, slot):
    rows = lax.broadcasted_iota(jnp.int32, (8, PAD), 0)
    x_value = jnp.where(rows < 6, rows, jnp.where(rows == 6, -1, 100))
    y_rim = jnp.where(rows < 2, rows + 8, jnp.where(rows == 2, -1, 100))
    base_x, base_y, base_z = [base[2 * a + slot : 2 * a + slot + 1, :] for a in range(3)]
    table_x = pick(x_value - base_x + 1, kernels, slot)
    table_y = pick(rows - base_y + 1, kernels, 2 + slot)
    table_rim = pick(y_rim - base_y + 1, kernels, 2 + slot)
    depth = lax.broadcasted_iota(jnp.int32, (CZ, PAD), 0)
    table_z = pick(jnp.bitwise_and(depth - base_z + 1, CZ - 1), kernels, 4 + slot)
    return table_x, table_y, table_rim, table_z


def halves(rows):
    high = rows.astype(jnp.bfloat16)
    return jnp.concatenate([high, (rows - high.astype(F32)).astype(jnp.bfloat16)], axis=0)


def vertex_force(offset, rest, scale, incidence):
    strain = offset - rest
    summed = jnp.dot(halves(strain), incidence[...], preferred_element_type=F32)
    summed = summed[:8] + summed[8:]
    rows = lax.broadcasted_iota(jnp.int32, summed.shape, 0)
    summed = jnp.where(rows == 6, 1.0, summed)
    pulled = lax.dot_general(
        halves(summed), incidence[...], (((1,), (1,)), ((), ())), preferred_element_type=F32
    )
    pulled = pulled[:8] + pulled[8:]
    return scale * (pulled - 3.0 * pulled[6:7] * strain)


def spread(offset, rest, scale, base, incidence, terms, main_ref, rim_ref, plane_ref, depth_ref):
    force = vertex_force(offset, rest, scale, incidence)
    kernels = stencil_kernels(offset)
    grid = None
    for slot in range(SLOTS):
        table_x, table_y, table_rim, table_z = vertex_tables(base, kernels, slot)
        high = table_z.astype(jnp.bfloat16)
        low = (table_z - high.astype(F32)).astype(jnp.bfloat16)
        if depth_ref is not None:
            for n, table in enumerate((table_x, table_y, table_rim)):
                plane_ref[slot, n] = table
            depth_ref[slot, 0] = high
            depth_ref[slot, 1] = low
        for a in range(3):
            pushed = force[2 * a + slot : 2 * a + slot + 1, :]
            along_x = table_x * pushed
            for n in range(7):
                terms[(a * 7 + n) * 8 : (a * 7 + n + 1) * 8, :] = row_of(along_x, n) * table_y
            along_y = table_rim * pushed
            for n in range(3):
                start = MAIN_ROWS + (a * 3 + n) * 8
                terms[start : start + 8, :] = row_of(along_y, n) * table_x
        both = halves(terms[...])
        contract = (((1,), (1,)), ((), ()))
        part = lax.dot_general(both, high, contract, preferred_element_type=F32)
        rest_part = lax.dot_general(both[:TABLE_ROWS], low, contract, preferred_element_type=F32)
        part = part[:TABLE_ROWS] + part[TABLE_ROWS:] + rest_part
        grid = part if grid is None else grid + part
    main_ref[...] = grid[:MAIN_ROWS].reshape(3, 7, 8, CZ)
    rim_ref[...] = grid[MAIN_ROWS:].reshape(3, 3, 8, CZ)


def spread_messages(info_ref, rim_ref, first_ref, second_ref):
    even = info_ref[1] == 0.0
    for a in range(3):
        down = rim_ref[a, 2]
        for n in range(2):
            up = rim_ref[a, n]
            first_ref[a, n] = choose(even, up, down)
            second_ref[a, n] = choose(even, down, up)


def incidence_kernel(triangles_ref, incidence_ref):
    vertex = lax.broadcasted_iota(jnp.int32, incidence_ref.shape, 0)
    corners = [triangles_ref[corner : corner + 1, :] == vertex for corner in range(3)]
    hit = corners[0] | corners[1] | corners[2]
    incidence_ref[...] = jnp.where(hit, 1.0, 0.0).astype(jnp.bfloat16)


def spread_kernel(
    info_ref, offset_in, rest_in, base_in, incidence_ref,
    main_ref, first_ref, second_ref, plane_ref, depth_ref, offset_ref, rest_ref, base_ref, rim_ref, terms,
):
    offset_ref[...] = six_rows(offset_in)
    rest_ref[...] = six_rows(rest_in)
    base_ref[...] = own_base(info_ref, base_in)
    spread(
        offset_ref[...], rest_ref[...], wide(info_ref[4]), base_ref[...],
        incidence_ref, terms, main_ref, rim_ref, plane_ref, depth_ref,
    )
    spread_messages(info_ref, rim_ref, first_ref, second_ref)


def force_kernel(info_ref, main_ref, first_y, second_y, whole_ref, first_ref, second_ref):
    even_x = info_ref[0] == 0.0
    even_y = info_ref[1] == 0.0
    rows = tile_rows()
    for a in range(3):
        below = [choose(even_y, second_y[a, n], first_y[a, n]) for n in range(2)]
        above = choose(even_y, first_y[a, 0], second_y[a, 0])
        tiles = []
        for n in range(7):
            added = jnp.where(
                rows == 0,
                row_of(below[0], n),
                jnp.where(rows == 1, row_of(below[1], n), jnp.where(rows == 7, row_of(above, n), 0.0)),
            )
            tiles.append(main_ref[a, n] + added)
            whole_ref[a, n] = tiles[n]
        ups = [tiles[2], tiles[3], tiles[4], tiles[5]]
        downs = [tiles[6], tiles[0], tiles[1], tiles[2]]
        for t in range(4):
            first_ref[a, t] = choose(even_x, ups[t], downs[t])
            second_ref[a, t] = choose(even_x, downs[t], ups[t])


def moment_sums(members, rows):
    groups = {}
    for step in (0, 1, -1):
        of_step = [(q, t) for q, t in members if VELOCITIES[q][1] == step]
        sums = []
        for what in (None, 0, 2):
            total = None
            for q, t in of_step:
                weight = 1 if what is None else VELOCITIES[q][what]
                if weight == 0:
                    continue
                term = t if weight == 1 else -t
                total = term if total is None else total + term
            sums.append(jnp.zeros(TILE, F32) if total is None else total)
        groups[step] = sums
    up = [jnp.where(rows == 0, 0.0, t) for t in groups[1]]
    down = [jnp.where(rows == 7, 0.0, t) for t in groups[-1]]
    density, along_x, along_z = [groups[0][k] + up[k] + down[k] for k in range(3)]
    inside = [density, along_x, up[0] - down[0], along_z]
    edge = [
        jnp.where(rows == 0, groups[1][k], jnp.where(rows == 7, groups[-1][k], 0.0)) for k in range(3)
    ]
    return inside, edge


def pack_edges(edge):
    return edge[0] + pltpu.roll(edge[1], 2, 0) + pltpu.roll(edge[2], 4, 0)


def unpack_edges(packed, rows):
    keep = (rows == 0) | (rows == 7)
    tiles = [packed, pltpu.roll(packed, 6, 0), pltpu.roll(packed, 4, 0)]
    return [jnp.where(keep, t, 0.0) for t in tiles]


def push(tile, q):
    vector = VELOCITIES[q]
    if vector[2] != 0:
        tile = pltpu.roll(tile, vector[2] % CZ, 1)
    if vector[1] != 0:
        tile = pltpu.roll(tile, vector[1] % 8, 0)
    return tile


def momentum(current, a):
    total = None
    for q in range(19):
        if VELOCITIES[q][a] != 0:
            term = current[q] if VELOCITIES[q][a] == 1 else -current[q]
            total = term if total is None else total + term
    return total


def gained(density, carried, force, directions):
    inverse = 1.0 / density
    return gained_from(density, [(0.5 * force[a] + carried[a]) * inverse for a in range(3)], force, directions)


def gained_from(density, velocity, force, directions):
    squared = velocity[0] * velocity[0] + velocity[1] * velocity[1] + velocity[2] * velocity[2]
    working = velocity[0] * force[0] + velocity[1] * force[1] + velocity[2] * force[2]
    common = 1.0 - 1.5 * squared
    factor = 1.0 - 0.5 / RELAX
    out = {}
    for q in directions:
        vector = VELOCITIES[q]
        w = LATTICE_WEIGHTS[q]
        if q == 0:
            out[q] = (w / RELAX) * density * common - (3.0 * factor * w) * working
            continue
        along, pushed = None, None
        for a in range(3):
            if vector[a] == 0:
                continue
            u = velocity[a] if vector[a] == 1 else -velocity[a]
            f = force[a] if vector[a] == 1 else -force[a]
            along = u if along is None else along + u
            pushed = f if pushed is None else pushed + f
        equilibrium = (w / RELAX) * density * (common + along * (3.0 + 4.5 * along))
        source = (factor * w) * (3.0 * (pushed - working) + 9.0 * along * pushed)
        out[q] = equilibrium + source
    return out


def kept(current, walled, q):
    return jnp.where(walled, current[OPPOSITE[q]], (1.0 - 1.0 / RELAX) * current[q])


def halo_messages(info_ref, populations_ref, solid_ref, first_ref, second_ref):
    even_x = info_ref[0] == 0.0
    rows = tile_rows()
    current = [[populations_ref[q, x] for q in range(19)] for x in range(4)]
    walled = [solid_ref[x] != 0 for x in range(4)]

    def state(x):
        density = functools.reduce(lambda u, v: u + v, current[x])
        tiles = [density] + [momentum(current[x], a) for a in range(3)]
        return [jnp.where(walled[x], 0.0, t) for t in tiles]

    def carried(x, directions):
        return [(q, push(kept(current[x], walled[x], q), q)) for q in directions]

    def sums(members):
        inside, edge = moment_sums(members, rows)
        return inside + [pack_edges(edge)]

    up = state(2) + state(3)
    up += sums(carried(2, UP_X) + carried(3, FLAT_X))
    up += [t for _, t in carried(3, UP_X)]
    down = state(0) + state(1) + state(2)
    down += sums(carried(0, FLAT_X) + carried(1, DOWN_X))
    down += sums(carried(0, UP_X) + carried(1, FLAT_X) + carried(2, DOWN_X))
    down += [t for _, t in carried(0, DOWN_X)]
    for t in range(27):
        u = up[t] if t < 18 else down[t]
        first_ref[t] = choose(even_x, u, down[t])
        second_ref[t] = choose(even_x, down[t], u)


def halo_kernel(
    stiffness_ref, occupied_ref, populations_in, solid_in,
    info_ref, populations_ref, solid_ref, first_ref, second_ref,
):
    place_x = lax.axis_index("gx")
    place_y = lax.axis_index("gy")
    even_row = lax.rem(tile_rows(), 2) == 0

    def by_slot(row):
        return jnp.where(even_row, row[:, 0:1], row[:, 1:2])

    held = by_slot(occupied_ref[...].astype(F32))
    info_ref[4] = by_slot(stiffness_ref[...]) * held
    info_ref[5] = held
    numbers = (lax.rem(place_x, 2), lax.rem(place_y, 2), place_x * CX, place_y * CY)
    for n, number in enumerate(numbers):
        info_ref[n] = jnp.full(TILE, number, jnp.int32).astype(F32)
    populations_ref[...] = populations_in[...]
    solid_ref[...] = solid_in[...]
    halo_messages(info_ref, populations_ref, solid_ref, first_ref, second_ref)


def collide_kernel(
    info_ref, populations_ref, solid_ref, whole_ref, first_x, second_x, first_h, second_h,
    stepped_ref, inside_ref, leaving_ref, first_ref, second_ref, edges, up_tiles, down_tiles,
):
    even_x = info_ref[0] == 0.0
    even_y = info_ref[1] == 0.0
    rows = tile_rows()
    below = [choose(even_x, second_h[t], first_h[t]) for t in range(18)]
    above = [choose(even_x, first_h[t], second_h[t]) for t in range(27)]
    from_below = [[choose(even_x, second_x[a, t], first_x[a, t]) for t in range(4)] for a in range(3)]
    from_above = [[choose(even_x, first_x[a, t], second_x[a, t]) for t in range(4)] for a in range(3)]
    force = {}
    for x in range(-2, 7):
        parts = []
        for a in range(3):
            terms = []
            if -1 <= x <= 5:
                terms.append(whole_ref[a, X_ORDER.index(x)])
            if x < 2:
                terms.append(from_below[a][x + 2])
            if x > 2:
                terms.append(from_above[a][x - 3])
            parts.append(functools.reduce(lambda u, v: u + v, terms))
        force[x] = parts

    def place(q, x, tile):
        stepped_ref[(q * 4 + x) * 8 : (q * 4 + x + 1) * 8, :] = tile

    out_up, out_down = [], []
    for x in range(4):
        current = [populations_ref[q, x] for q in range(19)]
        walled = solid_ref[x] != 0
        density = functools.reduce(lambda u, v: u + v, current)
        new = gained(density, [momentum(current, a) for a in range(3)], force[x], range(19))
        for q in range(19):
            relaxed = jnp.where(walled, current[OPPOSITE[q]], (1.0 - 1.0 / RELAX) * current[q] + new[q])
            relaxed = push(relaxed, q)
            target = x + VELOCITIES[q][0]
            if target == 4:
                out_up.append((q, relaxed))
            elif target == -1:
                out_down.append((q, relaxed))
            else:
                place(q, target, relaxed)

    def halo(x, tiles, directions):
        fluid = tiles[0] != 0.0
        pulled = [jnp.where(fluid, f, 0.0) for f in force[x]]
        density = tiles[0]
        inverse = 1.0 / jnp.where(fluid, density, 1.0)
        velocity = [(0.5 * pulled[a] + tiles[1 + a]) * inverse for a in range(3)]
        new = gained_from(density, velocity, pulled, directions)
        return {q: push(new[q], q) for q in directions}

    def members(part, directions):
        return [(q, part[q]) for q in directions]

    before = halo(-2, below[0:4], UP_X)
    last = halo(-1, below[4:8], FLAT_X + UP_X)
    for n, q in enumerate(UP_X):
        place(q, 0, below[13 + n] + last[q])
    reached = {-1: (below[8:13], members(before, UP_X) + members(last, FLAT_X) + out_down)}
    four = halo(4, above[0:4], range(19))
    five = halo(5, above[4:8], FLAT_X + DOWN_X)
    six = halo(6, above[8:12], DOWN_X)
    for n, q in enumerate(DOWN_X):
        place(q, 3, above[22 + n] + four[q])
    reached[4] = (above[12:17], members(four, FLAT_X) + members(five, DOWN_X) + out_up)
    reached[5] = (
        above[17:22],
        members(four, UP_X) + members(five, FLAT_X) + members(six, DOWN_X),
    )
    for n, x in enumerate(X_ORDER):
        if 0 <= x < 4:
            every = [(q, stepped_ref[(q * 4 + x) * 8 : (q * 4 + x + 1) * 8, :]) for q in range(19)]
            inside, edge = moment_sums(every, rows)
        else:
            received, arrived = reached[x]
            inside, edge = moment_sums(arrived, rows)
            inside = [u + v for u, v in zip(inside, received[:4])]
            edge = [u + v for u, v in zip(edge, unpack_edges(received[4], rows))]
        for k in range(3):
            inside[1 + k] = inside[1 + k] + 0.5 * force[x][k]
        for k in range(4):
            inside_ref[(k * 8 + n) * 8 : (k * 8 + n + 1) * 8, :] = inside[k]
        for k in range(3):
            edges[(k * 8 + n) * 8 : (k * 8 + n + 1) * 8, :] = edge[k]
    for k in range(4):
        inside_ref[(k * 8 + 7) * 8 : (k * 8 + 8) * 8, :] = jnp.ones(TILE, F32)
    for k in range(3):
        edges[(k * 8 + 7) * 8 : (k * 8 + 8) * 8, :] = jnp.zeros(TILE, F32)
    for k in range(3):
        up = edges[pl.ds(k * 64, 8, stride=8), :]
        down = edges[pl.ds(k * 64 + 7, 8, stride=8), :]
        leaving_ref[k] = up
        leaving_ref[3 + k] = down
        up_tiles[k] = up
        down_tiles[k] = down
    for n in range(5):
        t, r = (n, 0) if n < 4 else (3, 4)
        up_tiles[t, r : r + 4, :] = stepped_ref[pl.ds(UP_Y[n] * 32, 4, stride=8), :]
        down_tiles[t, r : r + 4, :] = stepped_ref[pl.ds(DOWN_Y[n] * 32 + 7, 4, stride=8), :]
    for k in range(4):
        up_tiles[4 + k] = inside_ref[pl.ds(k * 64 + 7, 8, stride=8), :]
        down_tiles[4 + k] = inside_ref[pl.ds(k * 64, 8, stride=8), :]
    inverse = 1.0 / inside_ref[pl.ds(1, 8, stride=8), :]
    for k in range(3):
        down_tiles[8 + k] = inside_ref[pl.ds((k + 1) * 64 + 1, 8, stride=8), :] * inverse
    for t in range(11):
        u = up_tiles[t] if t < 8 else down_tiles[t]
        d = down_tiles[t]
        first_ref[t] = choose(even_y, u, d)
        second_ref[t] = choose(even_y, d, u)


def crossing(tiles, n, x):
    return row_of(tiles[n], x) if n < 4 else row_of(tiles[3], 4 + x)


def finish_fluid(info_ref, stepped_ref, inside_ref, leaving_ref, first_y, second_y, out_ref, flow):
    even_y = info_ref[1] == 0.0
    rows = tile_rows()
    below = [choose(even_y, second_y[t], first_y[t]) for t in range(8)]
    above = [choose(even_y, first_y[t], second_y[t]) for t in range(11)]
    for q in range(19):
        for x in range(4):
            s = stepped_ref[(q * 4 + x) * 8 : (q * 4 + x + 1) * 8, :]
            if q in UP_Y:
                s = jnp.where(rows == 0, crossing(below, UP_Y.index(q), x), s)
            if q in DOWN_Y:
                s = jnp.where(rows == 7, crossing(above, DOWN_Y.index(q), x), s)
            out_ref[q, x] = s

    def arriving(tiles, members):
        crossed = list(tiles[:4]) + [pltpu.roll(tiles[3], 4, 0)]
        out = []
        for k, what in enumerate((None, 0, 2)):
            total = None
            for n, q in enumerate(members):
                weight = 1 if what is None else VELOCITIES[q][what]
                if weight:
                    term = crossed[n] if weight == 1 else -crossed[n]
                    total = term if total is None else total + term
            out.append(jnp.where(rows < 4, total, tiles[k]))
        return [out[0], out[1], None, out[2]]

    from_below = arriving(below, UP_Y)
    from_above = arriving(above, DOWN_Y)
    from_below[2] = from_below[0]
    from_above[2] = -from_above[0]
    for n in range(7):
        total = []
        for k in range(4):
            t = inside_ref[(k * 8 + n) * 8 : (k * 8 + n + 1) * 8, :]
            t = t + jnp.where(
                rows == 0,
                row_of(from_below[k], n),
                jnp.where(rows == 7, row_of(from_above[k], n), 0.0),
            )
            total.append(t)
        inverse = 1.0 / total[0]
        for a in range(3):
            flow[(a * 7 + n) * 8 : (a * 7 + n + 1) * 8, :] = total[1 + a] * inverse
    up = [leaving_ref[0], leaving_ref[1], leaving_ref[0], leaving_ref[2]]
    down = [leaving_ref[3], leaving_ref[4], -leaving_ref[3], leaving_ref[5]]
    rims = (
        (0, [above[4 + k] + up[k] for k in range(4)]),
        (2, [below[4 + k] + down[k] for k in range(4)]),
    )
    for n, total in rims:
        inverse = 1.0 / jnp.where(rows == 7, 1.0, total[0])
        for a in range(3):
            start = MAIN_ROWS + (a * 3 + n) * 8
            flow[start : start + 8, :] = jnp.where(rows == 7, 0.0, total[1 + a] * inverse)
    for a in range(3):
        start = MAIN_ROWS + (a * 3 + 1) * 8
        flow[start : start + 8, :] = above[8 + a]


def sample(offset, live, plane_ref, depth_ref, flow):
    moved = [None] * 8
    zero = jnp.zeros((1, PAD), F32)
    both = halves(flow[...])
    for slot in range(SLOTS):
        table_x, table_y, table_rim = [plane_ref[slot, n] for n in range(3)]
        along = jnp.dot(both, depth_ref[slot, 0], preferred_element_type=F32)
        rest = jnp.dot(both[:TABLE_ROWS], depth_ref[slot, 1], preferred_element_type=F32)
        along = along[:TABLE_ROWS] + along[TABLE_ROWS:] + rest
        for a in range(3):
            inner = None
            for n in range(7):
                tile = along[(a * 7 + n) * 8 : (a * 7 + n + 1) * 8, :]
                term = tile * row_of(table_x, n)
                inner = term if inner is None else inner + term
            total = inner * table_y
            outer = None
            for n in range(3):
                start = MAIN_ROWS + (a * 3 + n) * 8
                term = along[start : start + 8, :] * row_of(table_rim, n)
                outer = term if outer is None else outer + term
            total = total + outer * table_x
            moved[2 * a + slot] = jnp.sum(total, axis=0, keepdims=True)
    stacked = jnp.concatenate(moved[:6] + [zero, zero], axis=0)
    return offset + live * stacked


def finish_kernel(
    info_ref, stepped_ref, inside_ref, leaving_ref, first_y, second_y, solid_ref,
    out_ref, flow_ref, first_ref, second_ref,
):
    finish_fluid(info_ref, stepped_ref, inside_ref, leaving_ref, first_y, second_y, out_ref, flow_ref)
    halo_messages(info_ref, out_ref, solid_ref, first_ref, second_ref)


def next_kernel(
    info_ref, flow_ref, plane_in, depth_in, offset_ref, rest_ref, base_ref, incidence_ref,
    main_ref, first_ref, second_ref, plane_ref, depth_ref, offset_out, rim_ref, terms,
):
    offset = sample(offset_ref[...], wide(info_ref[5]), plane_in, depth_in, flow_ref)
    offset_out[...] = offset
    spread(
        offset, rest_ref[...], wide(info_ref[4]), base_ref[...],
        incidence_ref, terms, main_ref, rim_ref, plane_ref, depth_ref,
    )
    spread_messages(info_ref, rim_ref, first_ref, second_ref)


def last_kernel(
    info_ref, stepped_ref, inside_ref, leaving_ref, first_y, second_y, plane_in, depth_in, offset_ref,
    out_ref, offset_out, flow,
):
    finish_fluid(info_ref, stepped_ref, inside_ref, leaving_ref, first_y, second_y, out_ref, flow)
    offset = sample(offset_ref[...], wide(info_ref[5]), plane_in, depth_in, flow)
    for a in range(3):
        offset_out[a] = offset[2 * a : 2 * a + 2]


INTERPRET = False


def call(kernel, outs, scratch, *operands):
    return pl.pallas_call(
        kernel,
        out_shape=[jax.ShapeDtypeStruct(shape, dtype) for shape, dtype in outs],
        in_specs=[pl.BlockSpec(memory_space=pltpu.VMEM)] * len(operands),
        out_specs=[pl.BlockSpec(memory_space=pltpu.VMEM)] * len(outs),
        scratch_shapes=[pltpu.VMEM(shape, dtype) for shape, dtype in scratch],
        compiler_params=pltpu.CompilerParams(vmem_limit_bytes=24 * 1024 * 1024),
        interpret=INTERPRET,
    )(*operands)


def partner(index, kind, size):
    return (index + 1) % size if (index + kind) % 2 == 0 else (index - 1) % size


def exchange(first, second, axis):
    size = lax.axis_size(axis)
    out = [None, None]
    for kind, message in ((1, second), (0, first)):
        pairs = [(i, partner(i, kind, size)) for i in range(size)]
        out[kind] = lax.ppermute(message, axis, pairs)
    return out


SPREAD_OUT = [
    ((3, 7, 8, CZ), F32),
    ((3, 2, 8, CZ), F32),
    ((3, 2, 8, CZ), F32),
    ((SLOTS, 3, 8, PAD), F32),
    ((SLOTS, 2, CZ, PAD), jnp.bfloat16),
]
HALO_OUT = [((27, 8, CZ), F32)] * 2
STEPPED = ((19, 4, 8, CZ), F32)


def steps(populations, solid, base_cell, offset, rest_displacement, stiffness, occupied, triangles):
    stored = (3, SLOTS, PAD)
    rows = (8, PAD)
    scratch = [((3, 3, 8, CZ), F32), ((TABLE_ROWS, PAD), F32)]
    flow_out = ((TABLE_ROWS, CZ), F32)
    corners = triangles.T
    (incidence,) = call(incidence_kernel, [((PAD, corners.shape[1]), jnp.bfloat16)], [], corners)
    info, populations, solid, first_h, second_h = call(
        halo_kernel,
        [((6, 8, CZ), F32), STEPPED, (solid.shape, jnp.int32)] + HALO_OUT, [],
        stiffness.reshape(1, SLOTS), occupied.reshape(1, SLOTS), populations, solid,
    )
    main, first, second, plane, depth, where, rest, base = call(
        spread_kernel, SPREAD_OUT + [(rows, F32), (rows, F32), (rows, jnp.int32)], scratch,
        info, offset.reshape(stored), rest_displacement.reshape(stored), base_cell.reshape(stored),
        incidence,
    )
    for substep in range(SUBSTEPS):
        first_h, second_h = exchange(first_h, second_h, "gx")
        first, second = exchange(first, second, "gy")
        whole, first, second = call(
            force_kernel, [((3, 7, 8, CZ), F32), ((3, 4, 8, CZ), F32), ((3, 4, 8, CZ), F32)], [],
            info, main, first, second,
        )
        first, second = exchange(first, second, "gx")
        stepped, inside, leaving, first, second = call(
            collide_kernel,
            [
                ((19 * 4 * 8, CZ), F32), ((4 * 8 * 8, CZ), F32), ((6, 8, CZ), F32),
                ((11, 8, CZ), F32), ((11, 8, CZ), F32),
            ],
            [((3 * 8 * 8, CZ), F32), ((8, 8, CZ), F32), ((11, 8, CZ), F32)],
            info, populations, solid, whole, first, second, first_h, second_h,
        )
        first, second = exchange(first, second, "gy")
        fluid = (info, stepped, inside, leaving, first, second)
        if substep < SUBSTEPS - 1:
            populations, flow, first_h, second_h = call(
                finish_kernel, [STEPPED, flow_out] + HALO_OUT, [], *fluid, solid
            )
            main, first, second, plane, depth, where = call(
                next_kernel, SPREAD_OUT + [(rows, F32)], scratch,
                info, flow, plane, depth, where, rest, base, incidence,
            )
        else:
            populations, where = call(last_kernel, [STEPPED, (stored, F32)], [flow_out], *fluid, plane, depth, where)
    return populations, where.reshape(offset.shape)


def solution(mesh):
    in_specs = (
        P(None, "gx", "gy", None),
        P("gx", "gy", None),
        P(None, "gx", "gy", None, None),
        P(None, "gx", "gy", None, None),
        P(None, "gx", "gy", None, None),
        P("gx", "gy", None),
        P("gx", "gy", None),
        P(),
    )
    out_specs = (P(None, "gx", "gy", None), P(None, "gx", "gy", None, None))
    return jax.shard_map(steps, mesh=mesh, in_specs=in_specs, out_specs=out_specs, check_vma=False)
```

```python
import functools
import math

import jax
import jax.numpy as jnp
from jax import lax
from jax.experimental import pallas as pl
from jax.experimental.pallas import tpu as pltpu
from jax.sharding import PartitionSpec as P


SUBSTEPS = 3

VELOCITIES = [
    [0, 0, 0],
    [1, 0, 0],
    [-1, 0, 0],
    [0, 1, 0],
    [0, -1, 0],
    [0, 0, 1],
    [0, 0, -1],
    [1, 1, 0],
    [-1, -1, 0],
    [1, -1, 0],
    [-1, 1, 0],
    [1, 0, 1],
    [-1, 0, -1],
    [1, 0, -1],
    [-1, 0, 1],
    [0, 1, 1],
    [0, -1, -1],
    [0, 1, -1],
    [0, -1, 1],
]
OPPOSITE = [0, 2, 1, 4, 3, 6, 5, 8, 7, 10, 9, 12, 11, 14, 13, 16, 15, 18, 17]
LATTICE_WEIGHTS = [1.0 / 3.0] + [1.0 / 18.0] * 6 + [1.0 / 36.0] * 12
RELAX = 0.8
CX, CY, CZ = 4, 8, 128
SLOTS, PAD = 2, 768
UP_X = [q for q in range(19) if VELOCITIES[q][0] == 1]
DOWN_X = [q for q in range(19) if VELOCITIES[q][0] == -1]
UP_Y = [q for q in range(19) if VELOCITIES[q][1] == 1]
DOWN_Y = [q for q in range(19) if VELOCITIES[q][1] == -1]
FLAT_X = [q for q in range(19) if VELOCITIES[q][0] == 0]
X_ORDER = [0, 1, 2, 3, 4, 5, -1]
MAIN_ROWS = 3 * 7 * 8
RIM_ROWS = 3 * 3 * 8
TABLE_ROWS = MAIN_ROWS + RIM_ROWS
F32 = jnp.float32
TILE = (8, CZ)


def tile_rows():
    return lax.broadcasted_iota(jnp.int32, TILE, 0)


def wide(row):
    return jnp.concatenate([row] * (PAD // CZ), axis=1)


def six_rows(ref):
    return jnp.concatenate([ref[0], ref[1], ref[2], jnp.zeros((2, PAD), ref.dtype)], axis=0)


def own_base(info_ref, base_ref):
    base = six_rows(base_ref)
    rows = lax.broadcasted_iota(jnp.int32, TILE, 0)
    start = jnp.where(rows < 2, info_ref[2], jnp.where(rows < 4, info_ref[3], 0.0))
    return base - wide(start.astype(jnp.int32))


def row_of(tile, r):
    return jnp.broadcast_to(tile[r : r + 1, :], (8, tile.shape[1]))


def choose(first, a, b):
    return jnp.where(first, a, b)


def stencil_kernels(offset):
    angle = offset * (math.pi / 2.0)
    c, s = jnp.cos(angle), jnp.sin(angle)
    return [(1.0 - s) * 0.25, (1.0 + c) * 0.25, (1.0 + s) * 0.25, (1.0 - c) * 0.25]


def pick(distance, kernels, r):
    out = jnp.zeros(distance.shape, F32)
    for n in range(4):
        out = jnp.where(distance == n, kernels[n][r : r + 1, :], out)
    return out


def vertex_tables(base, kernels, slot):
    rows = lax.broadcasted_iota(jnp.int32, (8, PAD), 0)
    x_value = jnp.where(rows < 6, rows, jnp.where(rows == 6, -1, 100))
    y_rim = jnp.where(rows < 2, rows + 8, jnp.where(rows == 2, -1, 100))
    base_x, base_y, base_z = [base[2 * a + slot : 2 * a + slot + 1, :] for a in range(3)]
    table_x = pick(x_value - base_x + 1, kernels, slot)
    table_y = pick(rows - base_y + 1, kernels, 2 + slot)
    table_rim = pick(y_rim - base_y + 1, kernels, 2 + slot)
    depth = lax.broadcasted_iota(jnp.int32, (CZ, PAD), 0)
    table_z = pick(jnp.bitwise_and(depth - base_z + 1, CZ - 1), kernels, 4 + slot)
    return table_x, table_y, table_rim, table_z


def halves(rows):
    high = rows.astype(jnp.bfloat16)
    return jnp.concatenate([high, (rows - high.astype(F32)).astype(jnp.bfloat16)], axis=0)


def vertex_force(offset, rest, scale, incidence):
    strain = offset - rest
    summed = jnp.dot(halves(strain), incidence[...], preferred_element_type=F32)
    summed = summed[:8] + summed[8:]
    rows = lax.broadcasted_iota(jnp.int32, summed.shape, 0)
    summed = jnp.where(rows == 6, 1.0, summed)
    pulled = lax.dot_general(
        halves(summed), incidence[...], (((1,), (1,)), ((), ())), preferred_element_type=F32
    )
    pulled = pulled[:8] + pulled[8:]
    return scale * (pulled - 3.0 * pulled[6:7] * strain)


def spread(offset, rest, scale, base, incidence, terms, main_ref, rim_ref, plane_ref, depth_ref):
    force = vertex_force(offset, rest, scale, incidence)
    kernels = stencil_kernels(offset)
    grid = None
    for slot in range(SLOTS):
        table_x, table_y, table_rim, table_z = vertex_tables(base, kernels, slot)
        for n, table in enumerate((table_x, table_y, table_rim)):
            plane_ref[slot, n] = table
        depth_ref[slot] = halves(table_z)
        for a in range(3):
            pushed = force[2 * a + slot : 2 * a + slot + 1, :]
            along_x = table_x * pushed
            for n in range(7):
                terms[(a * 7 + n) * 8 : (a * 7 + n + 1) * 8, :] = row_of(along_x, n) * table_y
            along_y = table_rim * pushed
            for n in range(3):
                start = MAIN_ROWS + (a * 3 + n) * 8
                terms[start : start + 8, :] = row_of(along_y, n) * table_x
        part = lax.dot_general(
            halves(terms[...]), depth_ref[slot], (((1,), (1,)), ((), ())), preferred_element_type=F32
        )
        part = part[:TABLE_ROWS] + part[TABLE_ROWS:]
        part = part[:, :CZ] + part[:, CZ:]
        grid = part if grid is None else grid + part
    main_ref[...] = grid[:MAIN_ROWS].reshape(3, 7, 8, CZ)
    rim_ref[...] = grid[MAIN_ROWS:].reshape(3, 3, 8, CZ)


def spread_messages(info_ref, rim_ref, first_ref, second_ref):
    even = info_ref[1] == 0.0
    for a in range(3):
        down = rim_ref[a, 2]
        for n in range(2):
            up = rim_ref[a, n]
            first_ref[a, n] = choose(even, up, down)
            second_ref[a, n] = choose(even, down, up)


def incidence_kernel(triangles_ref, incidence_ref):
    vertex = lax.broadcasted_iota(jnp.int32, incidence_ref.shape, 0)
    corners = [triangles_ref[corner : corner + 1, :] == vertex for corner in range(3)]
    hit = corners[0] | corners[1] | corners[2]
    incidence_ref[...] = jnp.where(hit, 1.0, 0.0).astype(jnp.bfloat16)


def spread_kernel(
    info_ref, offset_in, rest_in, base_in, incidence_ref,
    main_ref, first_ref, second_ref, plane_ref, depth_ref, offset_ref, rest_ref, base_ref, rim_ref, terms,
):
    offset_ref[...] = six_rows(offset_in)
    rest_ref[...] = six_rows(rest_in)
    base_ref[...] = own_base(info_ref, base_in)
    spread(
        offset_ref[...], rest_ref[...], wide(info_ref[4]), base_ref[...],
        incidence_ref, terms, main_ref, rim_ref, plane_ref, depth_ref,
    )
    spread_messages(info_ref, rim_ref, first_ref, second_ref)


def force_kernel(info_ref, main_ref, first_y, second_y, whole_ref, first_ref, second_ref):
    even_x = info_ref[0] == 0.0
    even_y = info_ref[1] == 0.0
    rows = tile_rows()
    for a in range(3):
        below = [choose(even_y, second_y[a, n], first_y[a, n]) for n in range(2)]
        above = choose(even_y, first_y[a, 0], second_y[a, 0])
        tiles = []
        for n in range(7):
            added = jnp.where(
                rows == 0,
                row_of(below[0], n),
                jnp.where(rows == 1, row_of(below[1], n), jnp.where(rows == 7, row_of(above, n), 0.0)),
            )
            tiles.append(main_ref[a, n] + added)
            whole_ref[a, n] = tiles[n]
        ups = [tiles[2], tiles[3], tiles[4], tiles[5]]
        downs = [tiles[6], tiles[0], tiles[1], tiles[2]]
        for t in range(4):
            first_ref[a, t] = choose(even_x, ups[t], downs[t])
            second_ref[a, t] = choose(even_x, downs[t], ups[t])


def moment_sums(members, rows):
    groups = {}
    for step in (0, 1, -1):
        of_step = [(q, t) for q, t in members if VELOCITIES[q][1] == step]
        sums = []
        for what in (None, 0, 2):
            total = None
            for q, t in of_step:
                weight = 1 if what is None else VELOCITIES[q][what]
                if weight == 0:
                    continue
                term = t if weight == 1 else -t
                total = term if total is None else total + term
            sums.append(jnp.zeros(TILE, F32) if total is None else total)
        groups[step] = sums
    up = [jnp.where(rows == 0, 0.0, t) for t in groups[1]]
    down = [jnp.where(rows == 7, 0.0, t) for t in groups[-1]]
    density, along_x, along_z = [groups[0][k] + up[k] + down[k] for k in range(3)]
    inside = [density, along_x, up[0] - down[0], along_z]
    edge = [
        jnp.where(rows == 0, groups[1][k], jnp.where(rows == 7, groups[-1][k], 0.0)) for k in range(3)
    ]
    return inside, edge


def pack_edges(edge):
    return edge[0] + pltpu.roll(edge[1], 2, 0) + pltpu.roll(edge[2], 4, 0)


def unpack_edges(packed, rows):
    keep = (rows == 0) | (rows == 7)
    tiles = [packed, pltpu.roll(packed, 6, 0), pltpu.roll(packed, 4, 0)]
    return [jnp.where(keep, t, 0.0) for t in tiles]


def push(tile, q):
    vector = VELOCITIES[q]
    if vector[2] != 0:
        tile = pltpu.roll(tile, vector[2] % CZ, 1)
    if vector[1] != 0:
        tile = pltpu.roll(tile, vector[1] % 8, 0)
    return tile


def momentum(current, a):
    total = None
    for q in range(19):
        if VELOCITIES[q][a] != 0:
            term = current[q] if VELOCITIES[q][a] == 1 else -current[q]
            total = term if total is None else total + term
    return total


def gained(density, carried, force, directions):
    inverse = 1.0 / density
    return gained_from(density, [(0.5 * force[a] + carried[a]) * inverse for a in range(3)], force, directions)


def gained_from(density, velocity, force, directions):
    squared = velocity[0] * velocity[0] + velocity[1] * velocity[1] + velocity[2] * velocity[2]
    working = velocity[0] * force[0] + velocity[1] * force[1] + velocity[2] * force[2]
    common = 1.0 - 1.5 * squared
    factor = 1.0 - 0.5 / RELAX
    out = {}
    for q in directions:
        vector = VELOCITIES[q]
        w = LATTICE_WEIGHTS[q]
        if q == 0:
            out[q] = (w / RELAX) * density * common - (3.0 * factor * w) * working
            continue
        along, pushed = None, None
        for a in range(3):
            if vector[a] == 0:
                continue
            u = velocity[a] if vector[a] == 1 else -velocity[a]
            f = force[a] if vector[a] == 1 else -force[a]
            along = u if along is None else along + u
            pushed = f if pushed is None else pushed + f
        equilibrium = (w / RELAX) * density * (common + along * (3.0 + 4.5 * along))
        source = (factor * w) * (3.0 * (pushed - working) + 9.0 * along * pushed)
        out[q] = equilibrium + source
    return out


def kept(current, walled, q):
    return jnp.where(walled, current[OPPOSITE[q]], (1.0 - 1.0 / RELAX) * current[q])


def halo_messages(info_ref, populations_ref, solid_ref, first_ref, second_ref):
    even_x = info_ref[0] == 0.0
    rows = tile_rows()
    current = [[populations_ref[q, x] for q in range(19)] for x in range(4)]
    walled = [solid_ref[x] != 0 for x in range(4)]

    def state(x):
        density = functools.reduce(lambda u, v: u + v, current[x])
        tiles = [density] + [momentum(current[x], a) for a in range(3)]
        return [jnp.where(walled[x], 0.0, t) for t in tiles]

    def carried(x, directions):
        return [(q, push(kept(current[x], walled[x], q), q)) for q in directions]

    def sums(members):
        inside, edge = moment_sums(members, rows)
        return inside + [pack_edges(edge)]

    up = state(2) + state(3)
    up += sums(carried(2, UP_X) + carried(3, FLAT_X))
    up += [t for _, t in carried(3, UP_X)]
    down = state(0) + state(1) + state(2)
    down += sums(carried(0, FLAT_X) + carried(1, DOWN_X))
    down += sums(carried(0, UP_X) + carried(1, FLAT_X) + carried(2, DOWN_X))
    down += [t for _, t in carried(0, DOWN_X)]
    for t in range(27):
        u = up[t] if t < 18 else down[t]
        first_ref[t] = choose(even_x, u, down[t])
        second_ref[t] = choose(even_x, down[t], u)


def halo_kernel(
    stiffness_ref, occupied_ref, populations_in, solid_in,
    info_ref, populations_ref, solid_ref, first_ref, second_ref,
):
    place_x = lax.axis_index("gx")
    place_y = lax.axis_index("gy")
    even_row = lax.rem(tile_rows(), 2) == 0

    def by_slot(row):
        return jnp.where(even_row, row[:, 0:1], row[:, 1:2])

    held = by_slot(occupied_ref[...].astype(F32))
    info_ref[4] = by_slot(stiffness_ref[...]) * held
    info_ref[5] = held
    numbers = (lax.rem(place_x, 2), lax.rem(place_y, 2), place_x * CX, place_y * CY)
    for n, number in enumerate(numbers):
        info_ref[n] = jnp.full(TILE, number, jnp.int32).astype(F32)
    populations_ref[...] = populations_in[...]
    solid_ref[...] = solid_in[...]
    halo_messages(info_ref, populations_ref, solid_ref, first_ref, second_ref)


def collide_kernel(
    info_ref, populations_ref, solid_ref, whole_ref, first_x, second_x, first_h, second_h,
    stepped_ref, inside_ref, leaving_ref, first_ref, second_ref, edges, up_tiles, down_tiles,
):
    even_x = info_ref[0] == 0.0
    even_y = info_ref[1] == 0.0
    rows = tile_rows()
    below = [choose(even_x, second_h[t], first_h[t]) for t in range(18)]
    above = [choose(even_x, first_h[t], second_h[t]) for t in range(27)]
    from_below = [[choose(even_x, second_x[a, t], first_x[a, t]) for t in range(4)] for a in range(3)]
    from_above = [[choose(even_x, first_x[a, t], second_x[a, t]) for t in range(4)] for a in range(3)]
    force = {}
    for x in range(-2, 7):
        parts = []
        for a in range(3):
            terms = []
            if -1 <= x <= 5:
                terms.append(whole_ref[a, X_ORDER.index(x)])
            if x < 2:
                terms.append(from_below[a][x + 2])
            if x > 2:
                terms.append(from_above[a][x - 3])
            parts.append(functools.reduce(lambda u, v: u + v, terms))
        force[x] = parts

    def place(q, x, tile):
        stepped_ref[(q * 4 + x) * 8 : (q * 4 + x + 1) * 8, :] = tile

    out_up, out_down = [], []
    for x in range(4):
        current = [populations_ref[q, x] for q in range(19)]
        walled = solid_ref[x] != 0
        density = functools.reduce(lambda u, v: u + v, current)
        new = gained(density, [momentum(current, a) for a in range(3)], force[x], range(19))
        for q in range(19):
            relaxed = jnp.where(walled, current[OPPOSITE[q]], (1.0 - 1.0 / RELAX) * current[q] + new[q])
            relaxed = push(relaxed, q)
            target = x + VELOCITIES[q][0]
            if target == 4:
                out_up.append((q, relaxed))
            elif target == -1:
                out_down.append((q, relaxed))
            else:
                place(q, target, relaxed)

    def halo(x, tiles, directions):
        fluid = tiles[0] != 0.0
        pulled = [jnp.where(fluid, f, 0.0) for f in force[x]]
        density = tiles[0]
        inverse = 1.0 / jnp.where(fluid, density, 1.0)
        velocity = [(0.5 * pulled[a] + tiles[1 + a]) * inverse for a in range(3)]
        new = gained_from(density, velocity, pulled, directions)
        return {q: push(new[q], q) for q in directions}

    def members(part, directions):
        return [(q, part[q]) for q in directions]

    before = halo(-2, below[0:4], UP_X)
    last = halo(-1, below[4:8], FLAT_X + UP_X)
    for n, q in enumerate(UP_X):
        place(q, 0, below[13 + n] + last[q])
    reached = {-1: (below[8:13], members(before, UP_X) + members(last, FLAT_X) + out_down)}
    four = halo(4, above[0:4], range(19))
    five = halo(5, above[4:8], FLAT_X + DOWN_X)
    six = halo(6, above[8:12], DOWN_X)
    for n, q in enumerate(DOWN_X):
        place(q, 3, above[22 + n] + four[q])
    reached[4] = (above[12:17], members(four, FLAT_X) + members(five, DOWN_X) + out_up)
    reached[5] = (
        above[17:22],
        members(four, UP_X) + members(five, FLAT_X) + members(six, DOWN_X),
    )
    for n, x in enumerate(X_ORDER):
        if 0 <= x < 4:
            every = [(q, stepped_ref[(q * 4 + x) * 8 : (q * 4 + x + 1) * 8, :]) for q in range(19)]
            inside, edge = moment_sums(every, rows)
        else:
            received, arrived = reached[x]
            inside, edge = moment_sums(arrived, rows)
            inside = [u + v for u, v in zip(inside, received[:4])]
            edge = [u + v for u, v in zip(edge, unpack_edges(received[4], rows))]
        for k in range(3):
            inside[1 + k] = inside[1 + k] + 0.5 * force[x][k]
        for k in range(4):
            inside_ref[(k * 8 + n) * 8 : (k * 8 + n + 1) * 8, :] = inside[k]
        for k in range(3):
            edges[(k * 8 + n) * 8 : (k * 8 + n + 1) * 8, :] = edge[k]
    for k in range(4):
        inside_ref[(k * 8 + 7) * 8 : (k * 8 + 8) * 8, :] = jnp.ones(TILE, F32)
    for k in range(3):
        edges[(k * 8 + 7) * 8 : (k * 8 + 8) * 8, :] = jnp.zeros(TILE, F32)
    for k in range(3):
        up = edges[pl.ds(k * 64, 8, stride=8), :]
        down = edges[pl.ds(k * 64 + 7, 8, stride=8), :]
        leaving_ref[k] = up
        leaving_ref[3 + k] = down
        up_tiles[k] = up
        down_tiles[k] = down
    for n in range(5):
        t, r = (n, 0) if n < 4 else (3, 4)
        up_tiles[t, r : r + 4, :] = stepped_ref[pl.ds(UP_Y[n] * 32, 4, stride=8), :]
        down_tiles[t, r : r + 4, :] = stepped_ref[pl.ds(DOWN_Y[n] * 32 + 7, 4, stride=8), :]
    for k in range(4):
        up_tiles[4 + k] = inside_ref[pl.ds(k * 64 + 7, 8, stride=8), :]
        down_tiles[4 + k] = inside_ref[pl.ds(k * 64, 8, stride=8), :]
    inverse = 1.0 / inside_ref[pl.ds(1, 8, stride=8), :]
    for k in range(3):
        down_tiles[8 + k] = inside_ref[pl.ds((k + 1) * 64 + 1, 8, stride=8), :] * inverse
    for t in range(11):
        u = up_tiles[t] if t < 8 else down_tiles[t]
        d = down_tiles[t]
        first_ref[t] = choose(even_y, u, d)
        second_ref[t] = choose(even_y, d, u)


def crossing(tiles, n, x):
    return row_of(tiles[n], x) if n < 4 else row_of(tiles[3], 4 + x)


def finish_fluid(info_ref, stepped_ref, inside_ref, leaving_ref, first_y, second_y, out_ref, flow):
    even_y = info_ref[1] == 0.0
    rows = tile_rows()
    below = [choose(even_y, second_y[t], first_y[t]) for t in range(8)]
    above = [choose(even_y, first_y[t], second_y[t]) for t in range(11)]
    for q in range(19):
        for x in range(4):
            s = stepped_ref[(q * 4 + x) * 8 : (q * 4 + x + 1) * 8, :]
            if q in UP_Y:
                s = jnp.where(rows == 0, crossing(below, UP_Y.index(q), x), s)
            if q in DOWN_Y:
                s = jnp.where(rows == 7, crossing(above, DOWN_Y.index(q), x), s)
            out_ref[q, x] = s

    def arriving(tiles, members):
        crossed = list(tiles[:4]) + [pltpu.roll(tiles[3], 4, 0)]
        out = []
        for k, what in enumerate((None, 0, 2)):
            total = None
            for n, q in enumerate(members):
                weight = 1 if what is None else VELOCITIES[q][what]
                if weight:
                    term = crossed[n] if weight == 1 else -crossed[n]
                    total = term if total is None else total + term
            out.append(jnp.where(rows < 4, total, tiles[k]))
        return [out[0], out[1], None, out[2]]

    from_below = arriving(below, UP_Y)
    from_above = arriving(above, DOWN_Y)
    from_below[2] = from_below[0]
    from_above[2] = -from_above[0]
    for n in range(7):
        total = []
        for k in range(4):
            t = inside_ref[(k * 8 + n) * 8 : (k * 8 + n + 1) * 8, :]
            t = t + jnp.where(
                rows == 0,
                row_of(from_below[k], n),
                jnp.where(rows == 7, row_of(from_above[k], n), 0.0),
            )
            total.append(t)
        inverse = 1.0 / total[0]
        for a in range(3):
            flow[(a * 7 + n) * 8 : (a * 7 + n + 1) * 8, :] = total[1 + a] * inverse
    up = [leaving_ref[0], leaving_ref[1], leaving_ref[0], leaving_ref[2]]
    down = [leaving_ref[3], leaving_ref[4], -leaving_ref[3], leaving_ref[5]]
    rims = (
        (0, [above[4 + k] + up[k] for k in range(4)]),
        (2, [below[4 + k] + down[k] for k in range(4)]),
    )
    for n, total in rims:
        inverse = 1.0 / jnp.where(rows == 7, 1.0, total[0])
        for a in range(3):
            start = MAIN_ROWS + (a * 3 + n) * 8
            flow[start : start + 8, :] = jnp.where(rows == 7, 0.0, total[1 + a] * inverse)
    for a in range(3):
        start = MAIN_ROWS + (a * 3 + 1) * 8
        flow[start : start + 8, :] = above[8 + a]


def sample(offset, live, plane_ref, depth_ref, flow):
    moved = [None] * 8
    zero = jnp.zeros((1, PAD), F32)
    both = halves(flow[...])
    both = jnp.concatenate([both, both], axis=1)
    for slot in range(SLOTS):
        table_x, table_y, table_rim = [plane_ref[slot, n] for n in range(3)]
        along = jnp.dot(both, depth_ref[slot], preferred_element_type=F32)
        along = along[:TABLE_ROWS] + along[TABLE_ROWS:]
        for a in range(3):
            inner = None
            for n in range(7):
                tile = along[(a * 7 + n) * 8 : (a * 7 + n + 1) * 8, :]
                term = tile * row_of(table_x, n)
                inner = term if inner is None else inner + term
            total = inner * table_y
            outer = None
            for n in range(3):
                start = MAIN_ROWS + (a * 3 + n) * 8
                term = along[start : start + 8, :] * row_of(table_rim, n)
                outer = term if outer is None else outer + term
            total = total + outer * table_x
            moved[2 * a + slot] = jnp.sum(total, axis=0, keepdims=True)
    stacked = jnp.concatenate(moved[:6] + [zero, zero], axis=0)
    return offset + live * stacked


def finish_kernel(
    info_ref, stepped_ref, inside_ref, leaving_ref, first_y, second_y, solid_ref,
    out_ref, flow_ref, first_ref, second_ref,
):
    finish_fluid(info_ref, stepped_ref, inside_ref, leaving_ref, first_y, second_y, out_ref, flow_ref)
    halo_messages(info_ref, out_ref, solid_ref, first_ref, second_ref)


def next_kernel(
    info_ref, flow_ref, plane_in, depth_in, offset_ref, rest_ref, base_ref, incidence_ref,
    main_ref, first_ref, second_ref, plane_ref, depth_ref, offset_out, rim_ref, terms,
):
    offset = sample(offset_ref[...], wide(info_ref[5]), plane_in, depth_in, flow_ref)
    offset_out[...] = offset
    spread(
        offset, rest_ref[...], wide(info_ref[4]), base_ref[...],
        incidence_ref, terms, main_ref, rim_ref, plane_ref, depth_ref,
    )
    spread_messages(info_ref, rim_ref, first_ref, second_ref)


def last_kernel(
    info_ref, stepped_ref, inside_ref, leaving_ref, first_y, second_y, plane_in, depth_in, offset_ref,
    out_ref, offset_out, flow,
):
    finish_fluid(info_ref, stepped_ref, inside_ref, leaving_ref, first_y, second_y, out_ref, flow)
    offset = sample(offset_ref[...], wide(info_ref[5]), plane_in, depth_in, flow)
    for a in range(3):
        offset_out[a] = offset[2 * a : 2 * a + 2]


INTERPRET = False


def call(kernel, outs, scratch, *operands):
    return pl.pallas_call(
        kernel,
        out_shape=[jax.ShapeDtypeStruct(shape, dtype) for shape, dtype in outs],
        in_specs=[pl.BlockSpec(memory_space=pltpu.VMEM)] * len(operands),
        out_specs=[pl.BlockSpec(memory_space=pltpu.VMEM)] * len(outs),
        scratch_shapes=[pltpu.VMEM(shape, dtype) for shape, dtype in scratch],
        compiler_params=pltpu.CompilerParams(vmem_limit_bytes=24 * 1024 * 1024),
        interpret=INTERPRET,
    )(*operands)


def partner(index, kind, size):
    return (index + 1) % size if (index + kind) % 2 == 0 else (index - 1) % size


def exchange(first, second, axis):
    size = lax.axis_size(axis)
    out = [None, None]
    for kind, message in ((1, second), (0, first)):
        pairs = [(i, partner(i, kind, size)) for i in range(size)]
        out[kind] = lax.ppermute(message, axis, pairs)
    return out


SPREAD_OUT = [
    ((3, 7, 8, CZ), F32),
    ((3, 2, 8, CZ), F32),
    ((3, 2, 8, CZ), F32),
    ((SLOTS, 3, 8, PAD), F32),
    ((SLOTS, 2 * CZ, PAD), jnp.bfloat16),
]
HALO_OUT = [((27, 8, CZ), F32)] * 2
STEPPED = ((19, 4, 8, CZ), F32)


def steps(populations, solid, base_cell, offset, rest_displacement, stiffness, occupied, triangles):
    stored = (3, SLOTS, PAD)
    rows = (8, PAD)
    scratch = [((3, 3, 8, CZ), F32), ((TABLE_ROWS, PAD), F32)]
    flow_out = ((TABLE_ROWS, CZ), F32)
    corners = triangles.T
    (incidence,) = call(incidence_kernel, [((PAD, corners.shape[1]), jnp.bfloat16)], [], corners)
    info, populations, solid, first_h, second_h = call(
        halo_kernel,
        [((6, 8, CZ), F32), STEPPED, (solid.shape, jnp.int32)] + HALO_OUT, [],
        stiffness.reshape(1, SLOTS), occupied.reshape(1, SLOTS), populations, solid,
    )
    main, first, second, plane, depth, where, rest, base = call(
        spread_kernel, SPREAD_OUT + [(rows, F32), (rows, F32), (rows, jnp.int32)], scratch,
        info, offset.reshape(stored), rest_displacement.reshape(stored), base_cell.reshape(stored),
        incidence,
    )
    for substep in range(SUBSTEPS):
        first_h, second_h = exchange(first_h, second_h, "gx")
        first, second = exchange(first, second, "gy")
        whole, first, second = call(
            force_kernel, [((3, 7, 8, CZ), F32), ((3, 4, 8, CZ), F32), ((3, 4, 8, CZ), F32)], [],
            info, main, first, second,
        )
        first, second = exchange(first, second, "gx")
        stepped, inside, leaving, first, second = call(
            collide_kernel,
            [
                ((19 * 4 * 8, CZ), F32), ((4 * 8 * 8, CZ), F32), ((6, 8, CZ), F32),
                ((11, 8, CZ), F32), ((11, 8, CZ), F32),
            ],
            [((3 * 8 * 8, CZ), F32), ((8, 8, CZ), F32), ((11, 8, CZ), F32)],
            info, populations, solid, whole, first, second, first_h, second_h,
        )
        first, second = exchange(first, second, "gy")
        fluid = (info, stepped, inside, leaving, first, second)
        if substep < SUBSTEPS - 1:
            populations, flow, first_h, second_h = call(
                finish_kernel, [STEPPED, flow_out] + HALO_OUT, [], *fluid, solid
            )
            main, first, second, plane, depth, where = call(
                next_kernel, SPREAD_OUT + [(rows, F32)], scratch,
                info, flow, plane, depth, where, rest, base, incidence,
            )
        else:
            populations, where = call(last_kernel, [STEPPED, (stored, F32)], [flow_out], *fluid, plane, depth, where)
    return populations, where.reshape(offset.shape)


def solution(mesh):
    in_specs = (
        P(None, "gx", "gy", None),
        P("gx", "gy", None),
        P(None, "gx", "gy", None, None),
        P(None, "gx", "gy", None, None),
        P(None, "gx", "gy", None, None),
        P("gx", "gy", None),
        P("gx", "gy", None),
        P(),
    )
    out_specs = (P(None, "gx", "gy", None), P(None, "gx", "gy", None, None))
    return jax.shard_map(steps, mesh=mesh, in_specs=in_specs, out_specs=out_specs, check_vma=False)
```

```python
import functools
import math

import jax
import jax.numpy as jnp
from jax import lax
from jax.experimental import pallas as pl
from jax.experimental.pallas import tpu as pltpu
from jax.sharding import PartitionSpec as P


SUBSTEPS = 3

VELOCITIES = [
    [0, 0, 0],
    [1, 0, 0],
    [-1, 0, 0],
    [0, 1, 0],
    [0, -1, 0],
    [0, 0, 1],
    [0, 0, -1],
    [1, 1, 0],
    [-1, -1, 0],
    [1, -1, 0],
    [-1, 1, 0],
    [1, 0, 1],
    [-1, 0, -1],
    [1, 0, -1],
    [-1, 0, 1],
    [0, 1, 1],
    [0, -1, -1],
    [0, 1, -1],
    [0, -1, 1],
]
OPPOSITE = [0, 2, 1, 4, 3, 6, 5, 8, 7, 10, 9, 12, 11, 14, 13, 16, 15, 18, 17]
LATTICE_WEIGHTS = [1.0 / 3.0] + [1.0 / 18.0] * 6 + [1.0 / 36.0] * 12
RELAX = 0.8
CX, CY, CZ = 4, 8, 128
SLOTS, PAD = 2, 768
UP_X = [q for q in range(19) if VELOCITIES[q][0] == 1]
DOWN_X = [q for q in range(19) if VELOCITIES[q][0] == -1]
UP_Y = [q for q in range(19) if VELOCITIES[q][1] == 1]
DOWN_Y = [q for q in range(19) if VELOCITIES[q][1] == -1]
FLAT_X = [q for q in range(19) if VELOCITIES[q][0] == 0]
X_ORDER = [0, 1, 2, 3, 4, 5, -1]
MAIN_ROWS = 3 * 7 * 8
RIM_ROWS = 3 * 3 * 8
TABLE_ROWS = MAIN_ROWS + RIM_ROWS
LATE_ROWS = 3 * 5 * 8
F32 = jnp.float32
TILE = (8, CZ)


def tile_rows():
    return lax.broadcasted_iota(jnp.int32, TILE, 0)


def wide(row):
    return jnp.concatenate([row] * (PAD // CZ), axis=1)


def six_rows(ref):
    return jnp.concatenate([ref[0], ref[1], ref[2], jnp.zeros((2, PAD), ref.dtype)], axis=0)


def own_base(info_ref, base_ref):
    base = six_rows(base_ref)
    rows = lax.broadcasted_iota(jnp.int32, TILE, 0)
    start = jnp.where(rows < 2, info_ref[2], jnp.where(rows < 4, info_ref[3], 0.0))
    return base - wide(start.astype(jnp.int32))


def row_of(tile, r):
    return jnp.broadcast_to(tile[r : r + 1, :], (8, tile.shape[1]))


def choose(first, a, b):
    return jnp.where(first, a, b)


def stencil_kernels(offset):
    angle = offset * (math.pi / 2.0)
    c, s = jnp.cos(angle), jnp.sin(angle)
    return [(1.0 - s) * 0.25, (1.0 + c) * 0.25, (1.0 + s) * 0.25, (1.0 - c) * 0.25]


def pick(distance, kernels, r):
    out = jnp.zeros(distance.shape, F32)
    for n in range(4):
        out = jnp.where(distance == n, kernels[n][r : r + 1, :], out)
    return out


def vertex_tables(base, kernels, slot):
    rows = lax.broadcasted_iota(jnp.int32, (8, PAD), 0)
    x_value = jnp.where(rows < 6, rows, jnp.where(rows == 6, -1, 100))
    y_rim = jnp.where(rows < 2, rows + 8, jnp.where(rows == 2, -1, 100))
    y_rim = jnp.where(rows == 3, 0, jnp.where(rows == 4, 7, y_rim))
    base_x, base_y, base_z = [base[2 * a + slot : 2 * a + slot + 1, :] for a in range(3)]
    table_x = pick(x_value - base_x + 1, kernels, slot)
    table_y = pick(rows - base_y + 1, kernels, 2 + slot)
    table_rim = pick(y_rim - base_y + 1, kernels, 2 + slot)
    depth = lax.broadcasted_iota(jnp.int32, (CZ, PAD), 0)
    table_z = pick(jnp.bitwise_and(depth - base_z + 1, CZ - 1), kernels, 4 + slot)
    return table_x, table_y, table_rim, table_z


def halves(rows):
    high = rows.astype(jnp.bfloat16)
    return jnp.concatenate([high, (rows - high.astype(F32)).astype(jnp.bfloat16)], axis=0)


def vertex_force(offset, rest, scale, incidence):
    strain = offset - rest
    summed = jnp.dot(halves(strain), incidence[...], preferred_element_type=F32)
    summed = summed[:8] + summed[8:]
    rows = lax.broadcasted_iota(jnp.int32, summed.shape, 0)
    summed = jnp.where(rows == 6, 1.0, summed)
    pulled = lax.dot_general(
        halves(summed), incidence[...], (((1,), (1,)), ((), ())), preferred_element_type=F32
    )
    pulled = pulled[:8] + pulled[8:]
    return scale * (pulled - 3.0 * pulled[6:7] * strain)


def spread(offset, rest, scale, base, incidence, terms, main_ref, rim_ref, plane_ref, depth_ref):
    force = vertex_force(offset, rest, scale, incidence)
    kernels = stencil_kernels(offset)
    grid = None
    for slot in range(SLOTS):
        table_x, table_y, table_rim, table_z = vertex_tables(base, kernels, slot)
        for n, table in enumerate((table_x, table_y, table_rim)):
            plane_ref[slot, n] = table
        depth_ref[slot] = halves(table_z)
        for a in range(3):
            pushed = force[2 * a + slot : 2 * a + slot + 1, :]
            along_x = table_x * pushed
            for n in range(7):
                terms[(a * 7 + n) * 8 : (a * 7 + n + 1) * 8, :] = row_of(along_x, n) * table_y
            along_y = table_rim * pushed
            for n in range(3):
                start = MAIN_ROWS + (a * 3 + n) * 8
                terms[start : start + 8, :] = row_of(along_y, n) * table_x
        part = lax.dot_general(
            halves(terms[...]), depth_ref[slot], (((1,), (1,)), ((), ())), preferred_element_type=F32
        )
        part = part[:TABLE_ROWS] + part[TABLE_ROWS:]
        part = part[:, :CZ] + part[:, CZ:]
        grid = part if grid is None else grid + part
    main_ref[...] = grid[:MAIN_ROWS].reshape(3, 7, 8, CZ)
    rim_ref[...] = grid[MAIN_ROWS:].reshape(3, 3, 8, CZ)


def spread_messages(info_ref, rim_ref, first_ref, second_ref):
    even = info_ref[1] == 0.0
    for a in range(3):
        down = rim_ref[a, 2]
        for n in range(2):
            up = rim_ref[a, n]
            first_ref[a, n] = choose(even, up, down)
            second_ref[a, n] = choose(even, down, up)


def incidence_kernel(triangles_ref, incidence_ref):
    vertex = lax.broadcasted_iota(jnp.int32, incidence_ref.shape, 0)
    corners = [triangles_ref[corner : corner + 1, :] == vertex for corner in range(3)]
    hit = corners[0] | corners[1] | corners[2]
    incidence_ref[...] = jnp.where(hit, 1.0, 0.0).astype(jnp.bfloat16)


def spread_kernel(
    info_ref, offset_in, rest_in, base_in, incidence_ref,
    main_ref, first_ref, second_ref, plane_ref, depth_ref, offset_ref, rest_ref, base_ref, rim_ref, terms,
):
    offset_ref[...] = six_rows(offset_in)
    rest_ref[...] = six_rows(rest_in)
    base_ref[...] = own_base(info_ref, base_in)
    spread(
        offset_ref[...], rest_ref[...], wide(info_ref[4]), base_ref[...],
        incidence_ref, terms, main_ref, rim_ref, plane_ref, depth_ref,
    )
    spread_messages(info_ref, rim_ref, first_ref, second_ref)


def force_kernel(info_ref, main_ref, first_y, second_y, whole_ref, first_ref, second_ref):
    even_x = info_ref[0] == 0.0
    even_y = info_ref[1] == 0.0
    rows = tile_rows()
    for a in range(3):
        below = [choose(even_y, second_y[a, n], first_y[a, n]) for n in range(2)]
        above = choose(even_y, first_y[a, 0], second_y[a, 0])
        tiles = []
        for n in range(7):
            added = jnp.where(
                rows == 0,
                row_of(below[0], n),
                jnp.where(rows == 1, row_of(below[1], n), jnp.where(rows == 7, row_of(above, n), 0.0)),
            )
            tiles.append(main_ref[a, n] + added)
            whole_ref[a, n] = tiles[n]
        ups = [tiles[2], tiles[3], tiles[4], tiles[5]]
        downs = [tiles[6], tiles[0], tiles[1], tiles[2]]
        for t in range(4):
            first_ref[a, t] = choose(even_x, ups[t], downs[t])
            second_ref[a, t] = choose(even_x, downs[t], ups[t])


def moment_sums(members, rows):
    groups = {}
    for step in (0, 1, -1):
        of_step = [(q, t) for q, t in members if VELOCITIES[q][1] == step]
        sums = []
        for what in (None, 0, 2):
            total = None
            for q, t in of_step:
                weight = 1 if what is None else VELOCITIES[q][what]
                if weight == 0:
                    continue
                term = t if weight == 1 else -t
                total = term if total is None else total + term
            sums.append(jnp.zeros(TILE, F32) if total is None else total)
        groups[step] = sums
    up = [jnp.where(rows == 0, 0.0, t) for t in groups[1]]
    down = [jnp.where(rows == 7, 0.0, t) for t in groups[-1]]
    density, along_x, along_z = [groups[0][k] + up[k] + down[k] for k in range(3)]
    inside = [density, along_x, up[0] - down[0], along_z]
    edge = [
        jnp.where(rows == 0, groups[1][k], jnp.where(rows == 7, groups[-1][k], 0.0)) for k in range(3)
    ]
    return inside, edge


def pack_edges(edge):
    return edge[0] + pltpu.roll(edge[1], 2, 0) + pltpu.roll(edge[2], 4, 0)


def unpack_edges(packed, rows):
    keep = (rows == 0) | (rows == 7)
    tiles = [packed, pltpu.roll(packed, 6, 0), pltpu.roll(packed, 4, 0)]
    return [jnp.where(keep, t, 0.0) for t in tiles]


def push(tile, q):
    vector = VELOCITIES[q]
    if vector[2] != 0:
        tile = pltpu.roll(tile, vector[2] % CZ, 1)
    if vector[1] != 0:
        tile = pltpu.roll(tile, vector[1] % 8, 0)
    return tile


def momentum(current, a):
    total = None
    for q in range(19):
        if VELOCITIES[q][a] != 0:
            term = current[q] if VELOCITIES[q][a] == 1 else -current[q]
            total = term if total is None else total + term
    return total


def gained(density, carried, force, directions):
    inverse = 1.0 / density
    return gained_from(density, [(0.5 * force[a] + carried[a]) * inverse for a in range(3)], force, directions)


def gained_from(density, velocity, force, directions):
    squared = velocity[0] * velocity[0] + velocity[1] * velocity[1] + velocity[2] * velocity[2]
    working = velocity[0] * force[0] + velocity[1] * force[1] + velocity[2] * force[2]
    common = 1.0 - 1.5 * squared
    factor = 1.0 - 0.5 / RELAX
    out = {}
    for q in directions:
        vector = VELOCITIES[q]
        w = LATTICE_WEIGHTS[q]
        if q == 0:
            out[q] = (w / RELAX) * density * common - (3.0 * factor * w) * working
            continue
        along, pushed = None, None
        for a in range(3):
            if vector[a] == 0:
                continue
            u = velocity[a] if vector[a] == 1 else -velocity[a]
            f = force[a] if vector[a] == 1 else -force[a]
            along = u if along is None else along + u
            pushed = f if pushed is None else pushed + f
        equilibrium = (w / RELAX) * density * (common + along * (3.0 + 4.5 * along))
        source = (factor * w) * (3.0 * (pushed - working) + 9.0 * along * pushed)
        out[q] = equilibrium + source
    return out


def kept(current, walled, q):
    return jnp.where(walled, current[OPPOSITE[q]], (1.0 - 1.0 / RELAX) * current[q])


def halo_messages(info_ref, populations_ref, solid_ref, first_ref, second_ref):
    even_x = info_ref[0] == 0.0
    rows = tile_rows()
    current = [[populations_ref[q, x] for q in range(19)] for x in range(4)]
    walled = [solid_ref[x] != 0 for x in range(4)]

    def state(x):
        density = functools.reduce(lambda u, v: u + v, current[x])
        tiles = [density] + [momentum(current[x], a) for a in range(3)]
        return [jnp.where(walled[x], 0.0, t) for t in tiles]

    def carried(x, directions):
        return [(q, push(kept(current[x], walled[x], q), q)) for q in directions]

    def sums(members):
        inside, edge = moment_sums(members, rows)
        return inside + [pack_edges(edge)]

    up = state(2) + state(3)
    up += sums(carried(2, UP_X) + carried(3, FLAT_X))
    up += [t for _, t in carried(3, UP_X)]
    down = state(0) + state(1) + state(2)
    down += sums(carried(0, FLAT_X) + carried(1, DOWN_X))
    down += sums(carried(0, UP_X) + carried(1, FLAT_X) + carried(2, DOWN_X))
    down += [t for _, t in carried(0, DOWN_X)]
    for t in range(27):
        u = up[t] if t < 18 else down[t]
        first_ref[t] = choose(even_x, u, down[t])
        second_ref[t] = choose(even_x, down[t], u)


def halo_kernel(
    stiffness_ref, occupied_ref, populations_in, solid_in,
    info_ref, populations_ref, solid_ref, first_ref, second_ref,
):
    place_x = lax.axis_index("gx")
    place_y = lax.axis_index("gy")
    even_row = lax.rem(tile_rows(), 2) == 0

    def by_slot(row):
        return jnp.where(even_row, row[:, 0:1], row[:, 1:2])

    held = by_slot(occupied_ref[...].astype(F32))
    info_ref[4] = by_slot(stiffness_ref[...]) * held
    info_ref[5] = held
    numbers = (lax.rem(place_x, 2), lax.rem(place_y, 2), place_x * CX, place_y * CY)
    for n, number in enumerate(numbers):
        info_ref[n] = jnp.full(TILE, number, jnp.int32).astype(F32)
    populations_ref[...] = populations_in[...]
    solid_ref[...] = solid_in[...]
    halo_messages(info_ref, populations_ref, solid_ref, first_ref, second_ref)


def collide_kernel(
    info_ref, populations_ref, solid_ref, whole_ref, first_x, second_x, first_h, second_h,
    stepped_ref, inside_ref, leaving_ref, first_ref, second_ref, edges, up_tiles, down_tiles,
):
    even_x = info_ref[0] == 0.0
    even_y = info_ref[1] == 0.0
    rows = tile_rows()
    below = [choose(even_x, second_h[t], first_h[t]) for t in range(18)]
    above = [choose(even_x, first_h[t], second_h[t]) for t in range(27)]
    from_below = [[choose(even_x, second_x[a, t], first_x[a, t]) for t in range(4)] for a in range(3)]
    from_above = [[choose(even_x, first_x[a, t], second_x[a, t]) for t in range(4)] for a in range(3)]
    force = {}
    for x in range(-2, 7):
        parts = []
        for a in range(3):
            terms = []
            if -1 <= x <= 5:
                terms.append(whole_ref[a, X_ORDER.index(x)])
            if x < 2:
                terms.append(from_below[a][x + 2])
            if x > 2:
                terms.append(from_above[a][x - 3])
            parts.append(functools.reduce(lambda u, v: u + v, terms))
        force[x] = parts

    def place(q, x, tile):
        stepped_ref[(q * 4 + x) * 8 : (q * 4 + x + 1) * 8, :] = tile

    out_up, out_down = [], []
    for x in range(4):
        current = [populations_ref[q, x] for q in range(19)]
        walled = solid_ref[x] != 0
        density = functools.reduce(lambda u, v: u + v, current)
        new = gained(density, [momentum(current, a) for a in range(3)], force[x], range(19))
        for q in range(19):
            relaxed = jnp.where(walled, current[OPPOSITE[q]], (1.0 - 1.0 / RELAX) * current[q] + new[q])
            relaxed = push(relaxed, q)
            target = x + VELOCITIES[q][0]
            if target == 4:
                out_up.append((q, relaxed))
            elif target == -1:
                out_down.append((q, relaxed))
            else:
                place(q, target, relaxed)

    def halo(x, tiles, directions):
        fluid = tiles[0] != 0.0
        pulled = [jnp.where(fluid, f, 0.0) for f in force[x]]
        density = tiles[0]
        inverse = 1.0 / jnp.where(fluid, density, 1.0)
        velocity = [(0.5 * pulled[a] + tiles[1 + a]) * inverse for a in range(3)]
        new = gained_from(density, velocity, pulled, directions)
        return {q: push(new[q], q) for q in directions}

    def members(part, directions):
        return [(q, part[q]) for q in directions]

    before = halo(-2, below[0:4], UP_X)
    last = halo(-1, below[4:8], FLAT_X + UP_X)
    for n, q in enumerate(UP_X):
        place(q, 0, below[13 + n] + last[q])
    reached = {-1: (below[8:13], members(before, UP_X) + members(last, FLAT_X) + out_down)}
    four = halo(4, above[0:4], range(19))
    five = halo(5, above[4:8], FLAT_X + DOWN_X)
    six = halo(6, above[8:12], DOWN_X)
    for n, q in enumerate(DOWN_X):
        place(q, 3, above[22 + n] + four[q])
    reached[4] = (above[12:17], members(four, FLAT_X) + members(five, DOWN_X) + out_up)
    reached[5] = (
        above[17:22],
        members(four, UP_X) + members(five, FLAT_X) + members(six, DOWN_X),
    )
    for n, x in enumerate(X_ORDER):
        if 0 <= x < 4:
            every = [(q, stepped_ref[(q * 4 + x) * 8 : (q * 4 + x + 1) * 8, :]) for q in range(19)]
            inside, edge = moment_sums(every, rows)
        else:
            received, arrived = reached[x]
            inside, edge = moment_sums(arrived, rows)
            inside = [u + v for u, v in zip(inside, received[:4])]
            edge = [u + v for u, v in zip(edge, unpack_edges(received[4], rows))]
        for k in range(3):
            inside[1 + k] = inside[1 + k] + 0.5 * force[x][k]
        for k in range(4):
            inside_ref[(k * 8 + n) * 8 : (k * 8 + n + 1) * 8, :] = inside[k]
        for k in range(3):
            edges[(k * 8 + n) * 8 : (k * 8 + n + 1) * 8, :] = edge[k]
    for k in range(4):
        inside_ref[(k * 8 + 7) * 8 : (k * 8 + 8) * 8, :] = jnp.ones(TILE, F32)
    for k in range(3):
        edges[(k * 8 + 7) * 8 : (k * 8 + 8) * 8, :] = jnp.zeros(TILE, F32)
    for k in range(3):
        up = edges[pl.ds(k * 64, 8, stride=8), :]
        down = edges[pl.ds(k * 64 + 7, 8, stride=8), :]
        leaving_ref[k] = up
        leaving_ref[3 + k] = down
        up_tiles[k] = up
        down_tiles[k] = down
    for n in range(5):
        t, r = (n, 0) if n < 4 else (3, 4)
        up_tiles[t, r : r + 4, :] = stepped_ref[pl.ds(UP_Y[n] * 32, 4, stride=8), :]
        down_tiles[t, r : r + 4, :] = stepped_ref[pl.ds(DOWN_Y[n] * 32 + 7, 4, stride=8), :]
    for k in range(4):
        up_tiles[4 + k] = inside_ref[pl.ds(k * 64 + 7, 8, stride=8), :]
        down_tiles[4 + k] = inside_ref[pl.ds(k * 64, 8, stride=8), :]
    inverse = 1.0 / inside_ref[pl.ds(1, 8, stride=8), :]
    for k in range(3):
        down_tiles[8 + k] = inside_ref[pl.ds((k + 1) * 64 + 1, 8, stride=8), :] * inverse
    for t in range(11):
        u = up_tiles[t] if t < 8 else down_tiles[t]
        d = down_tiles[t]
        first_ref[t] = choose(even_y, u, d)
        second_ref[t] = choose(even_y, d, u)


def crossing(tiles, n, x):
    return row_of(tiles[n], x) if n < 4 else row_of(tiles[3], 4 + x)


def finish_fluid(info_ref, stepped_ref, inside_ref, leaving_ref, first_y, second_y, out_ref, flow):
    even_y = info_ref[1] == 0.0
    rows = tile_rows()
    below = [choose(even_y, second_y[t], first_y[t]) for t in range(8)]
    above = [choose(even_y, first_y[t], second_y[t]) for t in range(11)]
    for q in range(19):
        for x in range(4):
            s = stepped_ref[(q * 4 + x) * 8 : (q * 4 + x + 1) * 8, :]
            if q in UP_Y:
                s = jnp.where(rows == 0, crossing(below, UP_Y.index(q), x), s)
            if q in DOWN_Y:
                s = jnp.where(rows == 7, crossing(above, DOWN_Y.index(q), x), s)
            out_ref[q, x] = s

    def arriving(tiles, members):
        crossed = list(tiles[:4]) + [pltpu.roll(tiles[3], 4, 0)]
        out = []
        for k, what in enumerate((None, 0, 2)):
            total = None
            for n, q in enumerate(members):
                weight = 1 if what is None else VELOCITIES[q][what]
                if weight:
                    term = crossed[n] if weight == 1 else -crossed[n]
                    total = term if total is None else total + term
            out.append(jnp.where(rows < 4, total, tiles[k]))
        return [out[0], out[1], None, out[2]]

    from_below = arriving(below, UP_Y)
    from_above = arriving(above, DOWN_Y)
    from_below[2] = from_below[0]
    from_above[2] = -from_above[0]
    up = [leaving_ref[0], leaving_ref[1], leaving_ref[0], leaving_ref[2]]
    down = [leaving_ref[3], leaving_ref[4], -leaving_ref[3], leaving_ref[5]]
    edges = [[inside_ref[pl.ds(k * 64 + y, 8, stride=8), :] for k in range(4)] for y in (0, 7)]
    rims = (
        (0, [above[4 + k] + up[k] for k in range(4)]),
        (2, [below[4 + k] + down[k] for k in range(4)]),
        (3, [edges[0][k] + from_below[k] for k in range(4)]),
        (4, [edges[1][k] + from_above[k] for k in range(4)]),
    )
    for n, total in rims:
        inverse = 1.0 / jnp.where(rows == 7, 1.0, total[0])
        for a in range(3):
            start = (a * 5 + n) * 8
            flow[start : start + 8, :] = jnp.where(rows == 7, 0.0, total[1 + a] * inverse)
    for a in range(3):
        start = (a * 5 + 1) * 8
        flow[start : start + 8, :] = above[8 + a]


def along_depth(flow, depth_ref, slot):
    both = halves(flow)
    both = jnp.concatenate([both, both], axis=1)
    along = jnp.dot(both, depth_ref[slot], preferred_element_type=F32)
    return along[: flow.shape[0]] + along[flow.shape[0] :]


def six_sums(moved):
    return jnp.concatenate(moved + [jnp.zeros((2, PAD), F32)], axis=0)


def early_kernel(inside_ref, plane_ref, depth_ref, early_ref, flow):
    rows = tile_rows()
    inner_row = (rows > 0) & (rows < 7)
    for n in range(7):
        total = [inside_ref[(k * 8 + n) * 8 : (k * 8 + n + 1) * 8, :] for k in range(4)]
        inverse = 1.0 / total[0]
        for a in range(3):
            start = (a * 7 + n) * 8
            flow[start : start + 8, :] = jnp.where(inner_row, total[1 + a] * inverse, 0.0)
    moved = [None] * 6
    for slot in range(SLOTS):
        table_x, table_y = plane_ref[slot, 0], plane_ref[slot, 1]
        along = along_depth(flow[...], depth_ref, slot)
        for a in range(3):
            inner = None
            for n in range(7):
                term = along[(a * 7 + n) * 8 : (a * 7 + n + 1) * 8, :] * row_of(table_x, n)
                inner = term if inner is None else inner + term
            moved[2 * a + slot] = jnp.sum(inner * table_y, axis=0, keepdims=True)
    early_ref[...] = six_sums(moved)


def sample(offset, live, plane_ref, depth_ref, early_ref, flow):
    moved = [None] * 6
    for slot in range(SLOTS):
        table_x, table_rim = plane_ref[slot, 0], plane_ref[slot, 2]
        along = along_depth(flow[...], depth_ref, slot)
        for a in range(3):
            outer = None
            for n in range(5):
                term = along[(a * 5 + n) * 8 : (a * 5 + n + 1) * 8, :] * row_of(table_rim, n)
                outer = term if outer is None else outer + term
            moved[2 * a + slot] = jnp.sum(outer * table_x, axis=0, keepdims=True)
    return offset + live * (early_ref[...] + six_sums(moved))


def finish_kernel(
    info_ref, stepped_ref, inside_ref, leaving_ref, first_y, second_y, solid_ref,
    out_ref, flow_ref, first_ref, second_ref,
):
    finish_fluid(info_ref, stepped_ref, inside_ref, leaving_ref, first_y, second_y, out_ref, flow_ref)
    halo_messages(info_ref, out_ref, solid_ref, first_ref, second_ref)


def next_kernel(
    info_ref, flow_ref, plane_in, depth_in, early_ref, offset_ref, rest_ref, base_ref, incidence_ref,
    main_ref, first_ref, second_ref, plane_ref, depth_ref, offset_out, rim_ref, terms,
):
    offset = sample(offset_ref[...], wide(info_ref[5]), plane_in, depth_in, early_ref, flow_ref)
    offset_out[...] = offset
    spread(
        offset, rest_ref[...], wide(info_ref[4]), base_ref[...],
        incidence_ref, terms, main_ref, rim_ref, plane_ref, depth_ref,
    )
    spread_messages(info_ref, rim_ref, first_ref, second_ref)


def last_kernel(
    info_ref, stepped_ref, inside_ref, leaving_ref, first_y, second_y, plane_in, depth_in, early_ref, offset_ref,
    out_ref, offset_out, flow,
):
    finish_fluid(info_ref, stepped_ref, inside_ref, leaving_ref, first_y, second_y, out_ref, flow)
    offset = sample(offset_ref[...], wide(info_ref[5]), plane_in, depth_in, early_ref, flow)
    for a in range(3):
        offset_out[a] = offset[2 * a : 2 * a + 2]


INTERPRET = False


def call(kernel, outs, scratch, *operands):
    return pl.pallas_call(
        kernel,
        out_shape=[jax.ShapeDtypeStruct(shape, dtype) for shape, dtype in outs],
        in_specs=[pl.BlockSpec(memory_space=pltpu.VMEM)] * len(operands),
        out_specs=[pl.BlockSpec(memory_space=pltpu.VMEM)] * len(outs),
        scratch_shapes=[pltpu.VMEM(shape, dtype) for shape, dtype in scratch],
        compiler_params=pltpu.CompilerParams(vmem_limit_bytes=24 * 1024 * 1024),
        interpret=INTERPRET,
    )(*operands)


def partner(index, kind, size):
    return (index + 1) % size if (index + kind) % 2 == 0 else (index - 1) % size


def exchange(first, second, axis):
    size = lax.axis_size(axis)
    out = [None, None]
    for kind, message in ((1, second), (0, first)):
        pairs = [(i, partner(i, kind, size)) for i in range(size)]
        out[kind] = lax.ppermute(message, axis, pairs)
    return out


SPREAD_OUT = [
    ((3, 7, 8, CZ), F32),
    ((3, 2, 8, CZ), F32),
    ((3, 2, 8, CZ), F32),
    ((SLOTS, 3, 8, PAD), F32),
    ((SLOTS, 2 * CZ, PAD), jnp.bfloat16),
]
HALO_OUT = [((27, 8, CZ), F32)] * 2
STEPPED = ((19, 4, 8, CZ), F32)


def steps(populations, solid, base_cell, offset, rest_displacement, stiffness, occupied, triangles):
    stored = (3, SLOTS, PAD)
    rows = (8, PAD)
    scratch = [((3, 3, 8, CZ), F32), ((TABLE_ROWS, PAD), F32)]
    flow_out = ((LATE_ROWS, CZ), F32)
    corners = triangles.T
    (incidence,) = call(incidence_kernel, [((PAD, corners.shape[1]), jnp.bfloat16)], [], corners)
    info, populations, solid, first_h, second_h = call(
        halo_kernel,
        [((6, 8, CZ), F32), STEPPED, (solid.shape, jnp.int32)] + HALO_OUT, [],
        stiffness.reshape(1, SLOTS), occupied.reshape(1, SLOTS), populations, solid,
    )
    main, first, second, plane, depth, where, rest, base = call(
        spread_kernel, SPREAD_OUT + [(rows, F32), (rows, F32), (rows, jnp.int32)], scratch,
        info, offset.reshape(stored), rest_displacement.reshape(stored), base_cell.reshape(stored),
        incidence,
    )
    for substep in range(SUBSTEPS):
        first_h, second_h = exchange(first_h, second_h, "gx")
        first, second = exchange(first, second, "gy")
        whole, first, second = call(
            force_kernel, [((3, 7, 8, CZ), F32), ((3, 4, 8, CZ), F32), ((3, 4, 8, CZ), F32)], [],
            info, main, first, second,
        )
        first, second = exchange(first, second, "gx")
        stepped, inside, leaving, first, second = call(
            collide_kernel,
            [
                ((20 * 4 * 8 + 8, CZ), F32), ((5 * 8 * 8, CZ), F32), ((6, 8, CZ), F32),
                ((11, 8, CZ), F32), ((11, 8, CZ), F32),
            ],
            [((4 * 8 * 8, CZ), F32), ((8, 8, CZ), F32), ((11, 8, CZ), F32)],
            info, populations, solid, whole, first, second, first_h, second_h,
        )
        first, second = exchange(first, second, "gy")
        (early,) = call(early_kernel, [(rows, F32)], [((MAIN_ROWS, CZ), F32)], inside, plane, depth)
        fluid = (info, stepped, inside, leaving, first, second)
        if substep < SUBSTEPS - 1:
            populations, flow, first_h, second_h = call(
                finish_kernel, [STEPPED, flow_out] + HALO_OUT, [], *fluid, solid
            )
            main, first, second, plane, depth, where = call(
                next_kernel, SPREAD_OUT + [(rows, F32)], scratch,
                info, flow, plane, depth, early, where, rest, base, incidence,
            )
        else:
            populations, where = call(
                last_kernel, [STEPPED, (stored, F32)], [flow_out], *fluid, plane, depth, early, where
            )
    return populations, where.reshape(offset.shape)


def solution(mesh):
    in_specs = (
        P(None, "gx", "gy", None),
        P("gx", "gy", None),
        P(None, "gx", "gy", None, None),
        P(None, "gx", "gy", None, None),
        P(None, "gx", "gy", None, None),
        P("gx", "gy", None),
        P("gx", "gy", None),
        P(),
    )
    out_specs = (P(None, "gx", "gy", None), P(None, "gx", "gy", None, None))
    return jax.shard_map(steps, mesh=mesh, in_specs=in_specs, out_specs=out_specs, check_vma=False)
```
